8 devices in a mesh: data: 2 (over z, y), seq: 4 (over x, core).
Axes of the slice: x: 2, y: 2, z: 1, core: 2. Of those that a mesh axis runs over, the one named last changes fastest.
Arguments:
- dec_in: bfloat16 [2048, 768], P(('data', 'seq')), parts along dimension 0
- memory: bfloat16 [16384, 768], P(('data', 'seq')), parts along dimension 0
- mem_len: int32 [2], P('data'), parts along dimension 0
- grad_out: float32 [2048, 768], P(('data', 'seq')), parts along dimension 0
- norm_attn: bfloat16 [768], replicated
- wq_cross: bfloat16 [768, 12, 64], replicated
- wk_cross: bfloat16 [768, 12, 64], replicated
- wv_cross: bfloat16 [768, 12, 64], replicated
- wo_cross: bfloat16 [12, 64, 768], replicated
- norm_mlp: bfloat16 [768], replicated
- w_gate: bfloat16 [768, 3072], replicated
- w_up: bfloat16 [768, 3072], replicated
- w_down: bfloat16 [3072, 768], replicated
Outputs:
- output 1: float32 [2048, 768], P(('data', 'seq')), parts along dimension 0
- output 2: float32 [16384, 768], P(('data', 'seq')), parts along dimension 0
- output 3: float32 [1536], P('data'), parts along dimension 0
- output 4: float32 [1536, 12, 64], P('data'), parts along dimension 0
- output 5: float32 [1536, 12, 64], P('data'), parts along dimension 0
- output 6: float32 [1536, 12, 64], P('data'), parts along dimension 0
- output 7: float32 [24, 64, 768], P('data'), parts along dimension 0
- output 8: float32 [1536], P('data'), parts along dimension 0
- output 9: float32 [1536, 3072], P('data'), parts along dimension 0
- output 10: float32 [1536, 3072], P('data'), parts along dimension 0
- output 11: float32 [6144, 768], P('data'), parts along dimension 0
There are 2 independent parts. The reference program is written for one: setup_inputs(seed, part) draws one part's arguments, and reference() takes and returns one part's arrays. A program takes and returns all parts, laid end to end along the dimension named above; an argument that names none is the same for every part.
All inputs are finite; a program needn't handle non-finite values.
Results may differ from the reference program's by a relative error of at most 0.013332.
Values are sent between devices in bfloat16 or wider.
A program may use at most 1 GiB of HBM per device.

```python
import functools
import jax
import jax.numpy as jnp
from jax import lax

TQ = 1024
TM = 8192
D = 768
HEADS = 12
KV_HEADS = 12
HEAD = 64
FF = 3072
QBLK = 256
SEGMENTS = 16


def setup_inputs(seed: int = 0, part: int = 0) -> dict:
    part_keys = jax.random.split(jax.random.fold_in(jax.random.key(seed), part), 5)
    shared_keys = jax.random.split(jax.random.key(seed + 1), 11)
    inv_width = D ** -0.5

    def normal_draw(key, shape, spread):
        return spread * jax.random.normal(key, shape, jnp.float32)

    topics = normal_draw(part_keys[1], (SEGMENTS, D), 1.0)
    memory = normal_draw(part_keys[2], (TM, D), 0.6) + 0.8 * jnp.repeat(topics, TM // SEGMENTS, axis=0)
    quarter = TM // 4
    mem_len = jax.random.randint(part_keys[3], (1,), quarter, TM - quarter + 1, dtype=jnp.int32)
    return {
        'dec_in': normal_draw(part_keys[0], (TQ, D), 1.0).astype(jnp.bfloat16),
        'memory': memory.astype(jnp.bfloat16),
        'mem_len': mem_len,
        'grad_out': normal_draw(part_keys[4], (TQ, D), 1.0),
        'norm_attn': (1.0 + normal_draw(shared_keys[0], (D,), 0.3)).astype(jnp.bfloat16),
        'wq_cross': normal_draw(shared_keys[1], (D, HEADS, HEAD), 1.2 * inv_width).astype(jnp.bfloat16),
        'wk_cross': normal_draw(shared_keys[2], (D, KV_HEADS, HEAD), 1.2 * inv_width).astype(jnp.bfloat16),
        'wv_cross': normal_draw(shared_keys[3], (D, KV_HEADS, HEAD), inv_width).astype(jnp.bfloat16),
        'wo_cross': normal_draw(shared_keys[4], (HEADS, HEAD, D), 1.5 * inv_width).astype(jnp.bfloat16),
        'norm_mlp': (1.0 + normal_draw(shared_keys[5], (D,), 0.3)).astype(jnp.bfloat16),
        'w_gate': normal_draw(shared_keys[6], (D, FF), inv_width).astype(jnp.bfloat16),
        'w_up': normal_draw(shared_keys[7], (D, FF), inv_width).astype(jnp.bfloat16),
        'w_down': normal_draw(shared_keys[8], (FF, D), FF ** -0.5).astype(jnp.bfloat16),
    }


def to_bf16(tensor):
    return tensor + lax.stop_gradient(tensor.astype(jnp.bfloat16).astype(jnp.float32) - tensor)


def rms_norm(tensor, gain):
    mean_sq = jnp.mean(tensor * tensor, axis=-1, keepdims=True)
    return tensor * lax.rsqrt(mean_sq + 1e-6) * gain


def layer_forward(valid_mask, dec_in, memory, norm_attn, wq_cross, wk_cross, wv_cross, wo_cross, norm_mlp, w_gate, w_up, w_down):
    normed = to_bf16(rms_norm(dec_in, norm_attn))
    dec_query = to_bf16(jnp.einsum('td,dhe->the', normed, wq_cross))
    dec_query = dec_query.reshape(TQ // QBLK, QBLK, KV_HEADS, HEADS // KV_HEADS, HEAD)
    mem_keys = to_bf16(jnp.einsum('td,dke->tke', memory, wk_cross))
    mem_vals = to_bf16(jnp.einsum('td,dke->tke', memory, wv_cross))

    def block_attention(query_block):
        scores = jnp.einsum('qkge,tke->qkgt', query_block, mem_keys) * (HEAD ** -0.5)
        scores = jnp.where(valid_mask, scores, -1e30)
        attn_prob = jax.nn.softmax(scores, axis=-1)
        return jnp.einsum('qkgt,tke->qkge', attn_prob, mem_vals)

    attended = to_bf16(lax.map(jax.checkpoint(block_attention), dec_query).reshape(TQ, HEADS, HEAD))
    hidden = to_bf16(dec_in + jnp.einsum('the,hed->td', attended, wo_cross))
    normed_mlp = to_bf16(rms_norm(hidden, norm_mlp))
    gate_pre = jnp.dot(normed_mlp, w_gate, preferred_element_type=jnp.float32)
    up_pre = jnp.dot(normed_mlp, w_up, preferred_element_type=jnp.float32)
    mlp_act = to_bf16(jax.nn.silu(gate_pre) * up_pre)
    return hidden + jnp.dot(mlp_act, w_down, preferred_element_type=jnp.float32)


def reference(dec_in, memory, mem_len, grad_out, norm_attn, wq_cross, wk_cross, wv_cross, wo_cross, norm_mlp, w_gate, w_up, w_down):
    valid_mask = jnp.arange(TM) < mem_len[0]
    primals = [tensor.astype(jnp.float32) for tensor in (dec_in, memory, norm_attn, wq_cross, wk_cross, wv_cross, wo_cross, norm_mlp, w_gate, w_up, w_down)]
    _, pullback = jax.vjp(functools.partial(layer_forward, valid_mask), *primals)
    (g_dec, g_mem, g_norm_attn, g_wq, g_wk, g_wv, g_wo, g_norm_mlp, g_gate, g_up, g_down) = pullback(grad_out.astype(jnp.float32))
    return (g_dec, g_mem, g_norm_attn, g_wq, g_wk, g_wv, g_wo, g_norm_mlp, g_gate, g_up, g_down)
```

```python
import functools

import jax
import jax.numpy as jnp
from jax import lax
from jax.experimental import pallas as pl
from jax.experimental.pallas import tpu as pltpu
from jax.sharding import PartitionSpec as P

LOG2E = 1.4426950408889634
NEG = -1e30
BF = jnp.bfloat16
F32 = jnp.float32
FKB = 512
FQB = 512
BKB = 256
BQB = 512
PAIR = 128
OROWS = 72


def dot(a, b):
    return jnp.dot(a, b, preferred_element_type=F32)


def fwd_kernel(len_ref, qt_ref, k0_ref, k1_ref, vt0_ref, vt1_ref, o_ref, m_ref, l_ref, acc_ref, qz_ref):
    qb = qt_ref.shape[1]
    half = lax.broadcasted_iota(jnp.int32, (PAIR, qb), 0) // 64
    for h in range(2):
        qz_ref[h] = jnp.where(half == h, qt_ref[...], jnp.zeros((), BF))
    m_ref[...] = jnp.full(m_ref.shape, NEG, F32)
    l_ref[...] = jnp.zeros(l_ref.shape, F32)
    acc_ref[...] = jnp.zeros(acc_ref.shape, F32)

    for seg, (k_ref, vt_ref) in enumerate(((k0_ref, vt0_ref), (k1_ref, vt1_ref))):
        count = len_ref[seg]

        def step(j, masked):
            rows = pl.ds(pl.multiple_of(j * FKB, FKB), FKB)
            kb = k_ref[rows, :]
            for h in range(2):
                st = dot(kb, qz_ref[h])
                if masked:
                    pos = lax.broadcasted_iota(jnp.int32, st.shape, 0) + j * FKB
                    st = jnp.where(pos < count, st, NEG)
                m_old = m_ref[h]
                m_new = jnp.maximum(m_old, jnp.max(st, axis=0, keepdims=True))
                p = jnp.exp2((st - m_new) * LOG2E)
                alpha = jnp.exp2((m_old - m_new) * LOG2E)
                l_ref[h] = l_ref[h] * alpha + jnp.sum(p, axis=0, keepdims=True)
                pv = dot(vt_ref[h * 64:(h + 1) * 64, rows], p.astype(BF))
                acc_ref[h] = acc_ref[h] * alpha + pv
                m_ref[h] = m_new

        full = count // FKB

        @pl.loop(0, full)
        def _(j):
            step(j, False)

        @pl.when(full * FKB < count)
        def _():
            step(full, True)

    for h in range(2):
        o_ref[h, 0:64, :] = acc_ref[h]
        o_ref[h, 64:72, :] = jnp.concatenate(
            [m_ref[h], l_ref[h], jnp.zeros((6, qb), F32)], axis=0)


def attention_forward(lens, qt, k0, k1, vt0, vt1, pair0, pairs):
    nq = qt.shape[1]
    rows = k0.shape[0]
    off = pair0
    spec = pltpu.PrefetchScalarGridSpec(
        num_scalar_prefetch=1,
        grid=(pairs, nq // FQB),
        in_specs=[
            pl.BlockSpec((PAIR, FQB), lambda p, i, s: (p + off, i)),
            pl.BlockSpec((rows, PAIR), lambda p, i, s: (0, p + off)),
            pl.BlockSpec((rows, PAIR), lambda p, i, s: (0, p + off)),
            pl.BlockSpec((PAIR, rows), lambda p, i, s: (p + off, 0)),
            pl.BlockSpec((PAIR, rows), lambda p, i, s: (p + off, 0)),
        ],
        out_specs=pl.BlockSpec((2, OROWS, FQB), lambda p, i, s: (p, 0, i)),
        scratch_shapes=[
            pltpu.VMEM((2, 1, FQB), F32),
            pltpu.VMEM((2, 1, FQB), F32),
            pltpu.VMEM((2, 64, FQB), F32),
            pltpu.VMEM((2, PAIR, FQB), BF),
        ])
    work = 2 * pairs * nq * 2 * rows
    return pl.pallas_call(
        fwd_kernel,
        out_shape=jax.ShapeDtypeStruct((2 * pairs, OROWS, nq), F32),
        grid_spec=spec,
        compiler_params=pltpu.CompilerParams(vmem_limit_bytes=48 << 20),
        cost_estimate=pl.CostEstimate(flops=work * 256 * 2, bytes_accessed=8 << 20, transcendentals=work),
        name="attn_fwd",
    )(lens, qt, k0, k1, vt0, vt1)


def bwd_kernel(len_ref, qt_ref, q_ref, dot_ref, do_ref, lse_ref, dl_ref,
               k0_ref, k1_ref, v0_ref, v1_ref, kt0_ref, kt1_ref,
               dk0_ref, dk1_ref, dv0_ref, dv1_ref, dqt_ref,
               qzt_ref, qz_ref, dozt_ref, doz_ref):
    nq = q_ref.shape[0]
    half_r = lax.broadcasted_iota(jnp.int32, (PAIR, nq), 0) // 64
    half_c = lax.broadcasted_iota(jnp.int32, (nq, PAIR), 1) // 64
    zero = jnp.zeros((), BF)
    for h in range(2):
        qzt_ref[h] = jnp.where(half_r == h, qt_ref[...], zero)
        dozt_ref[h] = jnp.where(half_r == h, dot_ref[...], zero)
        qz_ref[h] = jnp.where(half_c == h, q_ref[...], zero)
        doz_ref[h] = jnp.where(half_c == h, do_ref[...], zero)
    dqt_ref[...] = jnp.zeros(dqt_ref.shape, F32)

    segs = ((k0_ref, v0_ref, kt0_ref, dk0_ref, dv0_ref), (k1_ref, v1_ref, kt1_ref, dk1_ref, dv1_ref))
    for seg, (k_ref, v_ref, kt_ref, dk_ref, dv_ref) in enumerate(segs):
        count = len_ref[seg]
        blocks = k_ref.shape[0] // BKB

        def step(j, masked):
            rows = pl.ds(pl.multiple_of(j * BKB, BKB), BKB)
            kb, vb = k_ref[rows, :], v_ref[rows, :]
            dk = jnp.zeros((BKB, PAIR), F32)
            dv = jnp.zeros((BKB, PAIR), F32)
            for h in range(2):
                ktb = kt_ref[h * 64:(h + 1) * 64, rows]
                for c in range(nq // BQB):
                    cols = slice(c * BQB, (c + 1) * BQB)
                    st = dot(kb, qzt_ref[h, :, cols])
                    p = jnp.exp2((st - lse_ref[h, :, cols]) * LOG2E)
                    if masked:
                        pos = lax.broadcasted_iota(jnp.int32, st.shape, 0) + j * BKB
                        p = jnp.where(pos < count, p, 0.0)
                    dp = dot(vb, dozt_ref[h, :, cols])
                    ds = (p * (dp - dl_ref[h, :, cols])).astype(BF)
                    dv = dv + dot(p.astype(BF), doz_ref[h, cols, :])
                    dk = dk + dot(ds, qz_ref[h, cols, :])
                    dqt_ref[h, :, cols] += dot(ktb, ds)
            dk_ref[rows, :] = dk.astype(BF)
            dv_ref[rows, :] = dv.astype(BF)

        full = count // BKB

        @pl.loop(0, full)
        def _(j):
            step(j, False)

        @pl.when(full * BKB < count)
        def _():
            step(full, True)

        @pl.loop((count + BKB - 1) // BKB, blocks)
        def _(j):
            rows = pl.ds(pl.multiple_of(j * BKB, BKB), BKB)
            dk_ref[rows, :] = jnp.zeros((BKB, PAIR), BF)
            dv_ref[rows, :] = jnp.zeros((BKB, PAIR), BF)


def attention_backward(lens, qt, q, dot_t, do, lse, delta, k0, k1, v0, v1, kt0, kt1, pair0, pairs):
    nq = q.shape[0]
    rows = k0.shape[0]
    off = pair0
    across = pl.BlockSpec((PAIR, nq), lambda p, s: (p + off, 0))
    down = pl.BlockSpec((nq, PAIR), lambda p, s: (0, p + off))
    stat = pl.BlockSpec((2, 1, nq), lambda p, s: (p + off, 0, 0))
    keys = pl.BlockSpec((rows, PAIR), lambda p, s: (0, p + off))
    keys_t = pl.BlockSpec((PAIR, rows), lambda p, s: (p + off, 0))
    keys_out = pl.BlockSpec((rows, PAIR), lambda p, s: (0, p))
    spec = pltpu.PrefetchScalarGridSpec(
        num_scalar_prefetch=1,
        grid=(pairs,),
        in_specs=[across, down, across, down, stat, stat, keys, keys, keys, keys, keys_t, keys_t],
        out_specs=[keys_out] * 4 + [pl.BlockSpec((2, 64, nq), lambda p, s: (p, 0, 0))],
        scratch_shapes=[
            pltpu.VMEM((2, PAIR, nq), BF), pltpu.VMEM((2, nq, PAIR), BF),
            pltpu.VMEM((2, PAIR, nq), BF), pltpu.VMEM((2, nq, PAIR), BF),
        ])
    work = 2 * pairs * nq * 2 * rows
    key_out = jax.ShapeDtypeStruct((rows, pairs * PAIR), BF)
    return pl.pallas_call(
        bwd_kernel,
        out_shape=[key_out] * 4 + [jax.ShapeDtypeStruct((2 * pairs, 64, nq), F32)],
        grid_spec=spec,
        compiler_params=pltpu.CompilerParams(vmem_limit_bytes=56 << 20),
        cost_estimate=pl.CostEstimate(flops=work * 640 * 2, bytes_accessed=16 << 20, transcendentals=work),
        name="attn_bwd",
    )(lens, qt, q, dot_t, do, lse, delta, k0, k1, v0, v1, kt0, kt1)


def inv_rms(tensor):
    return lax.rsqrt(jnp.mean(tensor * tensor, axis=-1, keepdims=True) + 1e-6)


def norm_back(unit, inv, gain, grad):
    scaled = grad * gain
    return inv * (scaled - unit * jnp.mean(scaled * unit, axis=-1, keepdims=True))


def mm(a, b, ca, cb, dtype=F32):
    out = lax.dot_general(a, b, (((ca,), (cb,)), ((), ())), preferred_element_type=F32)
    return out if dtype == F32 else out.astype(dtype)


def solution(mesh):
    n = mesh.shape['seq']
    near = [(i, i ^ 1) for i in range(n)]
    far = [(i, i ^ 2) for i in range(n)]
    row_spec = P(('data', 'seq'), None)
    weight_spec = P()
    part_vec = P('data')
    part_mat = P('data', None)
    part_cube = P('data', None, None)

    def to_near(a):
        return lax.ppermute(a, 'seq', near)

    def to_far(a):
        return lax.ppermute(a, 'seq', far)

    def device_step(dec_in, memory, mem_len, grad_out, norm_attn, wq, wk, wv, wo, norm_mlp, w_gate, w_up, w_down):
        rows, dim = dec_in.shape
        m_rows = memory.shape[0]
        heads, head = wq.shape[1], wq.shape[2]
        mine = heads // 2
        width = mine * head
        dev = lax.axis_index('seq')
        core = lax.rem(dev, 2)
        wq2, wk2, wv2 = (w.reshape(dim, heads * head) for w in (wq, wk, wv))
        wo2 = wo.reshape(heads * head, dim)
        lens = jnp.stack([jnp.clip(mem_len[0] - i * m_rows, 0, m_rows) for i in (dev, dev ^ 1)]).astype(jnp.int32)

        def gather_rows(a):
            across = to_far(a)
            out = jnp.zeros((n * rows,) + a.shape[1:], a.dtype)
            for part, who in ((a, dev), (across, dev ^ 2), (to_near(a), dev ^ 1), (to_near(across), dev ^ 3)):
                out = lax.dynamic_update_slice(out, part, (who * rows, 0))
            return out

        def my_cols(w):
            return lax.dynamic_slice(w, (0, core * width), (dim, width))

        x_all_b = gather_rows(dec_in)
        mem_near = to_near(memory)
        g_all = gather_rows(grad_out)
        gain1 = norm_attn.astype(F32)
        gain2 = norm_mlp.astype(F32)

        wq_m, wk_m, wv_m = my_cols(wq2), my_cols(wk2), my_cols(wv2)
        kv = []
        for mem in (memory, mem_near):
            kv.append((mm(mem, wk_m, 1, 0, BF), mm(mem, wv_m, 1, 0, BF),
                       mm(wk_m, mem, 0, 1, BF), mm(wv_m, mem, 0, 1, BF)))
        (k0, v0, kt0, vt0), (k1, v1, kt1, vt1) = kv

        x_all = x_all_b.astype(F32)
        inv1 = inv_rms(x_all)
        unit1 = x_all * inv1
        n1 = (unit1 * gain1).astype(BF)
        q = mm(n1, wq_m, 1, 0, BF)
        scale = jnp.asarray(head ** -0.5, BF)
        q_s = q * scale
        qt_s = q_s.T

        groups = [(0, 1), (1, 1), (2, 1)]
        parts = []
        for pair0, pairs in groups:
            part = attention_forward(lens, qt_s, k0, k1, vt0, vt1, pair0, pairs)
            parts.append((part, to_far(part)))
        outs, lses = [], []
        for a, b in parts:
            ma, mb = a[:, 64:65], b[:, 64:65]
            top = jnp.maximum(ma, mb)
            ea, eb = jnp.exp(ma - top), jnp.exp(mb - top)
            den = a[:, 65:66] * ea + b[:, 65:66] * eb
            outs.append((a[:, :64] * ea + b[:, :64] * eb) / den)
            lses.append(top + jnp.log(den))
        o_t = jnp.concatenate(outs, axis=0)
        lse = jnp.concatenate(lses, axis=0)
        o_t_b = o_t.astype(BF).reshape(width, n * rows)
        o_t_near = to_near(o_t_b)

        wo_m = lax.dynamic_slice(wo2, (core * width, 0), (width, dim))
        wo_n = lax.dynamic_slice(wo2, ((1 - core) * width, 0), (width, dim))
        hidden = (x_all + mm(o_t_b, wo_m, 0, 0) + mm(o_t_near, wo_n, 0, 0)).astype(BF)

        hid = hidden.astype(F32)
        inv2 = inv_rms(hid)
        unit2 = hid * inv2
        n2 = (unit2 * gain2).astype(BF)
        g_top = g_all.astype(BF)
        grad_act = mm(g_top, w_down, 1, 1)
        gate = mm(n2, w_gate, 1, 0)
        up = mm(n2, w_up, 1, 0)
        sig = jax.nn.sigmoid(gate)
        act = gate * sig
        mlp_act = (act * up).astype(BF)
        d_up = (grad_act * act).astype(BF)
        d_gate = (grad_act * up * (sig * (1.0 + gate * (1.0 - sig)))).astype(BF)
        d_n2 = mm(d_gate, w_gate, 1, 1) + mm(d_up, w_up, 1, 1)
        g_norm_mlp = jnp.sum(d_n2 * unit2, axis=0)
        d_hid = g_all + norm_back(unit2, inv2, gain2, d_n2)
        d_hid_b = d_hid.astype(BF)

        do_t_f = mm(wo_m, d_hid_b, 1, 1)
        delta = jnp.sum(do_t_f.reshape(mine, head, n * rows) * o_t, axis=1, keepdims=True)
        do_t = do_t_f.astype(BF)
        do = mm(d_hid_b, wo_m, 1, 1, BF)
        dks, dvs, dqs, dws = [], [], [], []
        for pair0, pairs in groups:
            dk0, dk1, dv0, dv1, dqt = attention_backward(
                lens, qt_s, q_s, do_t, do, lse, delta, k0, k1, v0, v1, kt0, kt1, pair0, pairs)
            dqs.append(dqt + to_far(dqt))
            dkv0 = jnp.concatenate([dk0, dv0], axis=1)
            dkv1 = jnp.concatenate([dk1, dv1], axis=1)
            dw = mm(memory, dkv0, 0, 0) + mm(mem_near, dkv1, 0, 0)
            dws.append(dw + to_far(dw))
            dks.append((dkv0, to_near(dkv1)))
        wide = PAIR
        dwk_m = jnp.concatenate([w[:, :wide] for w in dws], axis=1)
        dwv_m = jnp.concatenate([w[:, wide:] for w in dws], axis=1)
        dw_m = jnp.stack([dwk_m, dwv_m])
        dw_n = to_near(dw_m)
        low = jnp.where(core == 0, dw_m, dw_n)
        high = jnp.where(core == 0, dw_n, dw_m)
        dw_all = jnp.concatenate([low, high], axis=2).reshape(2, dim, heads, head)
        g_wk, g_wv = dw_all[0], dw_all[1]

        mine_kv = jnp.concatenate([a for a, _ in dks], axis=1)
        near_kv = jnp.concatenate([b for _, b in dks], axis=1)

        def pair_rows(wk_x, wv_x):
            cols = []
            for i in range(width // wide):
                cols += [wk_x[:, i * wide:(i + 1) * wide], wv_x[:, i * wide:(i + 1) * wide]]
            return jnp.concatenate(cols, axis=1)

        def near_cols(w):
            return lax.dynamic_slice(w, (0, (1 - core) * width), (dim, width))

        g_mem = (mm(mine_kv, pair_rows(wk_m, wv_m), 1, 1)
                 + mm(near_kv, pair_rows(near_cols(wk2), near_cols(wv2)), 1, 1))

        dqt_b = (jnp.concatenate(dqs, axis=0) * (head ** -0.5)).astype(BF).reshape(width, n * rows)
        dqt_near = to_near(dqt_b)
        dwq_m = mm(n1, dqt_b, 0, 1)
        dwq_n = mm(n1, dqt_near, 0, 1)
        g_wq = jnp.concatenate([jnp.where(core == 0, dwq_m, dwq_n), jnp.where(core == 0, dwq_n, dwq_m)],
                               axis=1).reshape(dim, heads, head)
        d_n1 = mm(dqt_b, wq_m, 0, 1) + mm(dqt_near, near_cols(wq2), 0, 1)
        g_norm_attn = jnp.sum(d_n1 * unit1, axis=0)
        d_x = d_hid + norm_back(unit1, inv1, gain1, d_n1)
        g_dec = lax.dynamic_slice(d_x, (dev * rows, 0), (rows, dim))

        gwo_m = mm(o_t_b, d_hid_b, 1, 0)
        gwo_n = mm(o_t_near, d_hid_b, 1, 0)
        g_wo = jnp.concatenate([jnp.where(core == 0, gwo_m, gwo_n), jnp.where(core == 0, gwo_n, gwo_m)],
                               axis=0).reshape(heads, head, dim)
        g_gate = mm(n2, d_gate, 0, 0)
        g_up = mm(n2, d_up, 0, 0)
        g_down = mm(mlp_act, g_top, 0, 0)
        return (g_dec, g_mem, g_norm_attn, g_wq, g_wk, g_wv, g_wo, g_norm_mlp, g_gate, g_up, g_down)

    return jax.shard_map(device_step, mesh=mesh,
                         in_specs=(row_spec, row_spec, part_vec, row_spec) + (weight_spec,) * 9,
                         out_specs=(row_spec, row_spec, part_vec, part_cube, part_cube, part_cube, part_cube,
                                    part_vec, part_mat, part_mat, part_mat),
                         check_vma=False)
```

```python
import functools

import jax
import jax.numpy as jnp
from jax import lax
from jax.experimental import pallas as pl
from jax.experimental.pallas import tpu as pltpu
from jax.sharding import PartitionSpec as P

LOG2E = 1.4426950408889634
NEG = -1e30
BF = jnp.bfloat16
F32 = jnp.float32
FKB = 512
FQB = 512
BKB = 512
BQB = 256
PAIR = 128
OROWS = 72
FFB = 512
MB = 512


def dot(a, b):
    return jnp.dot(a, b, preferred_element_type=F32)


def dot_nt(a, b):
    return lax.dot_general(a, b, (((1,), (1,)), ((), ())), preferred_element_type=F32)


def dot_tn(a, b):
    return lax.dot_general(a, b, (((0,), (0,)), ((), ())), preferred_element_type=F32)


def cost(flops, bytes_accessed, exps=0):
    return pl.CostEstimate(flops=int(flops), bytes_accessed=int(bytes_accessed), transcendentals=int(exps))


def proj_kernel(core_ref, m_ref, wk_ref, wv_ref, *refs):
    k_ref, v_ref, kt_ref, vt_ref = refs[-4:]
    m = m_ref[...]
    k = dot_nt(m, wk_ref[...]).astype(BF)
    v = dot_nt(m, wv_ref[...]).astype(BF)
    k_ref[...] = k
    v_ref[...] = v
    kt_ref[...] = k.T
    vt_ref[...] = v.T


def project(core, mem, wkt, wvt, seg, before):
    rows, dim = mem.shape
    width = wkt.shape[0] // 2
    steps = rows // MB
    base = seg * steps
    weights = pl.BlockSpec((width, dim), lambda i, s: (s[0], 0))
    down = pl.BlockSpec((MB, width), lambda i, s: (base + i, 0))
    across = pl.BlockSpec((width, MB), lambda i, s: (0, base + i))
    outs = [jax.ShapeDtypeStruct((2 * rows, width), BF)] * 2 + [jax.ShapeDtypeStruct((width, 2 * rows), BF)] * 2
    return pl.pallas_call(
        proj_kernel,
        out_shape=outs,
        grid_spec=pltpu.PrefetchScalarGridSpec(
            num_scalar_prefetch=1, grid=(steps,),
            in_specs=[pl.BlockSpec((MB, dim), lambda i, s: (i, 0)), weights, weights]
                     + [pl.BlockSpec(memory_space=pl.ANY)] * len(before),
            out_specs=[down, down, across, across]),
        input_output_aliases={4 + i: i for i in range(len(before))},
        compiler_params=pltpu.CompilerParams(vmem_limit_bytes=24 << 20),
        cost_estimate=cost(4 * rows * dim * width, 12 << 20),
        name="kv_proj",
    )(core, mem, wkt, wvt, *before)


def query_kernel(place_ref, x0_ref, x1_ref, x2_ref, x3_ref, gain_ref, wq_ref, x_ref, n_ref, q_ref, qt_ref):
    for part, src in enumerate((x0_ref, x1_ref, x2_ref, x3_ref)):
        @pl.when(pl.program_id(0) == part)
        def _():
            xb = src[...]
            x = xb.astype(F32)
            n1 = (x * inv_rms(x) * gain_ref[...]).astype(BF)
            q = dot_nt(n1, wq_ref[...]).astype(BF) * jnp.asarray(0.125, BF)
            x_ref[...] = xb
            n_ref[...] = n1
            q_ref[...] = q
            qt_ref[...] = q.T


def queries(place, parts, gain, wqt):
    rows, dim = parts[0].shape
    width = wqt.shape[0] // 2
    n = len(parts)
    whole = pl.BlockSpec((rows, dim), lambda i, s: (0, 0))
    put = pl.BlockSpec((rows, dim), lambda i, s: (s[i], 0))
    return pl.pallas_call(
        query_kernel,
        out_shape=[jax.ShapeDtypeStruct((n * rows, dim), BF)] * 2
                  + [jax.ShapeDtypeStruct((n * rows, width), BF), jax.ShapeDtypeStruct((width, n * rows), BF)],
        grid_spec=pltpu.PrefetchScalarGridSpec(
            num_scalar_prefetch=1, grid=(n,),
            in_specs=[whole] * n + [pl.BlockSpec((1, dim), lambda i, s: (0, 0)),
                                    pl.BlockSpec((width, dim), lambda i, s: (s[n], 0))],
            out_specs=[put, put, pl.BlockSpec((rows, width), lambda i, s: (s[i], 0)),
                       pl.BlockSpec((width, rows), lambda i, s: (0, s[i]))]),
        compiler_params=pltpu.CompilerParams(vmem_limit_bytes=24 << 20),
        cost_estimate=cost(2 * n * rows * dim * width, 6 << 20),
        name="queries",
    )(place, *parts, gain, wqt)


def place_kernel(place_ref, x0_ref, x1_ref, x2_ref, x3_ref, o_ref):
    for part, src in enumerate((x0_ref, x1_ref, x2_ref, x3_ref)):
        @pl.when(pl.program_id(0) == part)
        def _():
            o_ref[...] = src[...]


def place_rows(place, parts):
    rows, dim = parts[0].shape
    n = len(parts)
    return pl.pallas_call(
        place_kernel,
        out_shape=jax.ShapeDtypeStruct((n * rows, dim), parts[0].dtype),
        grid_spec=pltpu.PrefetchScalarGridSpec(
            num_scalar_prefetch=1, grid=(n,),
            in_specs=[pl.BlockSpec((rows, dim), lambda i, s: (0, 0))] * n,
            out_specs=pl.BlockSpec((rows, dim), lambda i, s: (s[i], 0))),
        compiler_params=pltpu.CompilerParams(vmem_limit_bytes=16 << 20),
        cost_estimate=cost(n * rows * dim, 6 << 20),
        name="place_rows",
    )(place, *parts)


def fwd_kernel(len_ref, qt_ref, k_ref, vt_ref, o_ref, m_ref, l_ref, acc_ref, qz_ref, sa_ref, sb_ref):
    qb = qt_ref.shape[1]
    seg_rows = k_ref.shape[0] // 2
    half = lax.broadcasted_iota(jnp.int32, (PAIR, qb), 0) // 64
    for h in range(2):
        qz_ref[h] = jnp.where(half == h, qt_ref[...], jnp.zeros((), BF))
    m_ref[...] = jnp.full(m_ref.shape, NEG, F32)
    l_ref[...] = jnp.zeros(l_ref.shape, F32)
    acc_ref[...] = jnp.zeros(acc_ref.shape, F32)
    first = len_ref[0] // FKB
    total = first + len_ref[1] // FKB

    def base(t):
        t = jnp.clip(t, 0, jnp.maximum(total - 1, 0))
        return pl.multiple_of(jnp.where(t < first, t * FKB, seg_rows + (t - first) * FKB), FKB)

    def scores(row, s_ref):
        kb = k_ref[pl.ds(row, FKB), :]
        for h in range(2):
            s_ref[h] = dot(kb, qz_ref[h])

    def absorb(row, s_ref, count=None):
        rows = pl.ds(row, FKB)
        for h in range(2):
            st = s_ref[h]
            if count is not None:
                st = jnp.where(lax.broadcasted_iota(jnp.int32, st.shape, 0) < count, st, NEG)
            m_old = m_ref[h]
            m_new = jnp.maximum(m_old, jnp.max(st, axis=0, keepdims=True))
            p = jnp.exp2((st - m_new) * LOG2E)
            alpha = jnp.exp2((m_old - m_new) * LOG2E)
            l_ref[h] = l_ref[h] * alpha + jnp.sum(p, axis=0, keepdims=True)
            pv = dot(vt_ref[h * 64:(h + 1) * 64, rows], p.astype(BF))
            acc_ref[h] = acc_ref[h] * alpha + pv
            m_ref[h] = m_new

    scores(base(0), sa_ref)

    @pl.loop(0, total // 2)
    def _(i):
        scores(base(2 * i + 1), sb_ref)
        absorb(base(2 * i), sa_ref)
        scores(base(2 * i + 2), sa_ref)
        absorb(base(2 * i + 1), sb_ref)

    @pl.when(total % 2 == 1)
    def _():
        absorb(base(total - 1), sa_ref)

    @pl.loop(0, 2)
    def _(s):
        full = len_ref[s] // FKB
        rest = len_ref[s] - full * FKB

        @pl.when(rest > 0)
        def _():
            row = pl.multiple_of(s * seg_rows + full * FKB, FKB)
            scores(row, sa_ref)
            absorb(row, sa_ref, rest)

    for h in range(2):
        o_ref[h, 0:64, :] = acc_ref[h]
        o_ref[h, 64:72, :] = jnp.concatenate([m_ref[h], l_ref[h], jnp.zeros((6, qb), F32)], axis=0)


def attention_forward(lens, qt, k, vt, pair0, pairs):
    nq = qt.shape[1]
    rows = k.shape[0]
    off = pair0
    spec = pltpu.PrefetchScalarGridSpec(
        num_scalar_prefetch=1,
        grid=(pairs, nq // FQB),
        in_specs=[
            pl.BlockSpec((PAIR, FQB), lambda p, i, s: (p + off, i)),
            pl.BlockSpec((rows, PAIR), lambda p, i, s: (0, p + off)),
            pl.BlockSpec((PAIR, rows), lambda p, i, s: (p + off, 0)),
        ],
        out_specs=pl.BlockSpec((2, OROWS, FQB), lambda p, i, s: (p, 0, i)),
        scratch_shapes=[
            pltpu.VMEM((2, 1, FQB), F32), pltpu.VMEM((2, 1, FQB), F32), pltpu.VMEM((2, 64, FQB), F32),
            pltpu.VMEM((2, PAIR, FQB), BF), pltpu.VMEM((2, FKB, FQB), F32), pltpu.VMEM((2, FKB, FQB), F32),
        ])
    work = 2 * pairs * nq * rows
    return pl.pallas_call(
        fwd_kernel,
        out_shape=jax.ShapeDtypeStruct((2 * pairs, OROWS, nq), F32),
        grid_spec=spec,
        compiler_params=pltpu.CompilerParams(vmem_limit_bytes=24 << 20),
        cost_estimate=cost(work * 1024, 4 << 20, work),
        name="attn_fwd",
    )(lens, qt, k, vt)


def bwd_kernel(len_ref, qt_ref, dot_ref, lse_ref, dl_ref, k_ref, v_ref, kt_ref, dkv_ref, dqt_ref, qzt_ref, dozt_ref):
    nq = qt_ref.shape[1]
    seg_rows = k_ref.shape[0] // 2
    blocks = seg_rows // BKB
    half = lax.broadcasted_iota(jnp.int32, (PAIR, nq), 0) // 64
    zero = jnp.zeros((), BF)
    for h in range(2):
        qzt_ref[h] = jnp.where(half == h, qt_ref[...], zero)
        dozt_ref[h] = jnp.where(half == h, dot_ref[...], zero)
    dqt_ref[...] = jnp.zeros(dqt_ref.shape, F32)

    def step(seg, j, count):
        cols = pl.ds(pl.multiple_of(j * BKB, BKB), BKB)
        allc = pl.ds(pl.multiple_of(seg * seg_rows + j * BKB, BKB), BKB)
        kb, vb = k_ref[allc, :], v_ref[allc, :]
        for h in range(2):
            hs = slice(h * 64, (h + 1) * 64)
            ktb = kt_ref[hs, allc]
            dk = jnp.zeros((64, BKB), F32)
            dv = jnp.zeros((64, BKB), F32)
            for c in range(nq // BQB):
                qs = slice(c * BQB, (c + 1) * BQB)
                st = dot(kb, qzt_ref[h, :, qs])
                p = jnp.exp2((st - lse_ref[h, :, qs]) * LOG2E)
                if count is not None:
                    p = jnp.where(lax.broadcasted_iota(jnp.int32, st.shape, 0) < count, p, 0.0)
                dp = dot(vb, dozt_ref[h, :, qs])
                ds = (p * (dp - dl_ref[h, :, qs])).astype(BF)
                dv = dv + dot_nt(dot_ref[hs, qs], p.astype(BF))
                dk = dk + dot_nt(qt_ref[hs, qs], ds)
                dqt_ref[h, :, qs] += dot(ktb, ds)
            dkv_ref[seg, hs, cols] = dk.astype(BF)
            dkv_ref[seg, PAIR + h * 64:PAIR + (h + 1) * 64, cols] = dv.astype(BF)

    first = len_ref[0] // BKB

    @pl.loop(0, first + len_ref[1] // BKB)
    def _(t):
        seg = jnp.where(t < first, 0, 1)
        step(seg, t - seg * first, None)

    @pl.loop(0, 2)
    def _(seg):
        full = len_ref[seg] // BKB
        rest = len_ref[seg] - full * BKB

        @pl.when(rest > 0)
        def _():
            step(seg, full, rest)

        @pl.loop(full + jnp.where(rest > 0, 1, 0), blocks)
        def _(j):
            cols = pl.ds(pl.multiple_of(j * BKB, BKB), BKB)
            dkv_ref[seg, :, cols] = jnp.zeros((2 * PAIR, BKB), BF)


def attention_backward(lens, qt, dot_t, lse, delta, k, v, kt, pair0):
    nq = qt.shape[1]
    rows = k.shape[0]
    off = pair0
    across = pl.BlockSpec((PAIR, nq), lambda p, s: (off, 0))
    stat = pl.BlockSpec((2, 1, nq), lambda p, s: (off, 0, 0))
    keys = pl.BlockSpec((rows, PAIR), lambda p, s: (0, off))
    keys_t = pl.BlockSpec((PAIR, rows), lambda p, s: (off, 0))
    spec = pltpu.PrefetchScalarGridSpec(
        num_scalar_prefetch=1,
        grid=(1,),
        in_specs=[across, across, stat, stat, keys, keys, keys_t],
        out_specs=[pl.BlockSpec((2, 2 * PAIR, rows // 2), lambda p, s: (0, 0, 0)),
                   pl.BlockSpec((2, 64, nq), lambda p, s: (0, 0, 0))],
        scratch_shapes=[pltpu.VMEM((2, PAIR, nq), BF), pltpu.VMEM((2, PAIR, nq), BF)])
    work = 2 * nq * rows
    return pl.pallas_call(
        bwd_kernel,
        out_shape=[jax.ShapeDtypeStruct((2, 2 * PAIR, rows // 2), BF), jax.ShapeDtypeStruct((2, 64, nq), F32)],
        grid_spec=spec,
        compiler_params=pltpu.CompilerParams(vmem_limit_bytes=40 << 20),
        cost_estimate=cost(work * 2000, 8 << 20, work),
        name="attn_bwd",
    )(lens, qt, dot_t, lse, delta, k, v, kt)


def mlp_kernel(h_ref, g_ref, gain_ref, w1_ref, w3_ref, w2_ref,
               n2t_ref, gt_ref, dgate_ref, dup_ref, ut_ref, dh_ref, dhb_ref, gn_ref, n2_ref, acc_ref):
    step = pl.program_id(0)
    rows = h_ref.shape[0]
    chunk = 512

    @pl.when(step == 0)
    def _():
        for c in range(rows // chunk):
            rs = slice(c * chunk, (c + 1) * chunk)
            hid = h_ref[rs, :].astype(F32)
            n2 = (hid * inv_rms(hid) * gain_ref[...]).astype(BF)
            n2_ref[rs, :] = n2
            n2t_ref[:, rs] = n2.T
            gt_ref[rs, :] = g_ref[rs, :].astype(BF)
        acc_ref[...] = jnp.zeros(acc_ref.shape, F32)

    w1, w3, w2 = w1_ref[...], w3_ref[...], w2_ref[...]
    for c in range(rows // chunk):
        rs = slice(c * chunk, (c + 1) * chunk)
        n2 = n2_ref[rs, :]
        gate = dot(n2, w1)
        up = dot(n2, w3)
        ga = dot_nt(gt_ref[rs, :], w2)
        sig = 1.0 / (1.0 + jnp.exp(-gate))
        act = gate * sig
        ut_ref[:, rs] = (act * up).astype(BF).T
        dup = (ga * act).astype(BF)
        dgate = (ga * up * (sig + act * (1.0 - sig))).astype(BF)
        dup_ref[rs, :] = dup
        dgate_ref[rs, :] = dgate
        acc_ref[rs, :] += dot_nt(dgate, w1) + dot_nt(dup, w3)

    @pl.when(step == pl.num_programs(0) - 1)
    def _():
        total = jnp.zeros(gn_ref.shape, F32)
        for c in range(rows // chunk):
            rs = slice(c * chunk, (c + 1) * chunk)
            hid = h_ref[rs, :].astype(F32)
            inv = inv_rms(hid)
            unit = hid * inv
            grad = acc_ref[rs, :]
            total += jnp.sum(grad * unit, axis=0, keepdims=True)
            dh = g_ref[rs, :] + norm_back(unit, inv, gain_ref[...], grad)
            dh_ref[rs, :] = dh
            dhb_ref[rs, :] = dh.astype(BF)
        gn_ref[...] = total


def mlp(hidden, g_all, gain, w_gate, w_up, w_down):
    rows, dim = hidden.shape
    ff = w_gate.shape[1]
    fix = lambda *shape: pl.BlockSpec(shape, lambda i: (0,) * len(shape))
    wide = pl.BlockSpec((dim, FFB), lambda i: (0, i))
    tall = pl.BlockSpec((FFB, dim), lambda i: (i, 0))
    act = pl.BlockSpec((rows, FFB), lambda i: (0, i))
    act_t = pl.BlockSpec((FFB, rows), lambda i: (i, 0))
    return pl.pallas_call(
        mlp_kernel,
        grid=(ff // FFB,),
        in_specs=[fix(rows, dim), fix(rows, dim), fix(1, dim), wide, wide, tall],
        out_specs=[fix(dim, rows), fix(rows, dim), act, act, act_t, fix(rows, dim), fix(rows, dim), fix(1, dim)],
        out_shape=[jax.ShapeDtypeStruct((dim, rows), BF), jax.ShapeDtypeStruct((rows, dim), BF),
                   jax.ShapeDtypeStruct((rows, ff), BF), jax.ShapeDtypeStruct((rows, ff), BF),
                   jax.ShapeDtypeStruct((ff, rows), BF), jax.ShapeDtypeStruct((rows, dim), F32),
                   jax.ShapeDtypeStruct((rows, dim), BF), jax.ShapeDtypeStruct((1, dim), F32)],
        scratch_shapes=[pltpu.VMEM((rows, dim), BF), pltpu.VMEM((rows, dim), F32)],
        compiler_params=pltpu.CompilerParams(vmem_limit_bytes=56 << 20),
        cost_estimate=cost(10 * rows * dim * ff, 40 << 20, rows * ff),
        name="mlp",
    )(hidden, g_all, gain, w_gate, w_up, w_down)


def mlp_weights_kernel(n2t_ref, gt_ref, dgate_ref, dup_ref, ut_ref, g1_ref, g3_ref, g2_ref):
    g1_ref[...] = dot(n2t_ref[...], dgate_ref[...])
    g3_ref[...] = dot(n2t_ref[...], dup_ref[...])
    g2_ref[...] = dot(ut_ref[...], gt_ref[...])


def mlp_weights(n2t, g_top, d_gate, d_up, act_t):
    dim, rows = n2t.shape
    ff = d_gate.shape[1]
    fix = lambda *shape: pl.BlockSpec(shape, lambda i: (0,) * len(shape))
    act = pl.BlockSpec((rows, FFB), lambda i: (0, i))
    wide = pl.BlockSpec((dim, FFB), lambda i: (0, i))
    return pl.pallas_call(
        mlp_weights_kernel,
        grid=(ff // FFB,),
        in_specs=[fix(dim, rows), fix(rows, dim), act, act, pl.BlockSpec((FFB, rows), lambda i: (i, 0))],
        out_specs=[wide, wide, pl.BlockSpec((FFB, dim), lambda i: (i, 0))],
        out_shape=[jax.ShapeDtypeStruct((dim, ff), F32)] * 2 + [jax.ShapeDtypeStruct((ff, dim), F32)],
        compiler_params=pltpu.CompilerParams(vmem_limit_bytes=32 << 20),
        cost_estimate=cost(6 * rows * dim * ff, 50 << 20),
        name="mlp_weights",
    )(n2t, g_top, d_gate, d_up, act_t)


def memory_kernel(core_ref, a0_ref, a1_ref, a2_ref, b0_ref, b1_ref, b2_ref, wk_ref, wv_ref, o_ref):
    core = core_ref[0]
    total = None
    for who, refs in ((core, (a0_ref, a1_ref, a2_ref)), (1 - core, (b0_ref, b1_ref, b2_ref))):
        for i, ref in enumerate(refs):
            rows = pl.ds(pl.multiple_of((who * 3 + i) * PAIR, PAIR), PAIR)
            both = ref[...].T
            part = dot(both[:, :PAIR], wk_ref[rows, :]) + dot(both[:, PAIR:], wv_ref[rows, :])
            total = part if total is None else total + part
    o_ref[...] = total


def memory_grad(core, mine, near, wkt, wvt):
    rows = mine[0].shape[-1]
    dim = wkt.shape[1]
    block = pl.BlockSpec((None, 2 * PAIR, MB), lambda i, s: (0, 0, i))
    block2 = pl.BlockSpec((2 * PAIR, MB), lambda i, s: (0, i))
    whole = pl.BlockSpec(wkt.shape, lambda i, s: (0, 0))
    return pl.pallas_call(
        memory_kernel,
        out_shape=jax.ShapeDtypeStruct((rows, dim), F32),
        grid_spec=pltpu.PrefetchScalarGridSpec(
            num_scalar_prefetch=1, grid=(rows // MB,),
            in_specs=[block] * 3 + [block2] * 3 + [whole, whole],
            out_specs=pl.BlockSpec((MB, dim), lambda i, s: (i, 0))),
        compiler_params=pltpu.CompilerParams(vmem_limit_bytes=32 << 20),
        cost_estimate=cost(4 * rows * dim * dim, 16 << 20),
        name="memory_grad",
    )(core, *mine, *near, wkt, wvt)


def inv_rms(tensor):
    return lax.rsqrt(jnp.mean(tensor * tensor, axis=-1, keepdims=True) + 1e-6)


def norm_back(unit, inv, gain, grad):
    scaled = grad * gain
    return inv * (scaled - unit * jnp.mean(scaled * unit, axis=-1, keepdims=True))


def mm(a, b, ca, cb, dtype=F32):
    out = lax.dot_general(a, b, (((ca,), (cb,)), ((), ())), preferred_element_type=F32)
    return out if dtype == F32 else out.astype(dtype)


def solution(mesh):
    n = mesh.shape['seq']
    near = [(i, i ^ 1) for i in range(n)]
    far = [(i, i ^ 2) for i in range(n)]
    row_spec = P(('data', 'seq'), None)
    weight_spec = P()
    part_vec = P('data')
    part_mat = P('data', None)
    part_cube = P('data', None, None)

    def to_near(a):
        return lax.ppermute(a, 'seq', near)

    def to_far(a):
        return lax.ppermute(a, 'seq', far)

    def device_step(dec_in, memory, mem_len, grad_out, norm_attn, wq, wk, wv, wo, norm_mlp, w_gate, w_up, w_down):
        rows, dim = dec_in.shape
        m_rows = memory.shape[0]
        heads, head = wq.shape[1], wq.shape[2]
        mine = heads // 2
        width = mine * head
        dev = lax.axis_index('seq')
        core = lax.rem(dev, 2)
        core1 = core.reshape(1).astype(jnp.int32)
        wqt, wkt, wvt = (w.transpose(1, 2, 0).reshape(heads * head, dim) for w in (wq, wk, wv))
        wo2 = wo.reshape(heads * head, dim)
        lens = jnp.stack([jnp.clip(mem_len[0] - i * m_rows, 0, m_rows) for i in (dev, dev ^ 1)]).astype(jnp.int32)
        place = jnp.stack([dev, dev ^ 1, dev ^ 2, dev ^ 3, core]).astype(jnp.int32)
        gain1 = norm_attn.astype(F32).reshape(1, dim)
        gain2 = norm_mlp.astype(F32).reshape(1, dim)

        def gather_parts(a):
            across = to_far(a)
            return a, to_near(a), across, to_near(across)

        x_parts = gather_parts(dec_in)
        mem_near = to_near(memory)
        g_parts = gather_parts(grad_out)

        first = project(core1, memory, wkt, wvt, 0, ())
        x_all_b, n1, q_s, qt_s = queries(place, x_parts, gain1, wqt)
        k, v, kt, vt = project(core1, mem_near, wkt, wvt, 1, first)

        pairs = mine // 2
        outs, lses = [], []
        parts = []
        for pair in range(pairs):
            part = attention_forward(lens, qt_s, k, vt, pair, 1)
            parts.append((part, to_far(part)))
        for a, b in parts:
            ma, mb = a[:, 64:65], b[:, 64:65]
            top = jnp.maximum(ma, mb)
            ea, eb = jnp.exp(ma - top), jnp.exp(mb - top)
            den = a[:, 65:66] * ea + b[:, 65:66] * eb
            outs.append((a[:, :64] * ea + b[:, :64] * eb) / den)
            lses.append(top + jnp.log(den))
        g_all = place_rows(place, g_parts)
        o_t = jnp.concatenate(outs, axis=0)
        lse = jnp.concatenate(lses, axis=0)
        o_t_b = o_t.astype(BF).reshape(width, n * rows)
        o_t_near = to_near(o_t_b)

        def half_rows(w, who):
            return lax.dynamic_slice(w, (who * width, 0), (width, dim))

        wo_m, wo_n = half_rows(wo2, core), half_rows(wo2, 1 - core)
        x_all = x_all_b.astype(F32)
        hidden = (x_all + mm(o_t_b, wo_m, 0, 0) + mm(o_t_near, wo_n, 0, 0)).astype(BF)

        n2t, g_top, d_gate, d_up, act_t, d_hid, d_hid_b, g_norm_mlp = mlp(hidden, g_all, gain2, w_gate, w_up, w_down)

        do_t_f = mm(wo_m, d_hid_b, 1, 1)
        delta = jnp.sum(do_t_f.reshape(mine, head, n * rows) * o_t, axis=1, keepdims=True)
        do_t = do_t_f.astype(BF)
        dkvs, dkvs_near, dqs, dws = [], [], [], []
        lens_now = lens
        for pair in range(pairs):
            dkv, dqt = attention_backward(lens_now, qt_s, do_t, lse, delta, k, v, kt, pair)
            dqs.append((dqt, to_far(dqt)))
            dw = mm(dkv[0], memory, 1, 0) + mm(dkv[1], mem_near, 1, 0)
            dws.append((dw, to_far(dw)))
            dkvs.append(dkv)
            dkvs_near.append(to_near(dkv[1]))
            lens_now, dw_last = lax.optimization_barrier((lens, dw))

        d_gate, _ = lax.optimization_barrier((d_gate, dw_last))
        g_gate, g_up, g_down = mlp_weights(n2t, g_top, d_gate, d_up, act_t)
        g_mem = memory_grad(core1, dkvs, dkvs_near, wkt, wvt)

        def both_cores(mine_half, near_half):
            return jnp.concatenate([jnp.where(core == 0, mine_half, near_half),
                                    jnp.where(core == 0, near_half, mine_half)], axis=0)

        def as_weight(rows_by_dim):
            return rows_by_dim.reshape(heads, head, dim).transpose(2, 0, 1)

        dqt_b = (jnp.concatenate([a + b for a, b in dqs], axis=0) * (head ** -0.5)).astype(BF).reshape(width, n * rows)
        dqt_near = to_near(dqt_b)
        g_wq = as_weight(both_cores(mm(dqt_b, n1, 1, 0), mm(dqt_near, n1, 1, 0)))
        d_n1 = mm(dqt_b, half_rows(wqt, core), 0, 0) + mm(dqt_near, half_rows(wqt, 1 - core), 0, 0)
        inv1 = inv_rms(x_all)
        unit1 = x_all * inv1
        g_norm_attn = jnp.sum(d_n1 * unit1, axis=0)

        def own(a):
            return lax.dynamic_slice(a, (dev * rows, 0), (rows, a.shape[1]))

        g_dec = own(d_hid) + norm_back(own(unit1), own(inv1), gain1, own(d_n1))

        dw_m = jnp.stack([a + b for a, b in dws])
        dw_n = to_near(dw_m)
        g_wk = as_weight(both_cores(dw_m[:, :PAIR].reshape(width, dim), dw_n[:, :PAIR].reshape(width, dim)))
        g_wv = as_weight(both_cores(dw_m[:, PAIR:].reshape(width, dim), dw_n[:, PAIR:].reshape(width, dim)))
        g_wo = both_cores(mm(o_t_b, d_hid_b, 1, 0), mm(o_t_near, d_hid_b, 1, 0)).reshape(heads, head, dim)
        return (g_dec, g_mem, g_norm_attn, g_wq, g_wk, g_wv, g_wo, g_norm_mlp.reshape(dim), g_gate, g_up, g_down)

    return jax.shard_map(device_step, mesh=mesh,
                         in_specs=(row_spec, row_spec, part_vec, row_spec) + (weight_spec,) * 9,
                         out_specs=(row_spec, row_spec, part_vec, part_cube, part_cube, part_cube, part_cube,
                                    part_vec, part_mat, part_mat, part_mat),
                         check_vma=False)
```

```python
import jax
import jax.numpy as jnp
from jax import lax
from jax.experimental import pallas as pl
from jax.experimental.pallas import tpu as pltpu
from jax.sharding import PartitionSpec as P


LOG2E = 1.4426950408889634
NEG = -1e30
BF = jnp.bfloat16
F32 = jnp.float32
FKB = 512
FQB = 512
BKB = 512
BQB = 256
PAIR = 128
OROWS = 72
FFB = 512
MB = 512


def dot(a, b):
    return jnp.dot(a, b, preferred_element_type=F32)


def dot_nt(a, b):
    return lax.dot_general(a, b, (((1,), (1,)), ((), ())), preferred_element_type=F32)


def cost(flops, bytes_accessed, exps=0):
    return pl.CostEstimate(flops=int(flops), bytes_accessed=int(bytes_accessed), transcendentals=int(exps))


def proj_kernel(core_ref, m_ref, wk_ref, wv_ref, *refs):
    k_ref, v_ref, kt_ref, vt_ref = refs[-4:]
    m = m_ref[...]
    k = dot_nt(m, wk_ref[...]).astype(BF)
    v = dot_nt(m, wv_ref[...]).astype(BF)
    k_ref[...] = k
    v_ref[...] = v
    kt_ref[...] = k.T
    vt_ref[...] = v.T


def project(core, mem, wkt, wvt, seg, before):
    rows, dim = mem.shape
    width = wkt.shape[0] // 2
    steps = rows // MB
    base = seg * steps
    weights = pl.BlockSpec((width, dim), lambda i, s: (s[0], 0))
    down = pl.BlockSpec((MB, width), lambda i, s: (base + i, 0))
    across = pl.BlockSpec((width, MB), lambda i, s: (0, base + i))
    outs = [jax.ShapeDtypeStruct((2 * rows, width), BF)] * 2 + [jax.ShapeDtypeStruct((width, 2 * rows), BF)] * 2
    return pl.pallas_call(
        proj_kernel,
        out_shape=outs,
        grid_spec=pltpu.PrefetchScalarGridSpec(
            num_scalar_prefetch=1, grid=(steps,),
            in_specs=[pl.BlockSpec((MB, dim), lambda i, s: (i, 0)), weights, weights]
                     + [pl.BlockSpec(memory_space=pl.ANY)] * len(before),
            out_specs=[down, down, across, across]),
        input_output_aliases={4 + i: i for i in range(len(before))},
        compiler_params=pltpu.CompilerParams(vmem_limit_bytes=60 << 20),
        cost_estimate=cost(4 * rows * dim * width, 12 << 20),
        name="kv_proj",
    )(core, mem, wkt, wvt, *before)


def query_kernel(place_ref, x0_ref, x1_ref, x2_ref, x3_ref, gain_ref, wq_ref, x_ref, n_ref, q_ref, qt_ref):
    for part, src in enumerate((x0_ref, x1_ref, x2_ref, x3_ref)):
        @pl.when(pl.program_id(0) == part)
        def _():
            xb = src[...]
            x = xb.astype(F32)
            n1 = (x * inv_rms(x) * gain_ref[...]).astype(BF)
            q = dot_nt(n1, wq_ref[...]).astype(BF) * jnp.asarray(0.125, BF)
            x_ref[...] = xb
            n_ref[...] = n1
            q_ref[...] = q
            qt_ref[...] = q.T


def queries(place, parts, gain, wqt):
    rows, dim = parts[0].shape
    width = wqt.shape[0] // 2
    n = len(parts)
    whole = pl.BlockSpec((rows, dim), lambda i, s: (0, 0))
    put = pl.BlockSpec((rows, dim), lambda i, s: (s[i], 0))
    return pl.pallas_call(
        query_kernel,
        out_shape=[jax.ShapeDtypeStruct((n * rows, dim), BF)] * 2
                  + [jax.ShapeDtypeStruct((n * rows, width), BF), jax.ShapeDtypeStruct((width, n * rows), BF)],
        grid_spec=pltpu.PrefetchScalarGridSpec(
            num_scalar_prefetch=1, grid=(n,),
            in_specs=[whole] * n + [pl.BlockSpec((1, dim), lambda i, s: (0, 0)),
                                    pl.BlockSpec((width, dim), lambda i, s: (s[n], 0))],
            out_specs=[put, put, pl.BlockSpec((rows, width), lambda i, s: (s[i], 0)),
                       pl.BlockSpec((width, rows), lambda i, s: (0, s[i]))]),
        compiler_params=pltpu.CompilerParams(vmem_limit_bytes=24 << 20),
        cost_estimate=cost(2 * n * rows * dim * width, 6 << 20),
        name="queries",
    )(place, *parts, gain, wqt)


def place_kernel(place_ref, x0_ref, x1_ref, x2_ref, x3_ref, o_ref):
    for part, src in enumerate((x0_ref, x1_ref, x2_ref, x3_ref)):
        @pl.when(pl.program_id(0) == part)
        def _():
            o_ref[...] = src[...]


def place_rows(place, parts):
    rows, dim = parts[0].shape
    n = len(parts)
    return pl.pallas_call(
        place_kernel,
        out_shape=jax.ShapeDtypeStruct((n * rows, dim), parts[0].dtype),
        grid_spec=pltpu.PrefetchScalarGridSpec(
            num_scalar_prefetch=1, grid=(n,),
            in_specs=[pl.BlockSpec((rows, dim), lambda i, s: (0, 0))] * n,
            out_specs=pl.BlockSpec((rows, dim), lambda i, s: (s[i], 0))),
        compiler_params=pltpu.CompilerParams(vmem_limit_bytes=16 << 20),
        cost_estimate=cost(n * rows * dim, 6 << 20),
        name="place_rows",
    )(place, *parts)


def fwd_kernel(len_ref, qt_ref, k_ref, vt_ref, o_ref, m_ref, l_ref, acc_ref, qz_ref, sa_ref, sb_ref):
    qb = qt_ref.shape[1]
    seg_rows = k_ref.shape[0] // 2
    half = lax.broadcasted_iota(jnp.int32, (PAIR, qb), 0) // 64
    for h in range(2):
        qz_ref[h] = jnp.where(half == h, qt_ref[...], jnp.zeros((), BF))
    m_ref[...] = jnp.full(m_ref.shape, NEG, F32)
    l_ref[...] = jnp.zeros(l_ref.shape, F32)
    acc_ref[...] = jnp.zeros(acc_ref.shape, F32)
    first = len_ref[0] // FKB
    total = first + len_ref[1] // FKB

    def base(t):
        t = jnp.clip(t, 0, jnp.maximum(total - 1, 0))
        return pl.multiple_of(jnp.where(t < first, t * FKB, seg_rows + (t - first) * FKB), FKB)

    def scores(row, s_ref):
        kb = k_ref[pl.ds(row, FKB), :]
        for h in range(2):
            s_ref[h] = dot(kb, qz_ref[h])

    def absorb(row, s_ref, count=None):
        rows = pl.ds(row, FKB)
        for h in range(2):
            st = s_ref[h]
            if count is not None:
                st = jnp.where(lax.broadcasted_iota(jnp.int32, st.shape, 0) < count, st, NEG)
            m_old = m_ref[h]
            m_new = jnp.maximum(m_old, jnp.max(st, axis=0, keepdims=True))
            p = jnp.exp2((st - m_new) * LOG2E)
            alpha = jnp.exp2((m_old - m_new) * LOG2E)
            l_ref[h] = l_ref[h] * alpha + jnp.sum(p, axis=0, keepdims=True)
            pv = dot(vt_ref[h * 64:(h + 1) * 64, rows], p.astype(BF))
            acc_ref[h] = acc_ref[h] * alpha + pv
            m_ref[h] = m_new

    scores(base(0), sa_ref)

    @pl.loop(0, total // 2)
    def _(i):
        scores(base(2 * i + 1), sb_ref)
        absorb(base(2 * i), sa_ref)
        scores(base(2 * i + 2), sa_ref)
        absorb(base(2 * i + 1), sb_ref)

    @pl.when(total % 2 == 1)
    def _():
        absorb(base(total - 1), sa_ref)

    @pl.loop(0, 2)
    def _(s):
        full = len_ref[s] // FKB
        rest = len_ref[s] - full * FKB

        @pl.when(rest > 0)
        def _():
            row = pl.multiple_of(s * seg_rows + full * FKB, FKB)
            scores(row, sa_ref)
            absorb(row, sa_ref, rest)

    for h in range(2):
        o_ref[h, 0:64, :] = acc_ref[h]
        o_ref[h, 64:72, :] = jnp.concatenate([m_ref[h], l_ref[h], jnp.zeros((6, qb), F32)], axis=0)


def attention_forward(lens, qt, k, vt, pair0, pairs):
    nq = qt.shape[1]
    rows = k.shape[0]
    off = pair0
    spec = pltpu.PrefetchScalarGridSpec(
        num_scalar_prefetch=1,
        grid=(pairs, nq // FQB),
        in_specs=[
            pl.BlockSpec((PAIR, FQB), lambda p, i, s: (p + off, i)),
            pl.BlockSpec((rows, PAIR), lambda p, i, s: (0, p + off)),
            pl.BlockSpec((PAIR, rows), lambda p, i, s: (p + off, 0)),
        ],
        out_specs=pl.BlockSpec((2, OROWS, FQB), lambda p, i, s: (p, 0, i)),
        scratch_shapes=[
            pltpu.VMEM((2, 1, FQB), F32), pltpu.VMEM((2, 1, FQB), F32), pltpu.VMEM((2, 64, FQB), F32),
            pltpu.VMEM((2, PAIR, FQB), BF), pltpu.VMEM((2, FKB, FQB), F32), pltpu.VMEM((2, FKB, FQB), F32),
        ])
    work = 2 * pairs * nq * rows
    return pl.pallas_call(
        fwd_kernel,
        out_shape=jax.ShapeDtypeStruct((2 * pairs, OROWS, nq), F32),
        grid_spec=spec,
        compiler_params=pltpu.CompilerParams(vmem_limit_bytes=24 << 20),
        cost_estimate=cost(work * 1024, 4 << 20, work),
        name="attn_fwd",
    )(lens, qt, k, vt)


def bwd_kernel(len_ref, qt_ref, dot_ref, lse_ref, dl_ref, k_ref, v_ref, kt_ref, dkv_ref, dqt_ref, qzt_ref, dozt_ref):
    nq = qt_ref.shape[1]
    seg_rows = k_ref.shape[0] // 2
    blocks = seg_rows // BKB
    half = lax.broadcasted_iota(jnp.int32, (PAIR, nq), 0) // 64
    zero = jnp.zeros((), BF)
    for h in range(2):
        qzt_ref[h] = jnp.where(half == h, qt_ref[...], zero)
        dozt_ref[h] = jnp.where(half == h, dot_ref[...], zero)
    dqt_ref[...] = jnp.zeros(dqt_ref.shape, F32)

    def step(seg, j, count):
        cols = pl.ds(pl.multiple_of(j * BKB, BKB), BKB)
        allc = pl.ds(pl.multiple_of(seg * seg_rows + j * BKB, BKB), BKB)
        kb, vb = k_ref[allc, :], v_ref[allc, :]
        for h in range(2):
            hs = slice(h * 64, (h + 1) * 64)
            ktb = kt_ref[hs, allc]
            dk = jnp.zeros((64, BKB), F32)
            dv = jnp.zeros((64, BKB), F32)
            for c in range(nq // BQB):
                qs = slice(c * BQB, (c + 1) * BQB)
                st = dot(kb, qzt_ref[h, :, qs])
                p = jnp.exp2((st - lse_ref[h, :, qs]) * LOG2E)
                if count is not None:
                    p = jnp.where(lax.broadcasted_iota(jnp.int32, st.shape, 0) < count, p, 0.0)
                dp = dot(vb, dozt_ref[h, :, qs])
                ds = (p * (dp - dl_ref[h, :, qs])).astype(BF)
                dv = dv + dot_nt(dot_ref[hs, qs], p.astype(BF))
                dk = dk + dot_nt(qt_ref[hs, qs], ds)
                dqt_ref[h, :, qs] += dot(ktb, ds)
            dkv_ref[seg, hs, cols] = dk.astype(BF)
            dkv_ref[seg, PAIR + h * 64:PAIR + (h + 1) * 64, cols] = dv.astype(BF)

    first = len_ref[0] // BKB

    @pl.loop(0, first + len_ref[1] // BKB)
    def _(t):
        seg = jnp.where(t < first, 0, 1)
        step(seg, t - seg * first, None)

    @pl.loop(0, 2)
    def _(seg):
        full = len_ref[seg] // BKB
        rest = len_ref[seg] - full * BKB

        @pl.when(rest > 0)
        def _():
            step(seg, full, rest)

        @pl.loop(full + jnp.where(rest > 0, 1, 0), blocks)
        def _(j):
            cols = pl.ds(pl.multiple_of(j * BKB, BKB), BKB)
            dkv_ref[seg, :, cols] = jnp.zeros((2 * PAIR, BKB), BF)


def attention_backward(lens, qt, dot_t, lse, delta, k, v, kt, pair0):
    nq = qt.shape[1]
    rows = k.shape[0]
    off = pair0
    across = pl.BlockSpec((PAIR, nq), lambda p, s: (off, 0))
    stat = pl.BlockSpec((2, 1, nq), lambda p, s: (off, 0, 0))
    keys = pl.BlockSpec((rows, PAIR), lambda p, s: (0, off))
    keys_t = pl.BlockSpec((PAIR, rows), lambda p, s: (off, 0))
    spec = pltpu.PrefetchScalarGridSpec(
        num_scalar_prefetch=1,
        grid=(1,),
        in_specs=[across, across, stat, stat, keys, keys, keys_t],
        out_specs=[pl.BlockSpec((2, 2 * PAIR, rows // 2), lambda p, s: (0, 0, 0)),
                   pl.BlockSpec((2, 64, nq), lambda p, s: (0, 0, 0))],
        scratch_shapes=[pltpu.VMEM((2, PAIR, nq), BF), pltpu.VMEM((2, PAIR, nq), BF)])
    work = 2 * nq * rows
    return pl.pallas_call(
        bwd_kernel,
        out_shape=[jax.ShapeDtypeStruct((2, 2 * PAIR, rows // 2), BF), jax.ShapeDtypeStruct((2, 64, nq), F32)],
        grid_spec=spec,
        compiler_params=pltpu.CompilerParams(vmem_limit_bytes=40 << 20),
        cost_estimate=cost(work * 2000, 8 << 20, work),
        name="attn_bwd",
    )(lens, qt, dot_t, lse, delta, k, v, kt)


def mlp_kernel(h_ref, g_ref, gain_ref, w1_ref, w3_ref, w2_ref,
               n2t_ref, gt_ref, dgate_ref, dup_ref, ut_ref, dh_ref, dhb_ref, gn_ref, n2_ref, acc_ref):
    step = pl.program_id(0)
    rows = h_ref.shape[0]
    chunk = 512

    @pl.when(step == 0)
    def _():
        for c in range(rows // chunk):
            rs = slice(c * chunk, (c + 1) * chunk)
            hid = h_ref[rs, :].astype(F32)
            n2 = (hid * inv_rms(hid) * gain_ref[...]).astype(BF)
            n2_ref[rs, :] = n2
            n2t_ref[:, rs] = n2.T
            gt_ref[rs, :] = g_ref[rs, :].astype(BF)
        acc_ref[...] = jnp.zeros(acc_ref.shape, F32)

    w1, w3, w2 = w1_ref[...], w3_ref[...], w2_ref[...]
    for c in range(rows // chunk):
        rs = slice(c * chunk, (c + 1) * chunk)
        n2 = n2_ref[rs, :]
        gate = dot(n2, w1)
        up = dot(n2, w3)
        ga = dot_nt(gt_ref[rs, :], w2)
        sig = 0.5 * jnp.tanh(0.5 * gate) + 0.5
        act = gate * sig
        ut_ref[:, rs] = (act * up).astype(BF).T
        dup = (ga * act).astype(BF)
        dgate = (ga * up * (sig + act * (1.0 - sig))).astype(BF)
        dup_ref[rs, :] = dup
        dgate_ref[rs, :] = dgate
        acc_ref[rs, :] += dot_nt(dgate, w1) + dot_nt(dup, w3)

    @pl.when(step == pl.num_programs(0) - 1)
    def _():
        total = jnp.zeros(gn_ref.shape, F32)
        for c in range(rows // chunk):
            rs = slice(c * chunk, (c + 1) * chunk)
            hid = h_ref[rs, :].astype(F32)
            inv = inv_rms(hid)
            unit = hid * inv
            grad = acc_ref[rs, :]
            total += jnp.sum(grad * unit, axis=0, keepdims=True)
            dh = g_ref[rs, :] + norm_back(unit, inv, gain_ref[...], grad)
            dh_ref[rs, :] = dh
            dhb_ref[rs, :] = dh.astype(BF)
        gn_ref[...] = total


def mlp(hidden, g_all, gain, w_gate, w_up, w_down):
    rows, dim = hidden.shape
    ff = w_gate.shape[1]
    fix = lambda *shape: pl.BlockSpec(shape, lambda i: (0,) * len(shape))
    wide = pl.BlockSpec((dim, FFB), lambda i: (0, i))
    tall = pl.BlockSpec((FFB, dim), lambda i: (i, 0))
    act = pl.BlockSpec((rows, FFB), lambda i: (0, i))
    act_t = pl.BlockSpec((FFB, rows), lambda i: (i, 0))
    return pl.pallas_call(
        mlp_kernel,
        grid=(ff // FFB,),
        in_specs=[fix(rows, dim), fix(rows, dim), fix(1, dim), wide, wide, tall],
        out_specs=[fix(dim, rows), fix(rows, dim), act, act, act_t, fix(rows, dim), fix(rows, dim), fix(1, dim)],
        out_shape=[jax.ShapeDtypeStruct((dim, rows), BF), jax.ShapeDtypeStruct((rows, dim), BF),
                   jax.ShapeDtypeStruct((rows, ff), BF), jax.ShapeDtypeStruct((rows, ff), BF),
                   jax.ShapeDtypeStruct((ff, rows), BF), jax.ShapeDtypeStruct((rows, dim), F32),
                   jax.ShapeDtypeStruct((rows, dim), BF), jax.ShapeDtypeStruct((1, dim), F32)],
        scratch_shapes=[pltpu.VMEM((rows, dim), BF), pltpu.VMEM((rows, dim), F32)],
        compiler_params=pltpu.CompilerParams(vmem_limit_bytes=56 << 20),
        cost_estimate=cost(10 * rows * dim * ff, 40 << 20, rows * ff),
        name="mlp",
    )(hidden, g_all, gain, w_gate, w_up, w_down)


def mlp_weights_kernel(n2t_ref, gt_ref, dgate_ref, dup_ref, ut_ref, g1_ref, g3_ref, g2_ref):
    g1_ref[...] = dot(n2t_ref[...], dgate_ref[...])
    g3_ref[...] = dot(n2t_ref[...], dup_ref[...])
    g2_ref[...] = dot(ut_ref[...], gt_ref[...])


def mlp_weights(n2t, g_top, d_gate, d_up, act_t):
    dim, rows = n2t.shape
    ff = d_gate.shape[1]
    fix = lambda *shape: pl.BlockSpec(shape, lambda i: (0,) * len(shape))
    act = pl.BlockSpec((rows, FFB), lambda i: (0, i))
    wide = pl.BlockSpec((dim, FFB), lambda i: (0, i))
    return pl.pallas_call(
        mlp_weights_kernel,
        grid=(ff // FFB,),
        in_specs=[fix(dim, rows), fix(rows, dim), act, act, pl.BlockSpec((FFB, rows), lambda i: (i, 0))],
        out_specs=[wide, wide, pl.BlockSpec((FFB, dim), lambda i: (i, 0))],
        out_shape=[jax.ShapeDtypeStruct((dim, ff), F32)] * 2 + [jax.ShapeDtypeStruct((ff, dim), F32)],
        compiler_params=pltpu.CompilerParams(vmem_limit_bytes=60 << 20),
        cost_estimate=cost(6 * rows * dim * ff, 50 << 20),
        name="mlp_weights",
    )(n2t, g_top, d_gate, d_up, act_t)


def memory_kernel(core_ref, a0_ref, a1_ref, a2_ref, b0_ref, b1_ref, b2_ref, wk_ref, wv_ref, o_ref):
    core = core_ref[0]
    total = None
    for who, refs in ((core, (a0_ref, a1_ref, a2_ref)), (1 - core, (b0_ref, b1_ref, b2_ref))):
        for i, ref in enumerate(refs):
            rows = pl.ds(pl.multiple_of((who * 3 + i) * PAIR, PAIR), PAIR)
            part = dot(ref[...].T, jnp.concatenate([wk_ref[rows, :], wv_ref[rows, :]], axis=0))
            total = part if total is None else total + part
    o_ref[...] = total


def memory_grad(core, mine, near, wkt, wvt):
    rows = mine[0].shape[-1]
    dim = wkt.shape[1]
    block = pl.BlockSpec((None, 2 * PAIR, MB), lambda i, s: (0, 0, i))
    block2 = pl.BlockSpec((2 * PAIR, MB), lambda i, s: (0, i))
    whole = pl.BlockSpec(wkt.shape, lambda i, s: (0, 0))
    return pl.pallas_call(
        memory_kernel,
        out_shape=jax.ShapeDtypeStruct((rows, dim), F32),
        grid_spec=pltpu.PrefetchScalarGridSpec(
            num_scalar_prefetch=1, grid=(rows // MB,),
            in_specs=[block] * 3 + [block2] * 3 + [whole, whole],
            out_specs=pl.BlockSpec((MB, dim), lambda i, s: (i, 0))),
        compiler_params=pltpu.CompilerParams(vmem_limit_bytes=32 << 20),
        cost_estimate=cost(4 * rows * dim * dim, 16 << 20),
        name="memory_grad",
    )(core, *mine, *near, wkt, wvt)


def inv_rms(tensor):
    return lax.rsqrt(jnp.mean(tensor * tensor, axis=-1, keepdims=True) + 1e-6)


def norm_back(unit, inv, gain, grad):
    scaled = grad * gain
    return inv * (scaled - unit * jnp.mean(scaled * unit, axis=-1, keepdims=True))


def mm(a, b, ca, cb, dtype=F32):
    out = lax.dot_general(a, b, (((ca,), (cb,)), ((), ())), preferred_element_type=F32)
    return out if dtype == F32 else out.astype(dtype)


def solution(mesh):
    n = mesh.shape['seq']
    near = [(i, i ^ 1) for i in range(n)]
    far = [(i, i ^ 2) for i in range(n)]
    row_spec = P(('data', 'seq'), None)
    weight_spec = P()
    part_vec = P('data')
    part_mat = P('data', None)
    part_cube = P('data', None, None)

    def to_near(a):
        return lax.ppermute(a, 'seq', near)

    def to_far(a):
        return lax.ppermute(a, 'seq', far)

    def device_work(dec_in, memory, mem_len, grad_out, norm_attn, wq, wk, wv, wo, norm_mlp, w_gate, w_up, w_down):
        rows, dim = dec_in.shape
        m_rows = memory.shape[0]
        heads, head = wq.shape[1], wq.shape[2]
        mine = heads // 2
        width = mine * head
        dev = lax.axis_index('seq')
        core = lax.rem(dev, 2)
        core1 = core.reshape(1).astype(jnp.int32)
        wqt, wkt, wvt = (w.transpose(1, 2, 0).reshape(heads * head, dim) for w in (wq, wk, wv))
        wo2 = wo.reshape(heads * head, dim)
        lens = jnp.stack([jnp.clip(mem_len[0] - i * m_rows, 0, m_rows) for i in (dev, dev ^ 1)]).astype(jnp.int32)
        place = jnp.stack([dev, dev ^ 1, dev ^ 2, dev ^ 3, core]).astype(jnp.int32)
        gain1 = norm_attn.astype(F32).reshape(1, dim)
        gain2 = norm_mlp.astype(F32).reshape(1, dim)

        def gather_parts(a):
            across = to_far(a)
            beside = to_near(a)
            return a, beside, across, to_near(across)

        x_parts = gather_parts(dec_in)
        mem_near = to_near(memory)
        g_parts = gather_parts(grad_out)

        first = project(core1, memory, wkt, wvt, 0, ())
        x_all_b, n1, _, qt_s = queries(place, x_parts, gain1, wqt)
        k, v, kt, vt = project(core1, mem_near, wkt, wvt, 1, first)

        pairs = mine // 2
        outs, lses = [], []
        parts = []
        for pair in range(pairs):
            part = attention_forward(lens, qt_s, k, vt, pair, 1)
            parts.append((part, to_far(part)))
        for a, b in parts:
            ma, mb = a[:, 64:65], b[:, 64:65]
            top = jnp.maximum(ma, mb)
            ea, eb = jnp.exp(ma - top), jnp.exp(mb - top)
            den = a[:, 65:66] * ea + b[:, 65:66] * eb
            outs.append((a[:, :64] * ea + b[:, :64] * eb) / den)
            lses.append(top + jnp.log(den))
        g_all = place_rows(place, g_parts)
        o_t = jnp.concatenate(outs, axis=0)
        lse = jnp.concatenate(lses, axis=0)
        o_t_b = o_t.astype(BF).reshape(width, n * rows)
        o_t_near = to_near(o_t_b)

        def half_rows(w, who):
            return lax.dynamic_slice(w, (who * width, 0), (width, dim))

        wo_m, wo_n = half_rows(wo2, core), half_rows(wo2, 1 - core)
        x_all = x_all_b.astype(F32)
        hidden = (x_all + mm(o_t_b, wo_m, 0, 0) + mm(o_t_near, wo_n, 0, 0)).astype(BF)

        n2t, g_top, d_gate, d_up, act_t, d_hid, d_hid_b, g_norm_mlp = mlp(hidden, g_all, gain2, w_gate, w_up, w_down)

        do_t_f = mm(wo_m, d_hid_b, 1, 1)
        delta = jnp.sum(do_t_f.reshape(mine, head, n * rows) * o_t, axis=1, keepdims=True)
        do_t = do_t_f.astype(BF)
        dkvs, dkvs_near, dqs, dws = [], [], [], []
        lens_now = lens
        for pair in range(pairs):
            dkv, dqt = attention_backward(lens_now, qt_s, do_t, lse, delta, k, v, kt, pair)
            dqs.append((dqt, to_far(dqt)))
            dw = mm(dkv[0], memory, 1, 0) + mm(dkv[1], mem_near, 1, 0)
            dws.append((dw, to_far(dw)))
            dkvs.append(dkv)
            dkvs_near.append(to_near(dkv[1]))
            lens_now, dw_last = lax.optimization_barrier((lens, dw))

        d_gate, _ = lax.optimization_barrier((d_gate, dw_last))
        g_gate, g_up, g_down = mlp_weights(n2t, g_top, d_gate, d_up, act_t)
        g_mem = memory_grad(core1, dkvs, dkvs_near, wkt, wvt)

        def both_cores(mine_half, near_half):
            return jnp.concatenate([jnp.where(core == 0, mine_half, near_half),
                                    jnp.where(core == 0, near_half, mine_half)], axis=0)

        def as_weight(rows_by_dim):
            return rows_by_dim.reshape(heads, head, dim).transpose(2, 0, 1)

        dqt_b = (jnp.concatenate([a + b for a, b in dqs], axis=0) * (head ** -0.5)).astype(BF).reshape(width, n * rows)
        dqt_near = to_near(dqt_b)
        g_wq = as_weight(both_cores(mm(dqt_b, n1, 1, 0), mm(dqt_near, n1, 1, 0)))
        d_n1 = mm(dqt_b, half_rows(wqt, core), 0, 0) + mm(dqt_near, half_rows(wqt, 1 - core), 0, 0)
        inv1 = inv_rms(x_all)
        unit1 = x_all * inv1
        g_norm_attn = jnp.sum(d_n1 * unit1, axis=0)

        def own(a):
            return lax.dynamic_slice(a, (dev * rows, 0), (rows, a.shape[1]))

        g_dec = own(d_hid) + norm_back(own(unit1), own(inv1), gain1, own(d_n1))

        dw_m = jnp.stack([a + b for a, b in dws])
        dw_n = to_near(dw_m)
        g_wk = as_weight(both_cores(dw_m[:, :PAIR].reshape(width, dim), dw_n[:, :PAIR].reshape(width, dim)))
        g_wv = as_weight(both_cores(dw_m[:, PAIR:].reshape(width, dim), dw_n[:, PAIR:].reshape(width, dim)))
        g_wo = both_cores(mm(o_t_b, d_hid_b, 1, 0), mm(o_t_near, d_hid_b, 1, 0)).reshape(heads, head, dim)
        return (g_dec, g_mem, g_norm_attn, g_wq, g_wk, g_wv, g_wo, g_norm_mlp.reshape(dim), g_gate, g_up, g_down)


    return jax.shard_map(device_work, mesh=mesh,
                         in_specs=(row_spec, row_spec, part_vec, row_spec) + (weight_spec,) * 9,
                         out_specs=(row_spec, row_spec, part_vec, part_cube, part_cube, part_cube, part_cube,
                                    part_vec, part_mat, part_mat, part_mat),
                         check_vma=False)
```

```python
import jax
import jax.numpy as jnp
from jax import lax
from jax.experimental import pallas as pl
from jax.experimental.pallas import tpu as pltpu
from jax.sharding import PartitionSpec as P


LOG2E = 1.4426950408889634
NEG = -1e30
BF = jnp.bfloat16
F32 = jnp.float32
FKB = 512
FQB = 512
BKB = 512
BQB = 256
PAIR = 128
OROWS = 72
FFB = 512
MB = 512


def dot(a, b):
    return jnp.dot(a, b, preferred_element_type=F32)


def dot_nt(a, b):
    return lax.dot_general(a, b, (((1,), (1,)), ((), ())), preferred_element_type=F32)


def cost(flops, bytes_accessed, exps=0):
    return pl.CostEstimate(flops=int(flops), bytes_accessed=int(bytes_accessed), transcendentals=int(exps))


def proj_kernel(core_ref, m_ref, wk_ref, wv_ref, *refs):
    k_ref, v_ref, kt_ref, vt_ref = refs[-4:]
    m = m_ref[...]
    k = dot_nt(m, wk_ref[...]).astype(BF)
    v = dot_nt(m, wv_ref[...]).astype(BF)
    k_ref[...] = k
    v_ref[...] = v
    kt_ref[...] = k.T
    vt_ref[...] = v.T


def project(core, mem, wkt, wvt, seg, before):
    rows, dim = mem.shape
    width = wkt.shape[0] // 2
    steps = rows // MB
    base = seg * steps
    weights = pl.BlockSpec((width, dim), lambda i, s: (s[0], 0))
    down = pl.BlockSpec((MB, width), lambda i, s: (base + i, 0))
    across = pl.BlockSpec((width, MB), lambda i, s: (0, base + i))
    outs = [jax.ShapeDtypeStruct((2 * rows, width), BF)] * 2 + [jax.ShapeDtypeStruct((width, 2 * rows), BF)] * 2
    return pl.pallas_call(
        proj_kernel,
        out_shape=outs,
        grid_spec=pltpu.PrefetchScalarGridSpec(
            num_scalar_prefetch=1, grid=(steps,),
            in_specs=[pl.BlockSpec((MB, dim), lambda i, s: (i, 0)), weights, weights]
                     + [pl.BlockSpec(memory_space=pl.ANY)] * len(before),
            out_specs=[down, down, across, across]),
        input_output_aliases={4 + i: i for i in range(len(before))},
        compiler_params=pltpu.CompilerParams(vmem_limit_bytes=60 << 20),
        cost_estimate=cost(4 * rows * dim * width, 12 << 20),
        name="kv_proj",
    )(core, mem, wkt, wvt, *before)


def query_kernel(place_ref, x0_ref, x1_ref, x2_ref, x3_ref, gain_ref, wq_ref, x_ref, n_ref, q_ref, qt_ref):
    for part, src in enumerate((x0_ref, x1_ref, x2_ref, x3_ref)):
        @pl.when(pl.program_id(0) == part)
        def _():
            xb = src[...]
            x = xb.astype(F32)
            n1 = (x * inv_rms(x) * gain_ref[...]).astype(BF)
            q = dot_nt(n1, wq_ref[...]).astype(BF) * jnp.asarray(0.125, BF)
            x_ref[...] = xb
            n_ref[...] = n1
            q_ref[...] = q
            qt_ref[...] = q.T


def queries(place, parts, gain, wqt):
    rows, dim = parts[0].shape
    width = wqt.shape[0] // 2
    n = len(parts)
    whole = pl.BlockSpec((rows, dim), lambda i, s: (0, 0))
    put = pl.BlockSpec((rows, dim), lambda i, s: (s[i], 0))
    return pl.pallas_call(
        query_kernel,
        out_shape=[jax.ShapeDtypeStruct((n * rows, dim), BF)] * 2
                  + [jax.ShapeDtypeStruct((n * rows, width), BF), jax.ShapeDtypeStruct((width, n * rows), BF)],
        grid_spec=pltpu.PrefetchScalarGridSpec(
            num_scalar_prefetch=1, grid=(n,),
            in_specs=[whole] * n + [pl.BlockSpec((1, dim), lambda i, s: (0, 0)),
                                    pl.BlockSpec((width, dim), lambda i, s: (s[n], 0))],
            out_specs=[put, put, pl.BlockSpec((rows, width), lambda i, s: (s[i], 0)),
                       pl.BlockSpec((width, rows), lambda i, s: (0, s[i]))]),
        compiler_params=pltpu.CompilerParams(vmem_limit_bytes=24 << 20),
        cost_estimate=cost(2 * n * rows * dim * width, 6 << 20),
        name="queries",
    )(place, *parts, gain, wqt)


def place_kernel(place_ref, x0_ref, x1_ref, x2_ref, x3_ref, o_ref):
    for part, src in enumerate((x0_ref, x1_ref, x2_ref, x3_ref)):
        @pl.when(pl.program_id(0) == part)
        def _():
            o_ref[...] = src[...]


def place_rows(place, parts):
    rows, dim = parts[0].shape
    n = len(parts)
    return pl.pallas_call(
        place_kernel,
        out_shape=jax.ShapeDtypeStruct((n * rows, dim), parts[0].dtype),
        grid_spec=pltpu.PrefetchScalarGridSpec(
            num_scalar_prefetch=1, grid=(n,),
            in_specs=[pl.BlockSpec((rows, dim), lambda i, s: (0, 0))] * n,
            out_specs=pl.BlockSpec((rows, dim), lambda i, s: (s[i], 0))),
        compiler_params=pltpu.CompilerParams(vmem_limit_bytes=16 << 20),
        cost_estimate=cost(n * rows * dim, 6 << 20),
        name="place_rows",
    )(place, *parts)


def fwd_kernel(len_ref, qt_ref, k_ref, vt_ref, o_ref, m_ref, l_ref, acc_ref, qz_ref, sa_ref, sb_ref):
    qb = qt_ref.shape[1]
    seg_rows = k_ref.shape[0] // 2
    half = lax.broadcasted_iota(jnp.int32, (PAIR, qb), 0) // 64
    for h in range(2):
        qz_ref[h] = jnp.where(half == h, qt_ref[...], jnp.zeros((), BF))
    m_ref[...] = jnp.full(m_ref.shape, NEG, F32)
    l_ref[...] = jnp.zeros(l_ref.shape, F32)
    acc_ref[...] = jnp.zeros(acc_ref.shape, F32)
    first = len_ref[0] // FKB
    total = first + len_ref[1] // FKB

    def base(t):
        t = jnp.clip(t, 0, jnp.maximum(total - 1, 0))
        return pl.multiple_of(jnp.where(t < first, t * FKB, seg_rows + (t - first) * FKB), FKB)

    def scores(row, s_ref):
        kb = k_ref[pl.ds(row, FKB), :]
        for h in range(2):
            s_ref[h] = dot(kb, qz_ref[h])

    def absorb(row, s_ref, count=None):
        rows = pl.ds(row, FKB)
        for h in range(2):
            st = s_ref[h]
            if count is not None:
                st = jnp.where(lax.broadcasted_iota(jnp.int32, st.shape, 0) < count, st, NEG)
            m_old = m_ref[h]
            m_new = jnp.maximum(m_old, jnp.max(st, axis=0, keepdims=True))
            p = jnp.exp2((st - m_new) * LOG2E)
            alpha = jnp.exp2((m_old - m_new) * LOG2E)
            l_ref[h] = l_ref[h] * alpha + jnp.sum(p, axis=0, keepdims=True)
            pv = dot(vt_ref[h * 64:(h + 1) * 64, rows], p.astype(BF))
            acc_ref[h] = acc_ref[h] * alpha + pv
            m_ref[h] = m_new

    scores(base(0), sa_ref)

    @pl.loop(0, total // 2)
    def _(i):
        scores(base(2 * i + 1), sb_ref)
        absorb(base(2 * i), sa_ref)
        scores(base(2 * i + 2), sa_ref)
        absorb(base(2 * i + 1), sb_ref)

    @pl.when(total % 2 == 1)
    def _():
        absorb(base(total - 1), sa_ref)

    @pl.loop(0, 2)
    def _(s):
        full = len_ref[s] // FKB
        rest = len_ref[s] - full * FKB

        @pl.when(rest > 0)
        def _():
            row = pl.multiple_of(s * seg_rows + full * FKB, FKB)
            scores(row, sa_ref)
            absorb(row, sa_ref, rest)

    for h in range(2):
        o_ref[h, 0:64, :] = acc_ref[h]
        o_ref[h, 64:72, :] = jnp.concatenate([m_ref[h], l_ref[h], jnp.zeros((6, qb), F32)], axis=0)


def attention_forward(lens, qt, k, vt, pair0, pairs, at, nq):
    q_off = at // FQB
    rows = k.shape[0]
    off = pair0
    spec = pltpu.PrefetchScalarGridSpec(
        num_scalar_prefetch=1,
        grid=(pairs, nq // FQB),
        in_specs=[
            pl.BlockSpec((PAIR, FQB), lambda p, i, s: (p + off, i + q_off)),
            pl.BlockSpec((rows, PAIR), lambda p, i, s: (0, p + off)),
            pl.BlockSpec((PAIR, rows), lambda p, i, s: (p + off, 0)),
        ],
        out_specs=pl.BlockSpec((2, OROWS, FQB), lambda p, i, s: (p, 0, i)),
        scratch_shapes=[
            pltpu.VMEM((2, 1, FQB), F32), pltpu.VMEM((2, 1, FQB), F32), pltpu.VMEM((2, 64, FQB), F32),
            pltpu.VMEM((2, PAIR, FQB), BF), pltpu.VMEM((2, FKB, FQB), F32), pltpu.VMEM((2, FKB, FQB), F32),
        ])
    work = 2 * pairs * nq * rows
    return pl.pallas_call(
        fwd_kernel,
        out_shape=jax.ShapeDtypeStruct((2 * pairs, OROWS, nq), F32),
        grid_spec=spec,
        compiler_params=pltpu.CompilerParams(vmem_limit_bytes=60 << 20),
        cost_estimate=cost(work * 1024, 4 << 20, work),
        name="attn_fwd",
    )(lens, qt, k, vt)


def bwd_kernel(len_ref, qt_ref, dot_ref, lse_ref, dl_ref, k_ref, v_ref, kt_ref, dkv_ref, dqt_ref, qzt_ref, dozt_ref):
    nq = qt_ref.shape[1]
    seg_rows = k_ref.shape[0] // 2
    blocks = seg_rows // BKB
    half = lax.broadcasted_iota(jnp.int32, (PAIR, nq), 0) // 64
    zero = jnp.zeros((), BF)
    for h in range(2):
        qzt_ref[h] = jnp.where(half == h, qt_ref[...], zero)
        dozt_ref[h] = jnp.where(half == h, dot_ref[...], zero)
    dqt_ref[...] = jnp.zeros(dqt_ref.shape, F32)

    def step(seg, j, count):
        cols = pl.ds(pl.multiple_of(j * BKB, BKB), BKB)
        allc = pl.ds(pl.multiple_of(seg * seg_rows + j * BKB, BKB), BKB)
        kb, vb = k_ref[allc, :], v_ref[allc, :]
        for h in range(2):
            hs = slice(h * 64, (h + 1) * 64)
            ktb = kt_ref[hs, allc]
            dk = jnp.zeros((64, BKB), F32)
            dv = jnp.zeros((64, BKB), F32)
            for c in range(nq // BQB):
                qs = slice(c * BQB, (c + 1) * BQB)
                st = dot(kb, qzt_ref[h, :, qs])
                p = jnp.exp2((st - lse_ref[h, :, qs]) * LOG2E)
                if count is not None:
                    p = jnp.where(lax.broadcasted_iota(jnp.int32, st.shape, 0) < count, p, 0.0)
                dp = dot(vb, dozt_ref[h, :, qs])
                ds = (p * (dp - dl_ref[h, :, qs])).astype(BF)
                dv = dv + dot_nt(dot_ref[hs, qs], p.astype(BF))
                dk = dk + dot_nt(qt_ref[hs, qs], ds)
                dqt_ref[h, :, qs] += dot(ktb, ds)
            dkv_ref[seg, hs, cols] = dk.astype(BF)
            dkv_ref[seg, PAIR + h * 64:PAIR + (h + 1) * 64, cols] = dv.astype(BF)

    first = len_ref[0] // BKB

    @pl.loop(0, first + len_ref[1] // BKB)
    def _(t):
        seg = jnp.where(t < first, 0, 1)
        step(seg, t - seg * first, None)

    @pl.loop(0, 2)
    def _(seg):
        full = len_ref[seg] // BKB
        rest = len_ref[seg] - full * BKB

        @pl.when(rest > 0)
        def _():
            step(seg, full, rest)

        @pl.loop(full + jnp.where(rest > 0, 1, 0), blocks)
        def _(j):
            cols = pl.ds(pl.multiple_of(j * BKB, BKB), BKB)
            dkv_ref[seg, :, cols] = jnp.zeros((2 * PAIR, BKB), BF)


def attention_backward(lens, qt, dot_t, lse, delta, k, v, kt, pair0):
    nq = qt.shape[1]
    rows = k.shape[0]
    off = pair0
    across = pl.BlockSpec((PAIR, nq), lambda p, s: (off, 0))
    stat = pl.BlockSpec((2, 1, nq), lambda p, s: (off, 0, 0))
    keys = pl.BlockSpec((rows, PAIR), lambda p, s: (0, off))
    keys_t = pl.BlockSpec((PAIR, rows), lambda p, s: (off, 0))
    spec = pltpu.PrefetchScalarGridSpec(
        num_scalar_prefetch=1,
        grid=(1,),
        in_specs=[across, across, stat, stat, keys, keys, keys_t],
        out_specs=[pl.BlockSpec((2, 2 * PAIR, rows // 2), lambda p, s: (0, 0, 0)),
                   pl.BlockSpec((2, 64, nq), lambda p, s: (0, 0, 0))],
        scratch_shapes=[pltpu.VMEM((2, PAIR, nq), BF), pltpu.VMEM((2, PAIR, nq), BF)])
    work = 2 * nq * rows
    return pl.pallas_call(
        bwd_kernel,
        out_shape=[jax.ShapeDtypeStruct((2, 2 * PAIR, rows // 2), BF), jax.ShapeDtypeStruct((2, 64, nq), F32)],
        grid_spec=spec,
        compiler_params=pltpu.CompilerParams(vmem_limit_bytes=40 << 20),
        cost_estimate=cost(work * 2000, 8 << 20, work),
        name="attn_bwd",
    )(lens, qt, dot_t, lse, delta, k, v, kt)


def mlp_kernel(h_ref, g_ref, gain_ref, w1_ref, w3_ref, w2_ref,
               n2t_ref, gt_ref, dgate_ref, dup_ref, ut_ref, dh_ref, dhb_ref, gn_ref, n2_ref, acc_ref):
    step = pl.program_id(0)
    rows = h_ref.shape[0]
    chunk = 512

    @pl.when(step == 0)
    def _():
        for c in range(rows // chunk):
            rs = slice(c * chunk, (c + 1) * chunk)
            hid = h_ref[rs, :].astype(F32)
            n2 = (hid * inv_rms(hid) * gain_ref[...]).astype(BF)
            n2_ref[rs, :] = n2
            n2t_ref[:, rs] = n2.T
            gt_ref[rs, :] = g_ref[rs, :].astype(BF)
        acc_ref[...] = jnp.zeros(acc_ref.shape, F32)

    w1, w3, w2 = w1_ref[...], w3_ref[...], w2_ref[...]
    for c in range(rows // chunk):
        rs = slice(c * chunk, (c + 1) * chunk)
        n2 = n2_ref[rs, :]
        gate = dot(n2, w1)
        up = dot(n2, w3)
        ga = dot_nt(gt_ref[rs, :], w2)
        sig = 0.5 * jnp.tanh(0.5 * gate) + 0.5
        act = gate * sig
        ut_ref[:, rs] = (act * up).astype(BF).T
        dup = (ga * act).astype(BF)
        dgate = (ga * up * (sig + act * (1.0 - sig))).astype(BF)
        dup_ref[rs, :] = dup
        dgate_ref[rs, :] = dgate
        acc_ref[rs, :] += dot_nt(dgate, w1) + dot_nt(dup, w3)

    @pl.when(step == pl.num_programs(0) - 1)
    def _():
        total = jnp.zeros(gn_ref.shape, F32)
        for c in range(rows // chunk):
            rs = slice(c * chunk, (c + 1) * chunk)
            hid = h_ref[rs, :].astype(F32)
            inv = inv_rms(hid)
            unit = hid * inv
            grad = acc_ref[rs, :]
            total += jnp.sum(grad * unit, axis=0, keepdims=True)
            dh = g_ref[rs, :] + norm_back(unit, inv, gain_ref[...], grad)
            dh_ref[rs, :] = dh
            dhb_ref[rs, :] = dh.astype(BF)
        gn_ref[...] = total


def mlp(hidden, g_all, gain, w_gate, w_up, w_down):
    rows, dim = hidden.shape
    ff = w_gate.shape[1]
    fix = lambda *shape: pl.BlockSpec(shape, lambda i: (0,) * len(shape))
    wide = pl.BlockSpec((dim, FFB), lambda i: (0, i))
    tall = pl.BlockSpec((FFB, dim), lambda i: (i, 0))
    act = pl.BlockSpec((rows, FFB), lambda i: (0, i))
    act_t = pl.BlockSpec((FFB, rows), lambda i: (i, 0))
    return pl.pallas_call(
        mlp_kernel,
        grid=(ff // FFB,),
        in_specs=[fix(rows, dim), fix(rows, dim), fix(1, dim), wide, wide, tall],
        out_specs=[fix(dim, rows), fix(rows, dim), act, act, act_t, fix(rows, dim), fix(rows, dim), fix(1, dim)],
        out_shape=[jax.ShapeDtypeStruct((dim, rows), BF), jax.ShapeDtypeStruct((rows, dim), BF),
                   jax.ShapeDtypeStruct((rows, ff), BF), jax.ShapeDtypeStruct((rows, ff), BF),
                   jax.ShapeDtypeStruct((ff, rows), BF), jax.ShapeDtypeStruct((rows, dim), F32),
                   jax.ShapeDtypeStruct((rows, dim), BF), jax.ShapeDtypeStruct((1, dim), F32)],
        scratch_shapes=[pltpu.VMEM((rows, dim), BF), pltpu.VMEM((rows, dim), F32)],
        compiler_params=pltpu.CompilerParams(vmem_limit_bytes=56 << 20),
        cost_estimate=cost(10 * rows * dim * ff, 40 << 20, rows * ff),
        name="mlp",
    )(hidden, g_all, gain, w_gate, w_up, w_down)


def mlp_weights_kernel(n2t_ref, gt_ref, dgate_ref, dup_ref, ut_ref, g1_ref, g3_ref, g2_ref):
    g1_ref[...] = dot(n2t_ref[...], dgate_ref[...])
    g3_ref[...] = dot(n2t_ref[...], dup_ref[...])
    g2_ref[...] = dot(ut_ref[...], gt_ref[...])


def mlp_weights(n2t, g_top, d_gate, d_up, act_t):
    dim, rows = n2t.shape
    ff = d_gate.shape[1]
    fix = lambda *shape: pl.BlockSpec(shape, lambda i: (0,) * len(shape))
    act = pl.BlockSpec((rows, FFB), lambda i: (0, i))
    wide = pl.BlockSpec((dim, FFB), lambda i: (0, i))
    return pl.pallas_call(
        mlp_weights_kernel,
        grid=(ff // FFB,),
        in_specs=[fix(dim, rows), fix(rows, dim), act, act, pl.BlockSpec((FFB, rows), lambda i: (i, 0))],
        out_specs=[wide, wide, pl.BlockSpec((FFB, dim), lambda i: (i, 0))],
        out_shape=[jax.ShapeDtypeStruct((dim, ff), F32)] * 2 + [jax.ShapeDtypeStruct((ff, dim), F32)],
        compiler_params=pltpu.CompilerParams(vmem_limit_bytes=60 << 20),
        cost_estimate=cost(6 * rows * dim * ff, 50 << 20),
        name="mlp_weights",
    )(n2t, g_top, d_gate, d_up, act_t)


def memory_kernel(core_ref, a0_ref, a1_ref, a2_ref, b0_ref, b1_ref, b2_ref, wk_ref, wv_ref, o_ref):
    core = core_ref[0]
    total = None
    for who, refs in ((core, (a0_ref, a1_ref, a2_ref)), (1 - core, (b0_ref, b1_ref, b2_ref))):
        for i, ref in enumerate(refs):
            rows = pl.ds(pl.multiple_of((who * 3 + i) * PAIR, PAIR), PAIR)
            part = dot(ref[...].T, jnp.concatenate([wk_ref[rows, :], wv_ref[rows, :]], axis=0))
            total = part if total is None else total + part
    o_ref[...] = total


def memory_grad(core, mine, near, wkt, wvt):
    rows = mine[0].shape[-1]
    dim = wkt.shape[1]
    block = pl.BlockSpec((None, 2 * PAIR, MB), lambda i, s: (0, 0, i))
    block2 = pl.BlockSpec((2 * PAIR, MB), lambda i, s: (0, i))
    whole = pl.BlockSpec(wkt.shape, lambda i, s: (0, 0))
    return pl.pallas_call(
        memory_kernel,
        out_shape=jax.ShapeDtypeStruct((rows, dim), F32),
        grid_spec=pltpu.PrefetchScalarGridSpec(
            num_scalar_prefetch=1, grid=(rows // MB,),
            in_specs=[block] * 3 + [block2] * 3 + [whole, whole],
            out_specs=pl.BlockSpec((MB, dim), lambda i, s: (i, 0))),
        compiler_params=pltpu.CompilerParams(vmem_limit_bytes=32 << 20),
        cost_estimate=cost(4 * rows * dim * dim, 16 << 20),
        name="memory_grad",
    )(core, *mine, *near, wkt, wvt)


def half_index(i, core):
    return i + core - 2 * i * core


def out_proj_kernel(core_ref, mine_ref, near_ref, dh_ref, o_ref):
    for who, ref in enumerate((mine_ref, near_ref)):
        @pl.when(pl.program_id(0) == who)
        def _():
            o_ref[...] = dot(ref[...], dh_ref[...])


def out_proj_grad(core, mine, near, dh):
    width, rows = mine.shape
    dim = dh.shape[1]
    whole = pl.BlockSpec((width, rows), lambda i, s: (0, 0))
    return pl.pallas_call(
        out_proj_kernel,
        out_shape=jax.ShapeDtypeStruct((2 * width, dim), F32),
        grid_spec=pltpu.PrefetchScalarGridSpec(
            num_scalar_prefetch=1, grid=(2,),
            in_specs=[whole, whole, pl.BlockSpec((rows, dim), lambda i, s: (0, 0))],
            out_specs=pl.BlockSpec((width, dim), lambda i, s: (half_index(i, s[0]), 0))),
        compiler_params=pltpu.CompilerParams(vmem_limit_bytes=24 << 20),
        cost_estimate=cost(4 * rows * dim * width, 6 << 20),
        name="out_proj_grad",
    )(core, mine, near, dh)


def query_grad_kernel(place_ref, mine_ref, near_ref, n1_ref, wq_ref, x_ref, dh_ref, gain_ref,
                      gw_ref, gx_ref, gn_ref, acc_ref):
    for who, ref in enumerate((mine_ref, near_ref)):
        @pl.when(pl.program_id(0) == who)
        def _():
            dq = ref[...]
            gw_ref[...] = dot(dq, n1_ref[...])
            part = dot(dq.T, wq_ref[...])
            acc_ref[...] = part if who == 0 else acc_ref[...] + part

    @pl.when(pl.program_id(0) == 1)
    def _():
        rows = gx_ref.shape[0]
        total = jnp.zeros(gn_ref.shape, F32)
        for c in range(acc_ref.shape[0] // rows):
            rs = slice(c * rows, (c + 1) * rows)
            x = x_ref[rs, :].astype(F32)
            total += jnp.sum(acc_ref[rs, :] * (x * inv_rms(x)), axis=0, keepdims=True)
        gn_ref[...] = total
        own = pl.ds(pl.multiple_of(place_ref[0] * rows, rows), rows)
        x = x_ref[own, :].astype(F32)
        inv = inv_rms(x)
        gx_ref[...] = dh_ref[...] + norm_back(x * inv, inv, gain_ref[...], acc_ref[own, :])


def query_grad(place, mine, near, n1, wqt, x_all, d_hid, gain, rows):
    width, total = mine.shape
    dim = n1.shape[1]
    fix = lambda *shape: pl.BlockSpec(shape, lambda i, s: (0,) * len(shape))
    half = pl.BlockSpec((width, dim), lambda i, s: (half_index(i, s[4]), 0))
    return pl.pallas_call(
        query_grad_kernel,
        out_shape=[jax.ShapeDtypeStruct((2 * width, dim), F32), jax.ShapeDtypeStruct((rows, dim), F32),
                   jax.ShapeDtypeStruct((1, dim), F32)],
        grid_spec=pltpu.PrefetchScalarGridSpec(
            num_scalar_prefetch=1, grid=(2,),
            in_specs=[fix(width, total), fix(width, total), fix(total, dim), half, fix(total, dim),
                      pl.BlockSpec((rows, dim), lambda i, s: (s[0], 0)), fix(1, dim)],
            out_specs=[half, fix(rows, dim), fix(1, dim)],
            scratch_shapes=[pltpu.VMEM((total, dim), F32)]),
        compiler_params=pltpu.CompilerParams(vmem_limit_bytes=32 << 20),
        cost_estimate=cost(8 * total * dim * width, 10 << 20),
        name="query_grad",
    )(place, mine, near, n1, wqt, x_all, d_hid, gain)


def key_weights_kernel(core_ref, a0_ref, a1_ref, a2_ref, b0_ref, b1_ref, b2_ref, gk_ref, gv_ref):
    for at, ref in enumerate((a0_ref, a1_ref, a2_ref, b0_ref, b1_ref, b2_ref)):
        @pl.when(pl.program_id(0) == at)
        def _():
            gk_ref[...] = ref[:PAIR, :]
            gv_ref[...] = ref[PAIR:, :]


def key_weights(core, mine, near):
    pairs = len(mine)
    dim = mine[0].shape[1]
    out = pl.BlockSpec((PAIR, dim), lambda i, s: (half_index(i // pairs, s[0]) * pairs + i % pairs, 0))
    return pl.pallas_call(
        key_weights_kernel,
        out_shape=[jax.ShapeDtypeStruct((2 * pairs * PAIR, dim), F32)] * 2,
        grid_spec=pltpu.PrefetchScalarGridSpec(
            num_scalar_prefetch=1, grid=(2 * pairs,),
            in_specs=[pl.BlockSpec((2 * PAIR, dim), lambda i, s: (0, 0))] * (2 * pairs),
            out_specs=[out, out]),
        compiler_params=pltpu.CompilerParams(vmem_limit_bytes=24 << 20),
        cost_estimate=cost(4 * pairs * PAIR * dim, 10 << 20),
        name="key_weights",
    )(core, *mine, *near)


def inv_rms(tensor):
    return lax.rsqrt(jnp.mean(tensor * tensor, axis=-1, keepdims=True) + 1e-6)


def norm_back(unit, inv, gain, grad):
    scaled = grad * gain
    return inv * (scaled - unit * jnp.mean(scaled * unit, axis=-1, keepdims=True))


def mm(a, b, ca, cb, dtype=F32):
    out = lax.dot_general(a, b, (((ca,), (cb,)), ((), ())), preferred_element_type=F32)
    return out if dtype == F32 else out.astype(dtype)


def solution(mesh):
    n = mesh.shape['seq']
    near = [(i, i ^ 1) for i in range(n)]
    far = [(i, i ^ 2) for i in range(n)]
    row_spec = P(('data', 'seq'), None)
    weight_spec = P()
    part_vec = P('data')
    part_mat = P('data', None)
    part_cube = P('data', None, None)

    def to_near(a):
        return lax.ppermute(a, 'seq', near)

    def to_far(a):
        return lax.ppermute(a, 'seq', far)

    def device_work(dec_in, memory, mem_len, grad_out, norm_attn, wq, wk, wv, wo, norm_mlp, w_gate, w_up, w_down):
        rows, dim = dec_in.shape
        m_rows = memory.shape[0]
        heads, head = wq.shape[1], wq.shape[2]
        mine = heads // 2
        width = mine * head
        dev = lax.axis_index('seq')
        core = lax.rem(dev, 2)
        core1 = core.reshape(1).astype(jnp.int32)
        wqt, wkt, wvt = (w.transpose(1, 2, 0).reshape(heads * head, dim) for w in (wq, wk, wv))
        wo2 = wo.reshape(heads * head, dim)
        lens = jnp.stack([jnp.clip(mem_len[0] - i * m_rows, 0, m_rows) for i in (dev, dev ^ 1)]).astype(jnp.int32)
        place = jnp.stack([dev, dev ^ 1, dev ^ 2, dev ^ 3, core]).astype(jnp.int32)
        gain1 = norm_attn.astype(F32).reshape(1, dim)
        gain2 = norm_mlp.astype(F32).reshape(1, dim)

        def gather_parts(a):
            across = to_far(a)
            beside = to_near(a)
            return a, beside, across, to_near(across)

        x_parts = gather_parts(dec_in)
        mem_near = to_near(memory)
        g_parts = gather_parts(grad_out)

        first = project(core1, memory, wkt, wvt, 0, ())
        x_all_b, n1, _, qt_s = queries(place, x_parts, gain1, wqt)
        k, v, kt, vt = project(core1, mem_near, wkt, wvt, 1, first)

        pairs = mine // 2
        pieces = [(pair, 0, n * rows) for pair in range(pairs - 1)]
        pieces += [(pairs - 1, 0, n * rows // 2), (pairs - 1, n * rows // 2, n * rows // 2)]
        outs, lses = [], []
        parts = []
        for pair, at, count in pieces:
            part = attention_forward(lens, qt_s, k, vt, pair, 1, at, count)
            parts.append((part, to_far(part)))
        for a, b in parts:
            ma, mb = a[:, 64:65], b[:, 64:65]
            top = jnp.maximum(ma, mb)
            ea, eb = jnp.exp(ma - top), jnp.exp(mb - top)
            den = a[:, 65:66] * ea + b[:, 65:66] * eb
            outs.append((a[:, :64] * ea + b[:, :64] * eb) / den)
            lses.append(top + jnp.log(den))
        outs[-2:] = [jnp.concatenate(outs[-2:], axis=2)]
        lses[-2:] = [jnp.concatenate(lses[-2:], axis=2)]
        g_all = place_rows(place, g_parts)
        o_t = jnp.concatenate(outs, axis=0)
        lse = jnp.concatenate(lses, axis=0)
        o_t_b = o_t.astype(BF).reshape(width, n * rows)
        o_t_near = to_near(o_t_b)

        def half_rows(w, who):
            return lax.dynamic_slice(w, (who * width, 0), (width, dim))

        wo_m, wo_n = half_rows(wo2, core), half_rows(wo2, 1 - core)
        x_all = x_all_b.astype(F32)
        hidden = (x_all + mm(o_t_b, wo_m, 0, 0) + mm(o_t_near, wo_n, 0, 0)).astype(BF)

        n2t, g_top, d_gate, d_up, act_t, d_hid, d_hid_b, g_norm_mlp = mlp(hidden, g_all, gain2, w_gate, w_up, w_down)

        do_t_f = mm(wo_m, d_hid_b, 1, 1)
        delta = jnp.sum(do_t_f.reshape(mine, head, n * rows) * o_t, axis=1, keepdims=True)
        do_t = do_t_f.astype(BF)
        dkvs, dkvs_near, dqs, dws = [], [], [], []
        lens_now = lens
        for pair in range(pairs):
            dkv, dqt = attention_backward(lens_now, qt_s, do_t, lse, delta, k, v, kt, pair)
            dqs.append((dqt, to_far(dqt)))
            dw = mm(dkv[0], memory, 1, 0) + mm(dkv[1], mem_near, 1, 0)
            dws.append((dw, to_far(dw)))
            dkvs.append(dkv)
            dkvs_near.append(to_near(dkv[1]))
            lens_now, dw_last = lax.optimization_barrier((lens, dw))

        d_gate, _ = lax.optimization_barrier((d_gate, dw_last))
        g_gate, g_up, g_down = mlp_weights(n2t, g_top, d_gate, d_up, act_t)
        g_mem = memory_grad(core1, dkvs, dkvs_near, wkt, wvt)

        def as_weight(rows_by_dim):
            return rows_by_dim.reshape(heads, head, dim).transpose(2, 0, 1)

        g_wo = out_proj_grad(core1, o_t_b, o_t_near, d_hid_b).reshape(heads, head, dim)

        dqt_b = (jnp.concatenate([a + b for a, b in dqs], axis=0) * (head ** -0.5)).astype(BF).reshape(width, n * rows)
        dqt_near = to_near(dqt_b)
        g_wqt, g_dec, g_norm_attn = query_grad(place, dqt_b, dqt_near, n1, wqt, x_all_b, d_hid, gain1, rows)

        dw_mine, dw_near = [], []
        for a, b in dws:
            dw_mine.append(a + b)
            dw_near.append(to_near(dw_mine[-1]))
        g_wkt, g_wvt = key_weights(core1, dw_mine, dw_near)
        g_wq, g_wk, g_wv = as_weight(g_wqt), as_weight(g_wkt), as_weight(g_wvt)
        return (g_dec, g_mem, g_norm_attn.reshape(dim), g_wq, g_wk, g_wv, g_wo, g_norm_mlp.reshape(dim), g_gate, g_up, g_down)


    return jax.shard_map(device_work, mesh=mesh,
                         in_specs=(row_spec, row_spec, part_vec, row_spec) + (weight_spec,) * 9,
                         out_specs=(row_spec, row_spec, part_vec, part_cube, part_cube, part_cube, part_cube,
                                    part_vec, part_mat, part_mat, part_mat),
                         check_vma=False)
```

```python
import jax
import jax.numpy as jnp
from jax import lax
from jax.experimental import pallas as pl
from jax.experimental.pallas import tpu as pltpu
from jax.sharding import PartitionSpec as P


LOG2E = 1.4426950408889634
NEG = -1e30
BF = jnp.bfloat16
F32 = jnp.float32
FKB = 512
FQB = 512
BKB = 512
BQB = 256
PAIR = 128
OROWS = 72
FFB = 512
MB = 512


def dot(a, b):
    return jnp.dot(a, b, preferred_element_type=F32)


def dot_nt(a, b):
    return lax.dot_general(a, b, (((1,), (1,)), ((), ())), preferred_element_type=F32)


def cost(flops, bytes_accessed, exps=0):
    return pl.CostEstimate(flops=int(flops), bytes_accessed=int(bytes_accessed), transcendentals=int(exps))


def proj_kernel(core_ref, m_ref, wk_ref, wv_ref, *refs):
    k_ref, v_ref, kt_ref, vt_ref = refs[-4:]
    m = m_ref[...]
    k = dot_nt(m, wk_ref[...]).astype(BF)
    v = dot_nt(m, wv_ref[...]).astype(BF)
    k_ref[...] = k
    v_ref[...] = v
    kt_ref[...] = k.T
    vt_ref[...] = v.T


def project(core, mem, wkt, wvt, seg, before):
    rows, dim = mem.shape
    width = wkt.shape[0] // 2
    steps = rows // MB
    base = seg * steps
    weights = pl.BlockSpec((width, dim), lambda i, s: (s[0], 0))
    down = pl.BlockSpec((MB, width), lambda i, s: (base + i, 0))
    across = pl.BlockSpec((width, MB), lambda i, s: (0, base + i))
    outs = [jax.ShapeDtypeStruct((2 * rows, width), BF)] * 2 + [jax.ShapeDtypeStruct((width, 2 * rows), BF)] * 2
    return pl.pallas_call(
        proj_kernel,
        out_shape=outs,
        grid_spec=pltpu.PrefetchScalarGridSpec(
            num_scalar_prefetch=1, grid=(steps,),
            in_specs=[pl.BlockSpec((MB, dim), lambda i, s: (i, 0)), weights, weights]
                     + [pl.BlockSpec(memory_space=pl.ANY)] * len(before),
            out_specs=[down, down, across, across]),
        input_output_aliases={4 + i: i for i in range(len(before))},
        compiler_params=pltpu.CompilerParams(vmem_limit_bytes=60 << 20),
        cost_estimate=cost(4 * rows * dim * width, 12 << 20),
        name="kv_proj",
    )(core, mem, wkt, wvt, *before)


def query_kernel(place_ref, x0_ref, x1_ref, x2_ref, x3_ref, gain_ref, wq_ref, x_ref, n_ref, q_ref, qt_ref):
    for part, src in enumerate((x0_ref, x1_ref, x2_ref, x3_ref)):
        @pl.when(pl.program_id(0) == part)
        def _():
            xb = src[...]
            x = xb.astype(F32)
            n1 = (x * inv_rms(x) * gain_ref[...]).astype(BF)
            q = dot_nt(n1, wq_ref[...]).astype(BF) * jnp.asarray(0.125, BF)
            x_ref[...] = xb
            n_ref[...] = n1
            q_ref[...] = q
            qt_ref[...] = q.T


def queries(place, parts, gain, wqt):
    rows, dim = parts[0].shape
    width = wqt.shape[0] // 2
    n = len(parts)
    whole = pl.BlockSpec((rows, dim), lambda i, s: (0, 0))
    put = pl.BlockSpec((rows, dim), lambda i, s: (s[i], 0))
    return pl.pallas_call(
        query_kernel,
        out_shape=[jax.ShapeDtypeStruct((n * rows, dim), BF)] * 2
                  + [jax.ShapeDtypeStruct((n * rows, width), BF), jax.ShapeDtypeStruct((width, n * rows), BF)],
        grid_spec=pltpu.PrefetchScalarGridSpec(
            num_scalar_prefetch=1, grid=(n,),
            in_specs=[whole] * n + [pl.BlockSpec((1, dim), lambda i, s: (0, 0)),
                                    pl.BlockSpec((width, dim), lambda i, s: (s[n], 0))],
            out_specs=[put, put, pl.BlockSpec((rows, width), lambda i, s: (s[i], 0)),
                       pl.BlockSpec((width, rows), lambda i, s: (0, s[i]))]),
        compiler_params=pltpu.CompilerParams(vmem_limit_bytes=24 << 20),
        cost_estimate=cost(2 * n * rows * dim * width, 6 << 20),
        name="queries",
    )(place, *parts, gain, wqt)


def place_kernel(place_ref, x0_ref, x1_ref, o_ref):
    for part, src in enumerate((x0_ref, x1_ref)):
        @pl.when(pl.program_id(0) == part)
        def _():
            o_ref[...] = src[...]


def place_rows(place, parts):
    rows, dim = parts[0].shape
    n = len(parts)
    return pl.pallas_call(
        place_kernel,
        out_shape=jax.ShapeDtypeStruct((n * rows, dim), parts[0].dtype),
        grid_spec=pltpu.PrefetchScalarGridSpec(
            num_scalar_prefetch=1, grid=(n,),
            in_specs=[pl.BlockSpec((rows, dim), lambda i, s: (0, 0))] * n,
            out_specs=pl.BlockSpec((rows, dim), lambda i, s: (s[2 * i], 0))),
        compiler_params=pltpu.CompilerParams(vmem_limit_bytes=16 << 20),
        cost_estimate=cost(n * rows * dim, 6 << 20),
        name="place_rows",
    )(place, *parts)


def fwd_kernel(len_ref, qt_ref, k_ref, vt_ref, o_ref, m_ref, l_ref, acc_ref, qz_ref, sa_ref, sb_ref):
    qb = qt_ref.shape[1]
    seg_rows = k_ref.shape[0] // 2
    half = lax.broadcasted_iota(jnp.int32, (PAIR, qb), 0) // 64
    for h in range(2):
        qz_ref[h] = jnp.where(half == h, qt_ref[...], jnp.zeros((), BF))
    m_ref[...] = jnp.full(m_ref.shape, NEG, F32)
    l_ref[...] = jnp.zeros(l_ref.shape, F32)
    acc_ref[...] = jnp.zeros(acc_ref.shape, F32)
    first = len_ref[0] // FKB
    total = first + len_ref[1] // FKB

    def base(t):
        t = jnp.clip(t, 0, jnp.maximum(total - 1, 0))
        return pl.multiple_of(jnp.where(t < first, t * FKB, seg_rows + (t - first) * FKB), FKB)

    def scores(row, s_ref):
        kb = k_ref[pl.ds(row, FKB), :]
        for h in range(2):
            s_ref[h] = dot(kb, qz_ref[h])

    def absorb(row, s_ref, count=None):
        rows = pl.ds(row, FKB)
        for h in range(2):
            st = s_ref[h]
            if count is not None:
                st = jnp.where(lax.broadcasted_iota(jnp.int32, st.shape, 0) < count, st, NEG)
            m_old = m_ref[h]
            m_new = jnp.maximum(m_old, jnp.max(st, axis=0, keepdims=True))
            p = jnp.exp2((st - m_new) * LOG2E)
            alpha = jnp.exp2((m_old - m_new) * LOG2E)
            l_ref[h] = l_ref[h] * alpha + jnp.sum(p, axis=0, keepdims=True)
            pv = dot(vt_ref[h * 64:(h + 1) * 64, rows], p.astype(BF))
            acc_ref[h] = acc_ref[h] * alpha + pv
            m_ref[h] = m_new

    scores(base(0), sa_ref)

    @pl.loop(0, total // 2)
    def _(i):
        scores(base(2 * i + 1), sb_ref)
        absorb(base(2 * i), sa_ref)
        scores(base(2 * i + 2), sa_ref)
        absorb(base(2 * i + 1), sb_ref)

    @pl.when(total % 2 == 1)
    def _():
        absorb(base(total - 1), sa_ref)

    @pl.loop(0, 2)
    def _(s):
        full = len_ref[s] // FKB
        rest = len_ref[s] - full * FKB

        @pl.when(rest > 0)
        def _():
            row = pl.multiple_of(s * seg_rows + full * FKB, FKB)
            scores(row, sa_ref)
            absorb(row, sa_ref, rest)

    for h in range(2):
        o_ref[h, 0:64, :] = acc_ref[h]
        o_ref[h, 64:72, :] = jnp.concatenate([m_ref[h], l_ref[h], jnp.zeros((6, qb), F32)], axis=0)


def attention_forward(lens, qt, k, vt, pair0, pairs, at, nq):
    q_off = at // FQB
    rows = k.shape[0]
    off = pair0
    spec = pltpu.PrefetchScalarGridSpec(
        num_scalar_prefetch=1,
        grid=(pairs, nq // FQB),
        in_specs=[
            pl.BlockSpec((PAIR, FQB), lambda p, i, s: (p + off, i + q_off)),
            pl.BlockSpec((rows, PAIR), lambda p, i, s: (0, p + off)),
            pl.BlockSpec((PAIR, rows), lambda p, i, s: (p + off, 0)),
        ],
        out_specs=pl.BlockSpec((2, OROWS, FQB), lambda p, i, s: (p, 0, i)),
        scratch_shapes=[
            pltpu.VMEM((2, 1, FQB), F32), pltpu.VMEM((2, 1, FQB), F32), pltpu.VMEM((2, 64, FQB), F32),
            pltpu.VMEM((2, PAIR, FQB), BF), pltpu.VMEM((2, FKB, FQB), F32), pltpu.VMEM((2, FKB, FQB), F32),
        ])
    work = 2 * pairs * nq * rows
    return pl.pallas_call(
        fwd_kernel,
        out_shape=jax.ShapeDtypeStruct((2 * pairs, OROWS, nq), F32),
        grid_spec=spec,
        compiler_params=pltpu.CompilerParams(vmem_limit_bytes=60 << 20),
        cost_estimate=cost(work * 1024, 4 << 20, work),
        name="attn_fwd",
    )(lens, qt, k, vt)


def bwd_kernel(len_ref, qt_ref, dot_ref, lse_ref, dl_ref, k_ref, v_ref, kt_ref, dkv_ref, dqt_ref, qzt_ref, dozt_ref):
    nq = qt_ref.shape[1]
    seg_rows = k_ref.shape[0] // 2
    blocks = seg_rows // BKB
    half = lax.broadcasted_iota(jnp.int32, (PAIR, nq), 0) // 64
    zero = jnp.zeros((), BF)
    for h in range(2):
        qzt_ref[h] = jnp.where(half == h, qt_ref[...], zero)
        dozt_ref[h] = jnp.where(half == h, dot_ref[...], zero)
    dqt_ref[...] = jnp.zeros(dqt_ref.shape, F32)

    def step(seg, j, count):
        cols = pl.ds(pl.multiple_of(j * BKB, BKB), BKB)
        allc = pl.ds(pl.multiple_of(seg * seg_rows + j * BKB, BKB), BKB)
        kb, vb = k_ref[allc, :], v_ref[allc, :]
        for h in range(2):
            hs = slice(h * 64, (h + 1) * 64)
            ktb = kt_ref[hs, allc]
            dk = jnp.zeros((64, BKB), F32)
            dv = jnp.zeros((64, BKB), F32)
            for c in range(nq // BQB):
                qs = slice(c * BQB, (c + 1) * BQB)
                st = dot(kb, qzt_ref[h, :, qs])
                p = jnp.exp2((st - lse_ref[h, :, qs]) * LOG2E)
                if count is not None:
                    p = jnp.where(lax.broadcasted_iota(jnp.int32, st.shape, 0) < count, p, 0.0)
                dp = dot(vb, dozt_ref[h, :, qs])
                ds = (p * (dp - dl_ref[h, :, qs])).astype(BF)
                dv = dv + dot_nt(dot_ref[hs, qs], p.astype(BF))
                dk = dk + dot_nt(qt_ref[hs, qs], ds)
                dqt_ref[h, :, qs] += dot(ktb, ds)
            dkv_ref[seg, hs, cols] = dk.astype(BF)
            dkv_ref[seg, PAIR + h * 64:PAIR + (h + 1) * 64, cols] = dv.astype(BF)

    first = len_ref[0] // BKB

    @pl.loop(0, first + len_ref[1] // BKB)
    def _(t):
        seg = jnp.where(t < first, 0, 1)
        step(seg, t - seg * first, None)

    @pl.loop(0, 2)
    def _(seg):
        full = len_ref[seg] // BKB
        rest = len_ref[seg] - full * BKB

        @pl.when(rest > 0)
        def _():
            step(seg, full, rest)

        @pl.loop(full + jnp.where(rest > 0, 1, 0), blocks)
        def _(j):
            cols = pl.ds(pl.multiple_of(j * BKB, BKB), BKB)
            dkv_ref[seg, :, cols] = jnp.zeros((2 * PAIR, BKB), BF)


def attention_backward(lens, qt, dot_t, lse, delta, k, v, kt, pair0):
    nq = qt.shape[1]
    rows = k.shape[0]
    off = pair0
    across = pl.BlockSpec((PAIR, nq), lambda p, s: (off, 0))
    stat = pl.BlockSpec((2, 1, nq), lambda p, s: (off, 0, 0))
    keys = pl.BlockSpec((rows, PAIR), lambda p, s: (0, off))
    keys_t = pl.BlockSpec((PAIR, rows), lambda p, s: (off, 0))
    spec = pltpu.PrefetchScalarGridSpec(
        num_scalar_prefetch=1,
        grid=(1,),
        in_specs=[across, across, stat, stat, keys, keys, keys_t],
        out_specs=[pl.BlockSpec((2, 2 * PAIR, rows // 2), lambda p, s: (0, 0, 0)),
                   pl.BlockSpec((2, 64, nq), lambda p, s: (0, 0, 0))],
        scratch_shapes=[pltpu.VMEM((2, PAIR, nq), BF), pltpu.VMEM((2, PAIR, nq), BF)])
    work = 2 * nq * rows
    return pl.pallas_call(
        bwd_kernel,
        out_shape=[jax.ShapeDtypeStruct((2, 2 * PAIR, rows // 2), BF), jax.ShapeDtypeStruct((2, 64, nq), F32)],
        grid_spec=spec,
        compiler_params=pltpu.CompilerParams(vmem_limit_bytes=40 << 20),
        cost_estimate=cost(work * 2000, 8 << 20, work),
        name="attn_bwd",
    )(lens, qt, dot_t, lse, delta, k, v, kt)


def mlp_kernel(h_ref, g_ref, gain_ref, w1_ref, w3_ref, w2_ref,
               n2t_ref, gt_ref, dgate_ref, dup_ref, ut_ref, dh_ref, dhb_ref, gn_ref, n2_ref, acc_ref):
    step = pl.program_id(0)
    rows = h_ref.shape[0]
    chunk = 256

    @pl.when(step == 0)
    def _():
        for c in range(rows // chunk):
            rs = slice(c * chunk, (c + 1) * chunk)
            hid = h_ref[rs, :].astype(F32)
            n2 = (hid * inv_rms(hid) * gain_ref[...]).astype(BF)
            n2_ref[rs, :] = n2
            n2t_ref[:, rs] = n2.T
            gt_ref[rs, :] = g_ref[rs, :].astype(BF)
        acc_ref[...] = jnp.zeros(acc_ref.shape, F32)

    w1, w3, w2 = w1_ref[...], w3_ref[...], w2_ref[...]
    for c in range(rows // chunk):
        rs = slice(c * chunk, (c + 1) * chunk)
        n2 = n2_ref[rs, :]
        gate = dot(n2, w1)
        up = dot(n2, w3)
        ga = dot_nt(gt_ref[rs, :], w2)
        sig = 0.5 * jnp.tanh(0.5 * gate) + 0.5
        act = gate * sig
        ut_ref[:, rs] = (act * up).astype(BF).T
        dup = (ga * act).astype(BF)
        dgate = (ga * up * (sig + act * (1.0 - sig))).astype(BF)
        dup_ref[rs, :] = dup
        dgate_ref[rs, :] = dgate
        acc_ref[rs, :] += dot_nt(dgate, w1) + dot_nt(dup, w3)

    @pl.when(step == pl.num_programs(0) - 1)
    def _():
        total = jnp.zeros(gn_ref.shape, F32)
        for c in range(rows // chunk):
            rs = slice(c * chunk, (c + 1) * chunk)
            hid = h_ref[rs, :].astype(F32)
            inv = inv_rms(hid)
            unit = hid * inv
            grad = acc_ref[rs, :]
            total += jnp.sum(grad * unit, axis=0, keepdims=True)
            dh = g_ref[rs, :] + norm_back(unit, inv, gain_ref[...], grad)
            dh_ref[rs, :] = dh
            dhb_ref[rs, :] = dh.astype(BF)
        gn_ref[...] = total


def mlp(hidden, g_all, gain, w_gate, w_up, w_down):
    rows, dim = hidden.shape
    ff = w_gate.shape[1]
    fix = lambda *shape: pl.BlockSpec(shape, lambda i: (0,) * len(shape))
    wide = pl.BlockSpec((dim, FFB), lambda i: (0, i))
    tall = pl.BlockSpec((FFB, dim), lambda i: (i, 0))
    act = pl.BlockSpec((rows, FFB), lambda i: (0, i))
    act_t = pl.BlockSpec((FFB, rows), lambda i: (i, 0))
    return pl.pallas_call(
        mlp_kernel,
        grid=(ff // FFB,),
        in_specs=[fix(rows, dim), fix(rows, dim), fix(1, dim), wide, wide, tall],
        out_specs=[fix(dim, rows), fix(rows, dim), act, act, act_t, fix(rows, dim), fix(rows, dim), fix(1, dim)],
        out_shape=[jax.ShapeDtypeStruct((dim, rows), BF), jax.ShapeDtypeStruct((rows, dim), BF),
                   jax.ShapeDtypeStruct((rows, ff), BF), jax.ShapeDtypeStruct((rows, ff), BF),
                   jax.ShapeDtypeStruct((ff, rows), BF), jax.ShapeDtypeStruct((rows, dim), F32),
                   jax.ShapeDtypeStruct((rows, dim), BF), jax.ShapeDtypeStruct((1, dim), F32)],
        scratch_shapes=[pltpu.VMEM((rows, dim), BF), pltpu.VMEM((rows, dim), F32)],
        compiler_params=pltpu.CompilerParams(vmem_limit_bytes=56 << 20),
        cost_estimate=cost(10 * rows * dim * ff, 40 << 20, rows * ff),
        name="mlp",
    )(hidden, g_all, gain, w_gate, w_up, w_down)


def mlp_weights_kernel(n2t_ref, gt_ref, dgate_ref, dup_ref, ut_ref, n2t2_ref, gt2_ref, dgate2_ref, dup2_ref, ut2_ref,
                       g1_ref, g3_ref, g2_ref):
    g1_ref[...] = dot(n2t_ref[...], dgate_ref[...]) + dot(n2t2_ref[...], dgate2_ref[...])
    g3_ref[...] = dot(n2t_ref[...], dup_ref[...]) + dot(n2t2_ref[...], dup2_ref[...])
    g2_ref[...] = dot(ut_ref[...], gt_ref[...]) + dot(ut2_ref[...], gt2_ref[...])


def mlp_weights(factors, factors_near):
    dim, rows = factors[0].shape
    ff = factors[2].shape[1]
    fix = lambda *shape: pl.BlockSpec(shape, lambda i: (0,) * len(shape))
    act = pl.BlockSpec((rows, FFB), lambda i: (0, i))
    wide = pl.BlockSpec((dim, FFB), lambda i: (0, i))
    ins = [fix(dim, rows), fix(rows, dim), act, act, pl.BlockSpec((FFB, rows), lambda i: (i, 0))]
    return pl.pallas_call(
        mlp_weights_kernel,
        grid=(ff // FFB,),
        in_specs=ins + ins,
        out_specs=[wide, wide, pl.BlockSpec((FFB, dim), lambda i: (i, 0))],
        out_shape=[jax.ShapeDtypeStruct((dim, ff), F32)] * 2 + [jax.ShapeDtypeStruct((ff, dim), F32)],
        compiler_params=pltpu.CompilerParams(vmem_limit_bytes=60 << 20),
        cost_estimate=cost(12 * rows * dim * ff, 50 << 20),
        name="mlp_weights",
    )(*factors, *factors_near)


def memory_kernel(core_ref, a0_ref, a1_ref, a2_ref, b0_ref, b1_ref, b2_ref, wk_ref, wv_ref, o_ref):
    core = core_ref[0]
    total = None
    for who, refs in ((core, (a0_ref, a1_ref, a2_ref)), (1 - core, (b0_ref, b1_ref, b2_ref))):
        for i, ref in enumerate(refs):
            rows = pl.ds(pl.multiple_of((who * 3 + i) * PAIR, PAIR), PAIR)
            part = dot(ref[...].T, jnp.concatenate([wk_ref[rows, :], wv_ref[rows, :]], axis=0))
            total = part if total is None else total + part
    o_ref[...] = total


def memory_grad(core, mine, near, wkt, wvt):
    rows = mine[0].shape[-1]
    dim = wkt.shape[1]
    block = pl.BlockSpec((None, 2 * PAIR, MB), lambda i, s: (0, 0, i))
    block2 = pl.BlockSpec((2 * PAIR, MB), lambda i, s: (0, i))
    whole = pl.BlockSpec(wkt.shape, lambda i, s: (0, 0))
    return pl.pallas_call(
        memory_kernel,
        out_shape=jax.ShapeDtypeStruct((rows, dim), F32),
        grid_spec=pltpu.PrefetchScalarGridSpec(
            num_scalar_prefetch=1, grid=(rows // MB,),
            in_specs=[block] * 3 + [block2] * 3 + [whole, whole],
            out_specs=pl.BlockSpec((MB, dim), lambda i, s: (i, 0))),
        compiler_params=pltpu.CompilerParams(vmem_limit_bytes=32 << 20),
        cost_estimate=cost(4 * rows * dim * dim, 16 << 20),
        name="memory_grad",
    )(core, *mine, *near, wkt, wvt)


def half_index(i, core):
    return i + core - 2 * i * core


def out_proj_kernel(core_ref, mine_ref, near0_ref, near1_ref, dh_ref, o_ref):
    half = near0_ref.shape[1]

    @pl.when(pl.program_id(0) == 0)
    def _():
        o_ref[...] = dot(mine_ref[...], dh_ref[...])

    @pl.when(pl.program_id(0) == 1)
    def _():
        o_ref[...] = dot(near0_ref[...], dh_ref[:half, :]) + dot(near1_ref[...], dh_ref[half:, :])


def out_proj_grad(core, mine, near, dh):
    width, rows = mine.shape
    dim = dh.shape[1]
    whole = pl.BlockSpec((width, rows), lambda i, s: (0, 0))
    part = pl.BlockSpec((width, rows // 2), lambda i, s: (0, 0))
    return pl.pallas_call(
        out_proj_kernel,
        out_shape=jax.ShapeDtypeStruct((2 * width, dim), F32),
        grid_spec=pltpu.PrefetchScalarGridSpec(
            num_scalar_prefetch=1, grid=(2,),
            in_specs=[whole, part, part, pl.BlockSpec((rows, dim), lambda i, s: (0, 0))],
            out_specs=pl.BlockSpec((width, dim), lambda i, s: (half_index(i, s[0]), 0))),
        compiler_params=pltpu.CompilerParams(vmem_limit_bytes=24 << 20),
        cost_estimate=cost(4 * rows * dim * width, 6 << 20),
        name="out_proj_grad",
    )(core, mine, *near, dh)


def query_grad_kernel(place_ref, mine_ref, near_ref, n1_ref, wq_ref, x_ref, dh_ref, gain_ref,
                      gw_ref, gx_ref, gn_ref, acc_ref):
    half = acc_ref.shape[0] // 2

    @pl.when(pl.program_id(0) == 0)
    def _():
        gw_ref[...] = dot(mine_ref[...], n1_ref[...])
        acc_ref[...] = dot(mine_ref[...].T, wq_ref[...])

    @pl.when(pl.program_id(0) == 1)
    def _():
        first, second = near_ref[:, half:], near_ref[:, :half]
        gw_ref[...] = dot(first, n1_ref[:half, :]) + dot(second, n1_ref[half:, :])
        acc_ref[:half, :] += dot(first.T, wq_ref[...])
        acc_ref[half:, :] += dot(second.T, wq_ref[...])

    @pl.when(pl.program_id(0) == 1)
    def _():
        rows = gx_ref.shape[0]
        total = jnp.zeros(gn_ref.shape, F32)
        for c in range(acc_ref.shape[0] // rows):
            rs = slice(c * rows, (c + 1) * rows)
            x = x_ref[rs, :].astype(F32)
            total += jnp.sum(acc_ref[rs, :] * (x * inv_rms(x)), axis=0, keepdims=True)
        gn_ref[...] = total
        own = pl.ds(pl.multiple_of(place_ref[0] * rows, rows), rows)
        x = x_ref[own, :].astype(F32)
        inv = inv_rms(x)
        gx_ref[...] = dh_ref[...] + norm_back(x * inv, inv, gain_ref[...], acc_ref[own, :])


def query_grad(place, mine, near, n1, wqt, x_all, d_hid, gain, rows):
    width, total = mine.shape
    dim = n1.shape[1]
    fix = lambda *shape: pl.BlockSpec(shape, lambda i, s: (0,) * len(shape))
    half = pl.BlockSpec((width, dim), lambda i, s: (half_index(i, s[4]), 0))
    return pl.pallas_call(
        query_grad_kernel,
        out_shape=[jax.ShapeDtypeStruct((2 * width, dim), F32), jax.ShapeDtypeStruct((rows, dim), F32),
                   jax.ShapeDtypeStruct((1, dim), F32)],
        grid_spec=pltpu.PrefetchScalarGridSpec(
            num_scalar_prefetch=1, grid=(2,),
            in_specs=[fix(width, total), fix(width, total), fix(total, dim), half, fix(total, dim),
                      pl.BlockSpec((rows, dim), lambda i, s: (s[0], 0)), fix(1, dim)],
            out_specs=[half, fix(rows, dim), fix(1, dim)],
            scratch_shapes=[pltpu.VMEM((total, dim), F32)]),
        compiler_params=pltpu.CompilerParams(vmem_limit_bytes=32 << 20),
        cost_estimate=cost(8 * total * dim * width, 10 << 20),
        name="query_grad",
    )(place, mine, near, n1, wqt, x_all, d_hid, gain)


def key_weights_kernel(core_ref, a0_ref, a1_ref, a2_ref, b0_ref, b1_ref, b2_ref, gk_ref, gv_ref):
    for at, ref in enumerate((a0_ref, a1_ref, a2_ref, b0_ref, b1_ref, b2_ref)):
        @pl.when(pl.program_id(0) == at)
        def _():
            gk_ref[...] = ref[:PAIR, :]
            gv_ref[...] = ref[PAIR:, :]


def key_weights(core, mine, near):
    pairs = len(mine)
    dim = mine[0].shape[1]
    out = pl.BlockSpec((PAIR, dim), lambda i, s: (half_index(i // pairs, s[0]) * pairs + i % pairs, 0))
    return pl.pallas_call(
        key_weights_kernel,
        out_shape=[jax.ShapeDtypeStruct((2 * pairs * PAIR, dim), F32)] * 2,
        grid_spec=pltpu.PrefetchScalarGridSpec(
            num_scalar_prefetch=1, grid=(2 * pairs,),
            in_specs=[pl.BlockSpec((2 * PAIR, dim), lambda i, s: (0, 0))] * (2 * pairs),
            out_specs=[out, out]),
        compiler_params=pltpu.CompilerParams(vmem_limit_bytes=24 << 20),
        cost_estimate=cost(4 * pairs * PAIR * dim, 10 << 20),
        name="key_weights",
    )(core, *mine, *near)


def inv_rms(tensor):
    return lax.rsqrt(jnp.mean(tensor * tensor, axis=-1, keepdims=True) + 1e-6)


def norm_back(unit, inv, gain, grad):
    scaled = grad * gain
    return inv * (scaled - unit * jnp.mean(scaled * unit, axis=-1, keepdims=True))


def mm(a, b, ca, cb, dtype=F32):
    out = lax.dot_general(a, b, (((ca,), (cb,)), ((), ())), preferred_element_type=F32)
    return out if dtype == F32 else out.astype(dtype)


def solution(mesh):
    n = mesh.shape['seq']
    near = [(i, i ^ 1) for i in range(n)]
    far = [(i, i ^ 2) for i in range(n)]
    row_spec = P(('data', 'seq'), None)
    weight_spec = P()
    part_vec = P('data')
    part_mat = P('data', None)
    part_cube = P('data', None, None)

    def to_near(a):
        return lax.ppermute(a, 'seq', near)

    def to_far(a):
        return lax.ppermute(a, 'seq', far)

    def device_work(dec_in, memory, mem_len, grad_out, norm_attn, wq, wk, wv, wo, norm_mlp, w_gate, w_up, w_down):
        rows, dim = dec_in.shape
        m_rows = memory.shape[0]
        heads, head = wq.shape[1], wq.shape[2]
        mine = heads // 2
        width = mine * head
        dev = lax.axis_index('seq')
        core = lax.rem(dev, 2)
        core1 = core.reshape(1).astype(jnp.int32)
        wqt, wkt, wvt = (w.transpose(1, 2, 0).reshape(heads * head, dim) for w in (wq, wk, wv))
        wo2 = wo.reshape(heads * head, dim)
        lens = jnp.stack([jnp.clip(mem_len[0] - i * m_rows, 0, m_rows) for i in (dev, dev ^ 1)]).astype(jnp.int32)
        chip = dev // 2
        place = jnp.stack([chip, 2 + chip, 1 - chip, 3 - chip, core]).astype(jnp.int32)
        gain1 = norm_attn.astype(F32).reshape(1, dim)
        gain2 = norm_mlp.astype(F32).reshape(1, dim)

        def gather_parts(a):
            across = to_far(a)
            beside = to_near(a)
            return a, beside, across, to_near(across)

        x_parts = gather_parts(dec_in)
        mem_near = to_near(memory)
        g_parts = (grad_out, to_far(grad_out))

        first = project(core1, memory, wkt, wvt, 0, ())
        x_all_b, n1, _, qt_s = queries(place, x_parts, gain1, wqt)
        k, v, kt, vt = project(core1, mem_near, wkt, wvt, 1, first)

        pairs = mine // 2
        pieces = [(pair, 0, n * rows) for pair in range(pairs - 1)]
        pieces += [(pairs - 1, 0, n * rows // 2), (pairs - 1, n * rows // 2, n * rows // 2)]
        outs, lses = [], []
        parts = []
        for pair, at, count in pieces:
            part = attention_forward(lens, qt_s, k, vt, pair, 1, at, count)
            parts.append((part, to_far(part)))
        for a, b in parts:
            ma, mb = a[:, 64:65], b[:, 64:65]
            top = jnp.maximum(ma, mb)
            ea, eb = jnp.exp(ma - top), jnp.exp(mb - top)
            den = a[:, 65:66] * ea + b[:, 65:66] * eb
            outs.append((a[:, :64] * ea + b[:, :64] * eb) / den)
            lses.append(top + jnp.log(den))
        outs[-2:] = [jnp.concatenate(outs[-2:], axis=2)]
        lses[-2:] = [jnp.concatenate(lses[-2:], axis=2)]
        g_half = place_rows(place, g_parts)
        o_t = jnp.concatenate(outs, axis=0)
        lse = jnp.concatenate(lses, axis=0)
        o_t_b = o_t.astype(BF).reshape(width, n * rows)
        half = n * rows // 2
        o_t_first, o_t_second = o_t_b[:, :half], o_t_b[:, half:]
        o_near_first = to_near(o_t_second)

        def half_rows(w, who):
            return lax.dynamic_slice(w, (who * width, 0), (width, dim))

        wo_m, wo_n = half_rows(wo2, core), half_rows(wo2, 1 - core)
        hidden = (x_all_b[:half].astype(F32) + mm(o_t_first, wo_m, 0, 0) + mm(o_near_first, wo_n, 0, 0)).astype(BF)

        n2t, g_top, d_gate, d_up, act_t, d_hid, d_hid_half, g_norm_half = mlp(
            hidden, g_half, gain2, w_gate, w_up, w_down)
        d_hid_b = jnp.concatenate([d_hid_half, to_near(d_hid_half)], axis=0)
        factors = (n2t, g_top, d_gate, d_up, act_t)
        factors_near = tuple(to_near(a) for a in factors)
        o_near_second = to_near(o_t_first)
        g_norm_mlp = g_norm_half + to_near(g_norm_half)

        do_t_f = mm(wo_m, d_hid_b, 1, 1)
        delta = jnp.sum(do_t_f.reshape(mine, head, n * rows) * o_t, axis=1, keepdims=True)
        do_t = do_t_f.astype(BF)
        dkvs, dkvs_near, dqs, dws = [], [], [], []
        lens_now = lens
        for pair in range(pairs):
            dkv, dqt = attention_backward(lens_now, qt_s, do_t, lse, delta, k, v, kt, pair)
            dqs.append((dqt, to_far(dqt)))
            dw = mm(dkv[0], memory, 1, 0) + mm(dkv[1], mem_near, 1, 0)
            dws.append((dw, to_far(dw)))
            dkvs.append(dkv)
            dkvs_near.append(to_near(dkv[1]))
            lens_now, dw_last = lax.optimization_barrier((lens, dw))

        act_t, _ = lax.optimization_barrier((act_t, dw_last))
        factors = (n2t, g_top, d_gate, d_up, act_t)
        g_gate, g_up, g_down = mlp_weights(factors, factors_near)
        g_mem = memory_grad(core1, dkvs, dkvs_near, wkt, wvt)

        def as_weight(rows_by_dim):
            return rows_by_dim.reshape(heads, head, dim).transpose(2, 0, 1)

        g_wo = out_proj_grad(core1, o_t_b, (o_near_first, o_near_second), d_hid_b).reshape(heads, head, dim)

        dqt_b = (jnp.concatenate([a + b for a, b in dqs], axis=0) * (head ** -0.5)).astype(BF).reshape(width, n * rows)
        dqt_near = to_near(dqt_b)
        g_wqt, g_dec, g_norm_attn = query_grad(place, dqt_b, dqt_near, n1, wqt, x_all_b, d_hid, gain1, rows)

        dw_mine, dw_near = [], []
        for a, b in dws:
            dw_mine.append(a + b)
            dw_near.append(to_near(dw_mine[-1]))
        g_wkt, g_wvt = key_weights(core1, dw_mine, dw_near)
        g_wq, g_wk, g_wv = as_weight(g_wqt), as_weight(g_wkt), as_weight(g_wvt)
        return (g_dec, g_mem, g_norm_attn.reshape(dim), g_wq, g_wk, g_wv, g_wo, g_norm_mlp.reshape(dim), g_gate, g_up, g_down)


    return jax.shard_map(device_work, mesh=mesh,
                         in_specs=(row_spec, row_spec, part_vec, row_spec) + (weight_spec,) * 9,
                         out_specs=(row_spec, row_spec, part_vec, part_cube, part_cube, part_cube, part_cube,
                                    part_vec, part_mat, part_mat, part_mat),
                         check_vma=False)
```

```python
import jax
import jax.numpy as jnp
from jax import lax
from jax.experimental import pallas as pl
from jax.experimental.pallas import tpu as pltpu
from jax.sharding import PartitionSpec as P


LOG2E = 1.4426950408889634
NEG = -1e30
BF = jnp.bfloat16
F32 = jnp.float32
FKB = 512
FQB = 512
BKB = 512
BQB = 256
PAIR = 128
OROWS = 72
FFB = 512
MB = 512


def dot(a, b):
    return jnp.dot(a, b, preferred_element_type=F32)


def dot_nt(a, b):
    return lax.dot_general(a, b, (((1,), (1,)), ((), ())), preferred_element_type=F32)


def cost(flops, bytes_accessed, exps=0):
    return pl.CostEstimate(flops=int(flops), bytes_accessed=int(bytes_accessed), transcendentals=int(exps))


def proj_kernel(core_ref, m_ref, wk_ref, wv_ref, *refs):
    k_ref, v_ref, kt_ref, vt_ref = refs[-4:]
    m = m_ref[...]
    k_ref[...] = dot_nt(m, wk_ref[...]).astype(BF)
    v_ref[...] = dot_nt(m, wv_ref[...]).astype(BF)
    kt_ref[...] = dot_nt(wk_ref[...], m).astype(BF)
    vt_ref[...] = dot_nt(wv_ref[...], m).astype(BF)


def project(core, mem, wkt, wvt, seg, before):
    rows, dim = mem.shape
    width = wkt.shape[0] // 2
    steps = rows // MB
    base = seg * steps
    weights = pl.BlockSpec((width, dim), lambda i, s: (s[0], 0))
    down = pl.BlockSpec((MB, width), lambda i, s: (base + i, 0))
    across = pl.BlockSpec((width, MB), lambda i, s: (0, base + i))
    outs = [jax.ShapeDtypeStruct((2 * rows, width), BF)] * 2 + [jax.ShapeDtypeStruct((width, 2 * rows), BF)] * 2
    return pl.pallas_call(
        proj_kernel,
        out_shape=outs,
        grid_spec=pltpu.PrefetchScalarGridSpec(
            num_scalar_prefetch=1, grid=(steps,),
            in_specs=[pl.BlockSpec((MB, dim), lambda i, s: (i, 0)), weights, weights]
                     + [pl.BlockSpec(memory_space=pl.ANY)] * len(before),
            out_specs=[down, down, across, across]),
        input_output_aliases={4 + i: i for i in range(len(before))},
        compiler_params=pltpu.CompilerParams(vmem_limit_bytes=60 << 20),
        cost_estimate=cost(4 * rows * dim * width, 12 << 20),
        name="kv_proj",
    )(core, mem, wkt, wvt, *before)


def query_kernel(place_ref, x0_ref, x1_ref, x2_ref, x3_ref, gain_ref, wq_ref, x_ref, n_ref, q_ref, qt_ref):
    for part, src in enumerate((x0_ref, x1_ref, x2_ref, x3_ref)):
        @pl.when(pl.program_id(0) == part)
        def _():
            xb = src[...]
            x = xb.astype(F32)
            n1 = (x * inv_rms(x) * gain_ref[...]).astype(BF)
            q = dot_nt(n1, wq_ref[...]).astype(BF) * jnp.asarray(0.125, BF)
            x_ref[...] = xb
            n_ref[...] = n1
            q_ref[...] = q
            qt_ref[...] = q.T


def queries(place, parts, gain, wqt):
    rows, dim = parts[0].shape
    width = wqt.shape[0] // 2
    n = len(parts)
    whole = pl.BlockSpec((rows, dim), lambda i, s: (0, 0))
    put = pl.BlockSpec((rows, dim), lambda i, s: (s[i], 0))
    return pl.pallas_call(
        query_kernel,
        out_shape=[jax.ShapeDtypeStruct((n * rows, dim), BF)] * 2
                  + [jax.ShapeDtypeStruct((n * rows, width), BF), jax.ShapeDtypeStruct((width, n * rows), BF)],
        grid_spec=pltpu.PrefetchScalarGridSpec(
            num_scalar_prefetch=1, grid=(n,),
            in_specs=[whole] * n + [pl.BlockSpec((1, dim), lambda i, s: (0, 0)),
                                    pl.BlockSpec((width, dim), lambda i, s: (s[n], 0))],
            out_specs=[put, put, pl.BlockSpec((rows, width), lambda i, s: (s[i], 0)),
                       pl.BlockSpec((width, rows), lambda i, s: (0, s[i]))]),
        compiler_params=pltpu.CompilerParams(vmem_limit_bytes=24 << 20),
        cost_estimate=cost(2 * n * rows * dim * width, 6 << 20),
        name="queries",
    )(place, *parts, gain, wqt)


def place_kernel(place_ref, x0_ref, x1_ref, o_ref):
    for part, src in enumerate((x0_ref, x1_ref)):
        @pl.when(pl.program_id(0) == part)
        def _():
            o_ref[...] = src[...]


def place_rows(place, parts):
    rows, dim = parts[0].shape
    n = len(parts)
    return pl.pallas_call(
        place_kernel,
        out_shape=jax.ShapeDtypeStruct((n * rows, dim), parts[0].dtype),
        grid_spec=pltpu.PrefetchScalarGridSpec(
            num_scalar_prefetch=1, grid=(n,),
            in_specs=[pl.BlockSpec((rows, dim), lambda i, s: (0, 0))] * n,
            out_specs=pl.BlockSpec((rows, dim), lambda i, s: (s[2 * i], 0))),
        compiler_params=pltpu.CompilerParams(vmem_limit_bytes=16 << 20),
        cost_estimate=cost(n * rows * dim, 6 << 20),
        name="place_rows",
    )(place, *parts)


def fwd_kernel(len_ref, qt_ref, k_ref, vt_ref, o_ref, m_ref, l_ref, acc_ref, qz_ref, sa_ref, sb_ref):
    qb = qt_ref.shape[1]
    seg_rows = k_ref.shape[0] // 2
    half = lax.broadcasted_iota(jnp.int32, (PAIR, qb), 0) // 64
    for h in range(2):
        qz_ref[h] = jnp.where(half == h, qt_ref[...], jnp.zeros((), BF))
    m_ref[...] = jnp.full(m_ref.shape, NEG, F32)
    l_ref[...] = jnp.zeros(l_ref.shape, F32)
    acc_ref[...] = jnp.zeros(acc_ref.shape, F32)
    first = len_ref[0] // FKB
    total = first + len_ref[1] // FKB

    def base(t):
        t = jnp.clip(t, 0, jnp.maximum(total - 1, 0))
        return pl.multiple_of(jnp.where(t < first, t * FKB, seg_rows + (t - first) * FKB), FKB)

    def scores(row, s_ref):
        kb = k_ref[pl.ds(row, FKB), :]
        for h in range(2):
            s_ref[h] = dot(kb, qz_ref[h])

    def absorb(row, s_ref, count=None):
        rows = pl.ds(row, FKB)
        for h in range(2):
            st = s_ref[h]
            if count is not None:
                st = jnp.where(lax.broadcasted_iota(jnp.int32, st.shape, 0) < count, st, NEG)
            m_old = m_ref[h]
            m_new = jnp.maximum(m_old, jnp.max(st, axis=0, keepdims=True))
            p = jnp.exp2((st - m_new) * LOG2E)
            alpha = jnp.exp2((m_old - m_new) * LOG2E)
            l_ref[h] = l_ref[h] * alpha + jnp.sum(p, axis=0, keepdims=True)
            pv = dot(vt_ref[h * 64:(h + 1) * 64, rows], p.astype(BF))
            acc_ref[h] = acc_ref[h] * alpha + pv
            m_ref[h] = m_new

    scores(base(0), sa_ref)

    @pl.loop(0, total // 2)
    def _(i):
        scores(base(2 * i + 1), sb_ref)
        absorb(base(2 * i), sa_ref)
        scores(base(2 * i + 2), sa_ref)
        absorb(base(2 * i + 1), sb_ref)

    @pl.when(total % 2 == 1)
    def _():
        absorb(base(total - 1), sa_ref)

    @pl.loop(0, 2)
    def _(s):
        full = len_ref[s] // FKB
        rest = len_ref[s] - full * FKB

        @pl.when(rest > 0)
        def _():
            row = pl.multiple_of(s * seg_rows + full * FKB, FKB)
            scores(row, sa_ref)
            absorb(row, sa_ref, rest)

    for h in range(2):
        o_ref[h, 0:64, :] = acc_ref[h]
        o_ref[h, 64:72, :] = jnp.concatenate([m_ref[h], l_ref[h], jnp.zeros((6, qb), F32)], axis=0)


def attention_forward(lens, qt, k, vt, pair0, pairs, at, nq):
    q_off = at // FQB
    rows = k.shape[0]
    off = pair0
    spec = pltpu.PrefetchScalarGridSpec(
        num_scalar_prefetch=1,
        grid=(pairs, nq // FQB),
        in_specs=[
            pl.BlockSpec((PAIR, FQB), lambda p, i, s: (p + off, i + q_off)),
            pl.BlockSpec((rows, PAIR), lambda p, i, s: (0, p + off)),
            pl.BlockSpec((PAIR, rows), lambda p, i, s: (p + off, 0)),
        ],
        out_specs=pl.BlockSpec((2, OROWS, FQB), lambda p, i, s: (p, 0, i)),
        scratch_shapes=[
            pltpu.VMEM((2, 1, FQB), F32), pltpu.VMEM((2, 1, FQB), F32), pltpu.VMEM((2, 64, FQB), F32),
            pltpu.VMEM((2, PAIR, FQB), BF), pltpu.VMEM((2, FKB, FQB), F32), pltpu.VMEM((2, FKB, FQB), F32),
        ])
    work = 2 * pairs * nq * rows
    return pl.pallas_call(
        fwd_kernel,
        out_shape=jax.ShapeDtypeStruct((2 * pairs, OROWS, nq), F32),
        grid_spec=spec,
        compiler_params=pltpu.CompilerParams(vmem_limit_bytes=60 << 20),
        cost_estimate=cost(work * 1024, 4 << 20, work),
        name="attn_fwd",
    )(lens, qt, k, vt)


def bwd_kernel(len_ref, qt_ref, dot_ref, lse_ref, dl_ref, k_ref, v_ref, kt_ref, dkv_ref, dqt_ref, qzt_ref, dozt_ref):
    nq = qt_ref.shape[1]
    seg_rows = k_ref.shape[0] // 2
    blocks = seg_rows // BKB
    half = lax.broadcasted_iota(jnp.int32, (PAIR, nq), 0) // 64
    zero = jnp.zeros((), BF)
    for h in range(2):
        qzt_ref[h] = jnp.where(half == h, qt_ref[...], zero)
        dozt_ref[h] = jnp.where(half == h, dot_ref[...], zero)
    dqt_ref[...] = jnp.zeros(dqt_ref.shape, F32)

    def step(seg, j, count):
        cols = pl.ds(pl.multiple_of(j * BKB, BKB), BKB)
        allc = pl.ds(pl.multiple_of(seg * seg_rows + j * BKB, BKB), BKB)
        kb, vb = k_ref[allc, :], v_ref[allc, :]
        chunks = [(h, slice(c * BQB, (c + 1) * BQB)) for h in range(2) for c in range(nq // BQB)]

        def products(h, qs):
            return dot(kb, qzt_ref[h, :, qs]), dot(vb, dozt_ref[h, :, qs])

        ahead = products(*chunks[0])
        for i, (h, qs) in enumerate(chunks):
            st, dp = ahead
            if i + 1 < len(chunks):
                ahead = products(*chunks[i + 1])
            hs = slice(h * 64, (h + 1) * 64)
            if qs.start == 0:
                dk = jnp.zeros((64, BKB), F32)
                dv = jnp.zeros((64, BKB), F32)
            p = jnp.exp2((st - lse_ref[h, :, qs]) * LOG2E)
            if count is not None:
                p = jnp.where(lax.broadcasted_iota(jnp.int32, st.shape, 0) < count, p, 0.0)
            ds = (p * (dp - dl_ref[h, :, qs])).astype(BF)
            dv = dv + dot_nt(dot_ref[hs, qs], p.astype(BF))
            dk = dk + dot_nt(qt_ref[hs, qs], ds)
            dqt_ref[h, :, qs] += dot(kt_ref[hs, allc], ds)
            if qs.stop == nq:
                dkv_ref[seg, hs, cols] = dk.astype(BF)
                dkv_ref[seg, PAIR + h * 64:PAIR + (h + 1) * 64, cols] = dv.astype(BF)

    first = len_ref[0] // BKB

    @pl.loop(0, first + len_ref[1] // BKB)
    def _(t):
        seg = jnp.where(t < first, 0, 1)
        step(seg, t - seg * first, None)

    @pl.loop(0, 2)
    def _(seg):
        full = len_ref[seg] // BKB
        rest = len_ref[seg] - full * BKB

        @pl.when(rest > 0)
        def _():
            step(seg, full, rest)

        @pl.loop(full + jnp.where(rest > 0, 1, 0), blocks)
        def _(j):
            cols = pl.ds(pl.multiple_of(j * BKB, BKB), BKB)
            dkv_ref[seg, :, cols] = jnp.zeros((2 * PAIR, BKB), BF)


def attention_backward(lens, qt, dot_t, lse, delta, k, v, kt, pair0):
    nq = qt.shape[1]
    rows = k.shape[0]
    off = pair0
    across = pl.BlockSpec((PAIR, nq), lambda p, s: (off, 0))
    stat = pl.BlockSpec((2, 1, nq), lambda p, s: (off, 0, 0))
    keys = pl.BlockSpec((rows, PAIR), lambda p, s: (0, off))
    keys_t = pl.BlockSpec((PAIR, rows), lambda p, s: (off, 0))
    spec = pltpu.PrefetchScalarGridSpec(
        num_scalar_prefetch=1,
        grid=(1,),
        in_specs=[across, across, stat, stat, keys, keys, keys_t],
        out_specs=[pl.BlockSpec((2, 2 * PAIR, rows // 2), lambda p, s: (0, 0, 0)),
                   pl.BlockSpec((2, 64, nq), lambda p, s: (0, 0, 0))],
        scratch_shapes=[pltpu.VMEM((2, PAIR, nq), BF), pltpu.VMEM((2, PAIR, nq), BF)])
    work = 2 * nq * rows
    return pl.pallas_call(
        bwd_kernel,
        out_shape=[jax.ShapeDtypeStruct((2, 2 * PAIR, rows // 2), BF), jax.ShapeDtypeStruct((2, 64, nq), F32)],
        grid_spec=spec,
        compiler_params=pltpu.CompilerParams(vmem_limit_bytes=40 << 20),
        cost_estimate=cost(work * 2000, 8 << 20, work),
        name="attn_bwd",
    )(lens, qt, dot_t, lse, delta, k, v, kt)


def pair_weights_kernel(dkv_ref, m0_ref, m1_ref, o_ref):
    step = pl.program_id(0)
    half = pl.num_programs(0) // 2

    @pl.when(step == 0)
    def _():
        o_ref[...] = dot(dkv_ref[...], m0_ref[...])

    @pl.when((step > 0) & (step < half))
    def _():
        o_ref[...] += dot(dkv_ref[...], m0_ref[...])

    @pl.when(step >= half)
    def _():
        o_ref[...] += dot(dkv_ref[...], m1_ref[...])


def pair_weights(dkv, mem, mem_near):
    _, width, rows = dkv.shape
    dim = mem.shape[1]
    block = 1024
    half = rows // block
    return pl.pallas_call(
        pair_weights_kernel,
        grid=(2 * half,),
        in_specs=[pl.BlockSpec((None, width, block), lambda i: (i // half, 0, i % half)),
                  pl.BlockSpec((block, dim), lambda i: (jnp.minimum(i, half - 1), 0)),
                  pl.BlockSpec((block, dim), lambda i: (jnp.maximum(i - half, 0), 0))],
        out_specs=pl.BlockSpec((width, dim), lambda i: (0, 0)),
        out_shape=jax.ShapeDtypeStruct((width, dim), F32),
        compiler_params=pltpu.CompilerParams(vmem_limit_bytes=24 << 20),
        cost_estimate=cost(4 * rows * dim * width, 8 << 20),
        name="pair_weights",
    )(dkv, mem, mem_near)


def combine_kernel(a_ref, b_ref, o_ref, ob_ref, lse_ref):
    for h in range(2):
        ma, mb = a_ref[h, 64:65, :], b_ref[h, 64:65, :]
        top = jnp.maximum(ma, mb)
        ea, eb = jnp.exp(ma - top), jnp.exp(mb - top)
        den = a_ref[h, 65:66, :] * ea + b_ref[h, 65:66, :] * eb
        o = (a_ref[h, :64, :] * ea + b_ref[h, :64, :] * eb) / den
        o_ref[h] = o
        ob_ref[h * 64:(h + 1) * 64, :] = o.astype(BF)
        lse_ref[h] = top + jnp.log(den)


def combine(a, b):
    _, rows, nq = a.shape
    fix = lambda *shape: pl.BlockSpec(shape, lambda i: (0,) * len(shape))
    return pl.pallas_call(
        combine_kernel,
        grid=(1,),
        in_specs=[fix(2, rows, nq)] * 2,
        out_specs=[fix(2, 64, nq), fix(PAIR, nq), fix(2, 1, nq)],
        out_shape=[jax.ShapeDtypeStruct((2, 64, nq), F32), jax.ShapeDtypeStruct((PAIR, nq), BF),
                   jax.ShapeDtypeStruct((2, 1, nq), F32)],
        compiler_params=pltpu.CompilerParams(vmem_limit_bytes=16 << 20),
        cost_estimate=cost(500 * nq, 2 << 20),
        name="combine",
    )(a, b)


def sum_queries_kernel(a0_ref, a1_ref, a2_ref, b0_ref, b1_ref, b2_ref, o_ref):
    for i, (a, b) in enumerate(((a0_ref, b0_ref), (a1_ref, b1_ref), (a2_ref, b2_ref))):
        for h in range(2):
            at = i * PAIR + h * 64
            o_ref[at:at + 64, :] = ((a[h] + b[h]) * 0.125).astype(BF)


def sum_queries(mine, far):
    nq = mine[0].shape[2]
    part = pl.BlockSpec((2, 64, nq // 2), lambda i: (0, 0, i))
    return pl.pallas_call(
        sum_queries_kernel,
        grid=(2,),
        in_specs=[part] * 6,
        out_specs=pl.BlockSpec((3 * PAIR, nq // 2), lambda i: (0, i)),
        out_shape=jax.ShapeDtypeStruct((3 * PAIR, nq), BF),
        compiler_params=pltpu.CompilerParams(vmem_limit_bytes=16 << 20),
        cost_estimate=cost(1000 * nq, 4 << 20),
        name="sum_queries",
    )(*mine, *far)


def mlp_kernel(h_ref, g_ref, gain_ref, w1_ref, w3_ref, w2_ref,
               n2t_ref, gt_ref, dgate_ref, dup_ref, ut_ref, dh_ref, dhb_ref, gn_ref, n2_ref, acc_ref):
    step = pl.program_id(0)
    rows = h_ref.shape[0]
    chunk = 256

    @pl.when(step == 0)
    def _():
        for c in range(rows // chunk):
            rs = slice(c * chunk, (c + 1) * chunk)
            hid = h_ref[rs, :].astype(F32)
            n2 = (hid * inv_rms(hid) * gain_ref[...]).astype(BF)
            n2_ref[rs, :] = n2
            n2t_ref[:, rs] = n2.T
            gt_ref[rs, :] = g_ref[rs, :].astype(BF)
        acc_ref[...] = jnp.zeros(acc_ref.shape, F32)

    w1, w3, w2 = w1_ref[...], w3_ref[...], w2_ref[...]
    for c in range(rows // chunk):
        rs = slice(c * chunk, (c + 1) * chunk)
        n2 = n2_ref[rs, :]
        gate = dot(n2, w1)
        up = dot(n2, w3)
        ga = dot_nt(gt_ref[rs, :], w2)
        sig = 0.5 * jnp.tanh(0.5 * gate) + 0.5
        act = gate * sig
        ut_ref[:, rs] = (act * up).astype(BF).T
        dup = (ga * act).astype(BF)
        dgate = (ga * up * (sig + act * (1.0 - sig))).astype(BF)
        dup_ref[rs, :] = dup
        dgate_ref[rs, :] = dgate
        acc_ref[rs, :] += dot_nt(dgate, w1) + dot_nt(dup, w3)

    @pl.when(step == pl.num_programs(0) - 1)
    def _():
        total = jnp.zeros(gn_ref.shape, F32)
        for c in range(rows // chunk):
            rs = slice(c * chunk, (c + 1) * chunk)
            hid = h_ref[rs, :].astype(F32)
            inv = inv_rms(hid)
            unit = hid * inv
            grad = acc_ref[rs, :]
            total += jnp.sum(grad * unit, axis=0, keepdims=True)
            dh = g_ref[rs, :] + norm_back(unit, inv, gain_ref[...], grad)
            dh_ref[rs, :] = dh
            dhb_ref[rs, :] = dh.astype(BF)
        gn_ref[...] = total


def mlp(hidden, g_all, gain, w_gate, w_up, w_down):
    rows, dim = hidden.shape
    ff = w_gate.shape[1]
    fix = lambda *shape: pl.BlockSpec(shape, lambda i: (0,) * len(shape))
    wide = pl.BlockSpec((dim, FFB), lambda i: (0, i))
    tall = pl.BlockSpec((FFB, dim), lambda i: (i, 0))
    act = pl.BlockSpec((rows, FFB), lambda i: (0, i))
    act_t = pl.BlockSpec((FFB, rows), lambda i: (i, 0))
    return pl.pallas_call(
        mlp_kernel,
        grid=(ff // FFB,),
        in_specs=[fix(rows, dim), fix(rows, dim), fix(1, dim), wide, wide, tall],
        out_specs=[fix(dim, rows), fix(rows, dim), act, act, act_t, fix(rows, dim), fix(rows, dim), fix(1, dim)],
        out_shape=[jax.ShapeDtypeStruct((dim, rows), BF), jax.ShapeDtypeStruct((rows, dim), BF),
                   jax.ShapeDtypeStruct((rows, ff), BF), jax.ShapeDtypeStruct((rows, ff), BF),
                   jax.ShapeDtypeStruct((ff, rows), BF), jax.ShapeDtypeStruct((rows, dim), F32),
                   jax.ShapeDtypeStruct((rows, dim), BF), jax.ShapeDtypeStruct((1, dim), F32)],
        scratch_shapes=[pltpu.VMEM((rows, dim), BF), pltpu.VMEM((rows, dim), F32)],
        compiler_params=pltpu.CompilerParams(vmem_limit_bytes=56 << 20),
        cost_estimate=cost(10 * rows * dim * ff, 40 << 20, rows * ff),
        name="mlp",
    )(hidden, g_all, gain, w_gate, w_up, w_down)


def mlp_weights_kernel(n2t_ref, gt_ref, dgate_ref, dup_ref, ut_ref, n2t2_ref, gt2_ref, dgate2_ref, dup2_ref, ut2_ref,
                       g1_ref, g3_ref, g2_ref):
    g1_ref[...] = dot(n2t_ref[...], dgate_ref[...]) + dot(n2t2_ref[...], dgate2_ref[...])
    g3_ref[...] = dot(n2t_ref[...], dup_ref[...]) + dot(n2t2_ref[...], dup2_ref[...])
    g2_ref[...] = dot(ut_ref[...], gt_ref[...]) + dot(ut2_ref[...], gt2_ref[...])


def mlp_weights(factors, factors_near):
    dim, rows = factors[0].shape
    ff = factors[2].shape[1]
    fix = lambda *shape: pl.BlockSpec(shape, lambda i: (0,) * len(shape))
    act = pl.BlockSpec((rows, FFB), lambda i: (0, i))
    wide = pl.BlockSpec((dim, FFB), lambda i: (0, i))
    ins = [fix(dim, rows), fix(rows, dim), act, act, pl.BlockSpec((FFB, rows), lambda i: (i, 0))]
    return pl.pallas_call(
        mlp_weights_kernel,
        grid=(ff // FFB,),
        in_specs=ins + ins,
        out_specs=[wide, wide, pl.BlockSpec((FFB, dim), lambda i: (i, 0))],
        out_shape=[jax.ShapeDtypeStruct((dim, ff), F32)] * 2 + [jax.ShapeDtypeStruct((ff, dim), F32)],
        compiler_params=pltpu.CompilerParams(vmem_limit_bytes=60 << 20),
        cost_estimate=cost(12 * rows * dim * ff, 50 << 20),
        name="mlp_weights",
    )(*factors, *factors_near)


def memory_kernel(core_ref, a0_ref, a1_ref, a2_ref, b0_ref, b1_ref, b2_ref, wk_ref, wv_ref, o_ref):
    core = core_ref[0]
    total = None
    for who, refs in ((core, (a0_ref, a1_ref, a2_ref)), (1 - core, (b0_ref, b1_ref, b2_ref))):
        for i, ref in enumerate(refs):
            rows = pl.ds(pl.multiple_of((who * 3 + i) * PAIR, PAIR), PAIR)
            part = dot(ref[...].T, jnp.concatenate([wk_ref[rows, :], wv_ref[rows, :]], axis=0))
            total = part if total is None else total + part
    o_ref[...] = total


def memory_grad(core, mine, near, wkt, wvt):
    rows = mine[0].shape[-1]
    dim = wkt.shape[1]
    block = pl.BlockSpec((None, 2 * PAIR, MB), lambda i, s: (0, 0, i))
    block2 = pl.BlockSpec((2 * PAIR, MB), lambda i, s: (0, i))
    whole = pl.BlockSpec(wkt.shape, lambda i, s: (0, 0))
    return pl.pallas_call(
        memory_kernel,
        out_shape=jax.ShapeDtypeStruct((rows, dim), F32),
        grid_spec=pltpu.PrefetchScalarGridSpec(
            num_scalar_prefetch=1, grid=(rows // MB,),
            in_specs=[block] * 3 + [block2] * 3 + [whole, whole],
            out_specs=pl.BlockSpec((MB, dim), lambda i, s: (i, 0))),
        compiler_params=pltpu.CompilerParams(vmem_limit_bytes=32 << 20),
        cost_estimate=cost(4 * rows * dim * dim, 16 << 20),
        name="memory_grad",
    )(core, *mine, *near, wkt, wvt)


def half_index(i, core):
    return i + core - 2 * i * core


def out_proj_kernel(core_ref, mine_ref, near0_ref, near1_ref, dh_ref, o_ref):
    half = near0_ref.shape[1]

    @pl.when(pl.program_id(0) == 0)
    def _():
        o_ref[...] = dot(mine_ref[...], dh_ref[...])

    @pl.when(pl.program_id(0) == 1)
    def _():
        o_ref[...] = dot(near0_ref[...], dh_ref[:half, :]) + dot(near1_ref[...], dh_ref[half:, :])


def out_proj_grad(core, mine, near, dh):
    width, rows = mine.shape
    dim = dh.shape[1]
    whole = pl.BlockSpec((width, rows), lambda i, s: (0, 0))
    part = pl.BlockSpec((width, rows // 2), lambda i, s: (0, 0))
    return pl.pallas_call(
        out_proj_kernel,
        out_shape=jax.ShapeDtypeStruct((2 * width, dim), F32),
        grid_spec=pltpu.PrefetchScalarGridSpec(
            num_scalar_prefetch=1, grid=(2,),
            in_specs=[whole, part, part, pl.BlockSpec((rows, dim), lambda i, s: (0, 0))],
            out_specs=pl.BlockSpec((width, dim), lambda i, s: (half_index(i, s[0]), 0))),
        compiler_params=pltpu.CompilerParams(vmem_limit_bytes=24 << 20),
        cost_estimate=cost(4 * rows * dim * width, 6 << 20),
        name="out_proj_grad",
    )(core, mine, *near, dh)


def query_grad_kernel(place_ref, mine_ref, near_ref, n1_ref, wq_ref, x_ref, dh_ref, gain_ref,
                      gw_ref, gx_ref, gn_ref, acc_ref):
    half = acc_ref.shape[0] // 2

    @pl.when(pl.program_id(0) == 0)
    def _():
        gw_ref[...] = dot(mine_ref[...], n1_ref[...])
        acc_ref[...] = dot(mine_ref[...].T, wq_ref[...])

    @pl.when(pl.program_id(0) == 1)
    def _():
        first, second = near_ref[:, half:], near_ref[:, :half]
        gw_ref[...] = dot(first, n1_ref[:half, :]) + dot(second, n1_ref[half:, :])
        acc_ref[:half, :] += dot(first.T, wq_ref[...])
        acc_ref[half:, :] += dot(second.T, wq_ref[...])

    @pl.when(pl.program_id(0) == 1)
    def _():
        rows = gx_ref.shape[0]
        total = jnp.zeros(gn_ref.shape, F32)
        for c in range(acc_ref.shape[0] // rows):
            rs = slice(c * rows, (c + 1) * rows)
            x = x_ref[rs, :].astype(F32)
            total += jnp.sum(acc_ref[rs, :] * (x * inv_rms(x)), axis=0, keepdims=True)
        gn_ref[...] = total
        own = pl.ds(pl.multiple_of(place_ref[0] * rows, rows), rows)
        x = x_ref[own, :].astype(F32)
        inv = inv_rms(x)
        gx_ref[...] = dh_ref[...] + norm_back(x * inv, inv, gain_ref[...], acc_ref[own, :])


def query_grad(place, mine, near, n1, wqt, x_all, d_hid, gain, rows):
    width, total = mine.shape
    dim = n1.shape[1]
    fix = lambda *shape: pl.BlockSpec(shape, lambda i, s: (0,) * len(shape))
    half = pl.BlockSpec((width, dim), lambda i, s: (half_index(i, s[4]), 0))
    return pl.pallas_call(
        query_grad_kernel,
        out_shape=[jax.ShapeDtypeStruct((2 * width, dim), F32), jax.ShapeDtypeStruct((rows, dim), F32),
                   jax.ShapeDtypeStruct((1, dim), F32)],
        grid_spec=pltpu.PrefetchScalarGridSpec(
            num_scalar_prefetch=1, grid=(2,),
            in_specs=[fix(width, total), fix(width, total), fix(total, dim), half, fix(total, dim),
                      pl.BlockSpec((rows, dim), lambda i, s: (s[0], 0)), fix(1, dim)],
            out_specs=[half, fix(rows, dim), fix(1, dim)],
            scratch_shapes=[pltpu.VMEM((total, dim), F32)]),
        compiler_params=pltpu.CompilerParams(vmem_limit_bytes=32 << 20),
        cost_estimate=cost(8 * total * dim * width, 10 << 20),
        name="query_grad",
    )(place, mine, near, n1, wqt, x_all, d_hid, gain)


def key_weights_kernel(core_ref, *refs):
    gk_ref, gv_ref = refs[-2:]
    count = (len(refs) - 2) // 2
    for at in range(count):
        @pl.when(pl.program_id(0) == at)
        def _():
            a, b = refs[at], refs[count + at]
            gk_ref[...] = a[:PAIR, :] + b[:PAIR, :]
            gv_ref[...] = a[PAIR:, :] + b[PAIR:, :]


def key_weights(core, parts, others):
    pairs = len(parts) // 2
    dim = parts[0].shape[1]
    out = pl.BlockSpec((PAIR, dim), lambda i, s: (half_index(i // pairs, s[0]) * pairs + i % pairs, 0))
    return pl.pallas_call(
        key_weights_kernel,
        out_shape=[jax.ShapeDtypeStruct((2 * pairs * PAIR, dim), F32)] * 2,
        grid_spec=pltpu.PrefetchScalarGridSpec(
            num_scalar_prefetch=1, grid=(2 * pairs,),
            in_specs=[pl.BlockSpec((2 * PAIR, dim), lambda i, s: (0, 0))] * (4 * pairs),
            out_specs=[out, out]),
        compiler_params=pltpu.CompilerParams(vmem_limit_bytes=24 << 20),
        cost_estimate=cost(4 * pairs * PAIR * dim, 10 << 20),
        name="key_weights",
    )(core, *parts, *others)


def inv_rms(tensor):
    return lax.rsqrt(jnp.mean(tensor * tensor, axis=-1, keepdims=True) + 1e-6)


def norm_back(unit, inv, gain, grad):
    scaled = grad * gain
    return inv * (scaled - unit * jnp.mean(scaled * unit, axis=-1, keepdims=True))


def mm(a, b, ca, cb, dtype=F32):
    out = lax.dot_general(a, b, (((ca,), (cb,)), ((), ())), preferred_element_type=F32)
    return out if dtype == F32 else out.astype(dtype)


def solution(mesh):
    n = mesh.shape['seq']
    near = [(i, i ^ 1) for i in range(n)]
    far = [(i, i ^ 2) for i in range(n)]
    row_spec = P(('data', 'seq'), None)
    weight_spec = P()
    part_vec = P('data')
    part_mat = P('data', None)
    part_cube = P('data', None, None)

    def to_near(a):
        return lax.ppermute(a, 'seq', near)

    def to_far(a):
        return lax.ppermute(a, 'seq', far)

    def device_work(dec_in, memory, mem_len, grad_out, norm_attn, wq, wk, wv, wo, norm_mlp, w_gate, w_up, w_down):
        rows, dim = dec_in.shape
        m_rows = memory.shape[0]
        heads, head = wq.shape[1], wq.shape[2]
        mine = heads // 2
        width = mine * head
        dev = lax.axis_index('seq')
        core = lax.rem(dev, 2)
        core1 = core.reshape(1).astype(jnp.int32)
        wqt, wkt, wvt = (w.transpose(1, 2, 0).reshape(heads * head, dim) for w in (wq, wk, wv))
        wo2 = wo.reshape(heads * head, dim)
        lens = jnp.stack([jnp.clip(mem_len[0] - i * m_rows, 0, m_rows) for i in (dev, dev ^ 1)]).astype(jnp.int32)
        chip = dev // 2
        place = jnp.stack([chip, 2 + chip, 1 - chip, 3 - chip, core]).astype(jnp.int32)
        gain1 = norm_attn.astype(F32).reshape(1, dim)
        gain2 = norm_mlp.astype(F32).reshape(1, dim)

        def gather_parts(a):
            across = to_far(a)
            beside = to_near(a)
            return a, beside, across, to_near(across)

        x_parts = gather_parts(dec_in)
        mem_near = to_near(memory)
        g_parts = (grad_out, to_far(grad_out))

        first = project(core1, memory, wkt, wvt, 0, ())
        x_all_b, n1, _, qt_s = queries(place, x_parts, gain1, wqt)
        k, v, kt, vt = project(core1, mem_near, wkt, wvt, 1, first)

        pairs = mine // 2
        pieces = [(pair, 0, n * rows) for pair in range(pairs - 1)]
        pieces += [(pairs - 1, 0, n * rows // 2), (pairs - 1, n * rows // 2, n * rows // 2)]
        outs, lses = [], []
        parts = []
        for pair, at, count in pieces:
            part = attention_forward(lens, qt_s, k, vt, pair, 1, at, count)
            parts.append((part, to_far(part)))
        outs_b = []
        for a, b in parts:
            o_piece, ob_piece, lse_piece = combine(a, b)
            outs.append(o_piece)
            outs_b.append(ob_piece)
            lses.append(lse_piece)
        for pieces_of, axis in ((outs, 2), (outs_b, 1), (lses, 2)):
            pieces_of[-2:] = [jnp.concatenate(pieces_of[-2:], axis=axis)]
        g_half = place_rows(place, g_parts)
        o_t = jnp.concatenate(outs, axis=0)
        lse = jnp.concatenate(lses, axis=0)
        o_t_b = jnp.concatenate(outs_b, axis=0)
        half = n * rows // 2
        o_t_first, o_t_second = o_t_b[:, :half], o_t_b[:, half:]
        o_near_first = to_near(o_t_second)

        def half_rows(w, who):
            return lax.dynamic_slice(w, (who * width, 0), (width, dim))

        wo_m, wo_n = half_rows(wo2, core), half_rows(wo2, 1 - core)
        hidden = (x_all_b[:half].astype(F32) + mm(o_t_first, wo_m, 0, 0) + mm(o_near_first, wo_n, 0, 0)).astype(BF)

        n2t, g_top, d_gate, d_up, act_t, d_hid, d_hid_half, g_norm_half = mlp(
            hidden, g_half, gain2, w_gate, w_up, w_down)
        d_hid_b = jnp.concatenate([d_hid_half, to_near(d_hid_half)], axis=0)
        factors = (n2t, g_top, d_gate, d_up, act_t)
        factors_near = tuple(to_near(a) for a in factors)
        o_near_second = to_near(o_t_first)
        g_norm_mlp = g_norm_half + to_near(g_norm_half)

        do_t_f = mm(wo_m, d_hid_b, 1, 1)
        delta = jnp.sum(do_t_f.reshape(mine, head, n * rows) * o_t, axis=1, keepdims=True)
        do_t = do_t_f.astype(BF)
        dkvs, dkvs_near, dqs, dws = [], [], [], []
        lens_now = lens
        for pair in range(pairs):
            dkv, dqt = attention_backward(lens_now, qt_s, do_t, lse, delta, k, v, kt, pair)
            dqs.append((dqt, to_far(dqt)))
            dw = pair_weights(dkv, memory, mem_near)
            dws.append((dw, to_far(dw)))
            dkvs.append(dkv)
            dkvs_near.append(to_near(dkv[1]))
            lens_now, dw_last = lax.optimization_barrier((lens, dw))

        act_t, _ = lax.optimization_barrier((act_t, dw_last))
        factors = (n2t, g_top, d_gate, d_up, act_t)
        g_gate, g_up, g_down = mlp_weights(factors, factors_near)
        g_mem = memory_grad(core1, dkvs, dkvs_near, wkt, wvt)

        def as_weight(rows_by_dim):
            return rows_by_dim.reshape(heads, head, dim).transpose(2, 0, 1)

        g_wo = out_proj_grad(core1, o_t_b, (o_near_first, o_near_second), d_hid_b).reshape(heads, head, dim)

        dqt_b = sum_queries([a for a, _ in dqs], [b for _, b in dqs])
        dqt_near = to_near(dqt_b)
        g_wqt, g_dec, g_norm_attn = query_grad(place, dqt_b, dqt_near, n1, wqt, x_all_b, d_hid, gain1, rows)

        mine_near = []
        for a, b in dws:
            mine_near.append((to_near(a), to_near(b)))
        g_wkt, g_wvt = key_weights(core1, [a for a, _ in dws] + [a for a, _ in mine_near],
                                   [b for _, b in dws] + [b for _, b in mine_near])
        g_wq, g_wk, g_wv = as_weight(g_wqt), as_weight(g_wkt), as_weight(g_wvt)
        return (g_dec, g_mem, g_norm_attn.reshape(dim), g_wq, g_wk, g_wv, g_wo, g_norm_mlp.reshape(dim), g_gate, g_up, g_down)


    return jax.shard_map(device_work, mesh=mesh,
                         in_specs=(row_spec, row_spec, part_vec, row_spec) + (weight_spec,) * 9,
                         out_specs=(row_spec, row_spec, part_vec, part_cube, part_cube, part_cube, part_cube,
                                    part_vec, part_mat, part_mat, part_mat),
                         check_vma=False)
```

```python
import jax
import jax.numpy as jnp
from jax import lax
from jax.experimental import pallas as pl
from jax.experimental.pallas import tpu as pltpu
from jax.sharding import PartitionSpec as P


LOG2E = 1.4426950408889634
NEG = -1e30
BF = jnp.bfloat16
F32 = jnp.float32
FKB = 512
FQB = 512
BKB = 512
BQB = 256
WKB = 1024
PAIR = 128
OROWS = 72
FFB = 512
WFB = 1024
MB = 512


def dot(a, b):
    return jnp.dot(a, b, preferred_element_type=F32)


def dot_nt(a, b):
    return lax.dot_general(a, b, (((1,), (1,)), ((), ())), preferred_element_type=F32)


def cost(flops, bytes_accessed, exps=0):
    return pl.CostEstimate(flops=int(flops), bytes_accessed=int(bytes_accessed), transcendentals=int(exps))


def proj_kernel(core_ref, m0_ref, m1_ref, wk_ref, wv_ref, k_ref, v_ref, kt_ref, vt_ref):
    step = pl.program_id(0)
    half = pl.num_programs(0) // 2
    for seg, m_ref in enumerate((m0_ref, m1_ref)):
        @pl.when((step >= half) == (seg == 1))
        def _():
            m = m_ref[...]
            k = dot_nt(m, wk_ref[...]).astype(BF)
            v = dot_nt(m, wv_ref[...]).astype(BF)
            k_ref[...] = k
            v_ref[...] = v
            kt_ref[...] = k.T
            vt_ref[...] = v.T


def project(core, mem, mem_near, wkt, wvt):
    rows, dim = mem.shape
    width = wkt.shape[0] // 2
    half = rows // MB
    weights = pl.BlockSpec((width, dim), lambda i, s: (s[0], 0))
    down = pl.BlockSpec((MB, width), lambda i, s: (i, 0))
    across = pl.BlockSpec((width, MB), lambda i, s: (0, i))
    outs = [jax.ShapeDtypeStruct((2 * rows, width), BF)] * 2 + [jax.ShapeDtypeStruct((width, 2 * rows), BF)] * 2
    return pl.pallas_call(
        proj_kernel,
        out_shape=outs,
        grid_spec=pltpu.PrefetchScalarGridSpec(
            num_scalar_prefetch=1, grid=(2 * half,),
            in_specs=[pl.BlockSpec((MB, dim), lambda i, s: (jnp.minimum(i, half - 1), 0)),
                      pl.BlockSpec((MB, dim), lambda i, s: (jnp.maximum(i - half, 0), 0)), weights, weights],
            out_specs=[down, down, across, across]),
        compiler_params=pltpu.CompilerParams(vmem_limit_bytes=24 << 20),
        cost_estimate=cost(8 * rows * dim * width, 24 << 20),
        name="kv_proj",
    )(core, mem, mem_near, wkt, wvt)


def query_kernel(place_ref, x0_ref, x1_ref, x2_ref, x3_ref, gain_ref, wq_ref, x_ref, n_ref, q_ref, qt_ref):
    for part, src in enumerate((x0_ref, x1_ref, x2_ref, x3_ref)):
        @pl.when(pl.program_id(0) == part)
        def _():
            xb = src[...]
            x = xb.astype(F32)
            n1 = (x * inv_rms(x) * gain_ref[...]).astype(BF)
            q = dot_nt(n1, wq_ref[...]).astype(BF) * jnp.asarray(0.125, BF)
            x_ref[...] = xb
            n_ref[...] = n1
            q_ref[...] = q
            qt_ref[...] = q.T


def queries(place, parts, gain, wqt):
    rows, dim = parts[0].shape
    width = wqt.shape[0] // 2
    n = len(parts)
    whole = pl.BlockSpec((rows, dim), lambda i, s: (0, 0))
    put = pl.BlockSpec((rows, dim), lambda i, s: (s[i], 0))
    return pl.pallas_call(
        query_kernel,
        out_shape=[jax.ShapeDtypeStruct((n * rows, dim), BF)] * 2
                  + [jax.ShapeDtypeStruct((n * rows, width), BF), jax.ShapeDtypeStruct((width, n * rows), BF)],
        grid_spec=pltpu.PrefetchScalarGridSpec(
            num_scalar_prefetch=1, grid=(n,),
            in_specs=[whole] * n + [pl.BlockSpec((1, dim), lambda i, s: (0, 0)),
                                    pl.BlockSpec((width, dim), lambda i, s: (s[n], 0))],
            out_specs=[put, put, pl.BlockSpec((rows, width), lambda i, s: (s[i], 0)),
                       pl.BlockSpec((width, rows), lambda i, s: (0, s[i]))]),
        compiler_params=pltpu.CompilerParams(vmem_limit_bytes=24 << 20),
        cost_estimate=cost(2 * n * rows * dim * width, 6 << 20),
        name="queries",
    )(place, *parts, gain, wqt)


def place_kernel(place_ref, x0_ref, x1_ref, o_ref):
    for part, src in enumerate((x0_ref, x1_ref)):
        @pl.when(pl.program_id(0) == part)
        def _():
            o_ref[...] = src[...]


def place_rows(place, parts):
    rows, dim = parts[0].shape
    n = len(parts)
    return pl.pallas_call(
        place_kernel,
        out_shape=jax.ShapeDtypeStruct((n * rows, dim), parts[0].dtype),
        grid_spec=pltpu.PrefetchScalarGridSpec(
            num_scalar_prefetch=1, grid=(n,),
            in_specs=[pl.BlockSpec((rows, dim), lambda i, s: (0, 0))] * n,
            out_specs=pl.BlockSpec((rows, dim), lambda i, s: (s[2 * i], 0))),
        compiler_params=pltpu.CompilerParams(vmem_limit_bytes=16 << 20),
        cost_estimate=cost(n * rows * dim, 6 << 20),
        name="place_rows",
    )(place, *parts)


def fwd_kernel(len_ref, qt_ref, k_ref, vt_ref, o_ref, m_ref, l_ref, acc_ref, qz_ref, sa_ref, sb_ref):
    qb = qt_ref.shape[1]
    seg_rows = k_ref.shape[0] // 2
    half = lax.broadcasted_iota(jnp.int32, (PAIR, qb), 0) // 64
    for h in range(2):
        qz_ref[h] = jnp.where(half == h, qt_ref[...], jnp.zeros((), BF))
    m_ref[...] = jnp.full(m_ref.shape, NEG, F32)
    l_ref[...] = jnp.zeros(l_ref.shape, F32)
    acc_ref[...] = jnp.zeros(acc_ref.shape, F32)
    first = len_ref[0] // FKB
    total = first + len_ref[1] // FKB

    def base(t):
        t = jnp.clip(t, 0, jnp.maximum(total - 1, 0))
        return pl.multiple_of(jnp.where(t < first, t * FKB, seg_rows + (t - first) * FKB), FKB)

    def scores(row, s_ref):
        kb = k_ref[pl.ds(row, FKB), :]
        for h in range(2):
            s_ref[h] = dot(kb, qz_ref[h])

    def absorb(row, s_ref, count=None):
        rows = pl.ds(row, FKB)
        for h in range(2):
            st = s_ref[h]
            if count is not None:
                st = jnp.where(lax.broadcasted_iota(jnp.int32, st.shape, 0) < count, st, NEG)
            m_old = m_ref[h]
            m_new = jnp.maximum(m_old, jnp.max(st, axis=0, keepdims=True))
            p = jnp.exp2((st - m_new) * LOG2E)
            alpha = jnp.exp2((m_old - m_new) * LOG2E)
            l_ref[h] = l_ref[h] * alpha + jnp.sum(p, axis=0, keepdims=True)
            pv = dot(vt_ref[h * 64:(h + 1) * 64, rows], p.astype(BF))
            acc_ref[h] = acc_ref[h] * alpha + pv
            m_ref[h] = m_new

    scores(base(0), sa_ref)

    @pl.loop(0, total // 2)
    def _(i):
        scores(base(2 * i + 1), sb_ref)
        absorb(base(2 * i), sa_ref)
        scores(base(2 * i + 2), sa_ref)
        absorb(base(2 * i + 1), sb_ref)

    @pl.when(total % 2 == 1)
    def _():
        absorb(base(total - 1), sa_ref)

    @pl.loop(0, 2)
    def _(s):
        full = len_ref[s] // FKB
        rest = len_ref[s] - full * FKB

        @pl.when(rest > 0)
        def _():
            row = pl.multiple_of(s * seg_rows + full * FKB, FKB)
            scores(row, sa_ref)
            absorb(row, sa_ref, rest)

    for h in range(2):
        o_ref[h, 0:64, :] = acc_ref[h]
        o_ref[h, 64:72, :] = jnp.concatenate([m_ref[h], l_ref[h], jnp.zeros((6, qb), F32)], axis=0)


def attention_forward(lens, qt, k, vt, pair0, pairs, at, nq):
    q_off = at // FQB
    rows = k.shape[0]
    off = pair0
    spec = pltpu.PrefetchScalarGridSpec(
        num_scalar_prefetch=1,
        grid=(pairs, nq // FQB),
        in_specs=[
            pl.BlockSpec((PAIR, FQB), lambda p, i, s: (p + off, i + q_off)),
            pl.BlockSpec((rows, PAIR), lambda p, i, s: (0, p + off)),
            pl.BlockSpec((PAIR, rows), lambda p, i, s: (p + off, 0)),
        ],
        out_specs=pl.BlockSpec((2, OROWS, FQB), lambda p, i, s: (p, 0, i)),
        scratch_shapes=[
            pltpu.VMEM((2, 1, FQB), F32), pltpu.VMEM((2, 1, FQB), F32), pltpu.VMEM((2, 64, FQB), F32),
            pltpu.VMEM((2, PAIR, FQB), BF), pltpu.VMEM((2, FKB, FQB), F32), pltpu.VMEM((2, FKB, FQB), F32),
        ])
    work = 2 * pairs * nq * rows
    return pl.pallas_call(
        fwd_kernel,
        out_shape=jax.ShapeDtypeStruct((2 * pairs, OROWS, nq), F32),
        grid_spec=spec,
        compiler_params=pltpu.CompilerParams(vmem_limit_bytes=24 << 20),
        cost_estimate=cost(work * 1024, 4 << 20, work),
        name="attn_fwd",
    )(lens, qt, k, vt)


def bwd_kernel(len_ref, qt_ref, dot_ref, lse_ref, dl_ref, k_ref, v_ref, kt_ref, m0_ref, m1_ref,
               dkv0_ref, dkv1_ref, dqt_ref, dw_ref, qzt_ref, dozt_ref, dkv_ref, m_ref, sems):
    copies = [pltpu.make_async_copy(src, m_ref.at[i], sems.at[i]) for i, src in enumerate((m0_ref, m1_ref))]
    for copy in copies:
        copy.start()
    nq = qt_ref.shape[1]
    seg_rows = k_ref.shape[0] // 2
    blocks = seg_rows // BKB
    half = lax.broadcasted_iota(jnp.int32, (PAIR, nq), 0) // 64
    zero = jnp.zeros((), BF)
    for h in range(2):
        qzt_ref[h] = jnp.where(half == h, qt_ref[...], zero)
        dozt_ref[h] = jnp.where(half == h, dot_ref[...], zero)
    dqt_ref[...] = jnp.zeros(dqt_ref.shape, F32)

    def step(seg, j, count):
        cols = pl.ds(pl.multiple_of(j * BKB, BKB), BKB)
        allc = pl.ds(pl.multiple_of(seg * seg_rows + j * BKB, BKB), BKB)
        kb, vb = k_ref[allc, :], v_ref[allc, :]
        chunks = [(h, slice(c * BQB, (c + 1) * BQB)) for h in range(2) for c in range(nq // BQB)]

        def products(h, qs):
            return dot(kb, qzt_ref[h, :, qs]), dot(vb, dozt_ref[h, :, qs])

        ahead = products(*chunks[0])
        for i, (h, qs) in enumerate(chunks):
            st, dp = ahead
            if i + 1 < len(chunks):
                ahead = products(*chunks[i + 1])
            hs = slice(h * 64, (h + 1) * 64)
            if qs.start == 0:
                dk = jnp.zeros((64, BKB), F32)
                dv = jnp.zeros((64, BKB), F32)
            p = jnp.exp2((st - lse_ref[h, :, qs]) * LOG2E)
            if count is not None:
                p = jnp.where(lax.broadcasted_iota(jnp.int32, st.shape, 0) < count, p, 0.0)
            ds = (p * (dp - dl_ref[h, :, qs])).astype(BF)
            dv = dv + dot_nt(dot_ref[hs, qs], p.astype(BF))
            dk = dk + dot_nt(qt_ref[hs, qs], ds)
            dqt_ref[h, :, qs] += dot(kt_ref[hs, allc], ds)
            if qs.stop == nq:
                dkv_ref[seg, hs, cols] = dk.astype(BF)
                dkv_ref[seg, PAIR + h * 64:PAIR + (h + 1) * 64, cols] = dv.astype(BF)

    first = len_ref[0] // BKB

    @pl.loop(0, first + len_ref[1] // BKB)
    def _(t):
        seg = jnp.where(t < first, 0, 1)
        step(seg, t - seg * first, None)

    @pl.loop(0, 2)
    def _(seg):
        full = len_ref[seg] // BKB
        rest = len_ref[seg] - full * BKB

        @pl.when(rest > 0)
        def _():
            step(seg, full, rest)

        @pl.loop(full + jnp.where(rest > 0, 1, 0), blocks)
        def _(j):
            cols = pl.ds(pl.multiple_of(j * BKB, BKB), BKB)
            dkv_ref[seg, :, cols] = jnp.zeros((2 * PAIR, BKB), BF)

    dw_ref[...] = jnp.zeros(dw_ref.shape, F32)
    for seg, copy in enumerate(copies):
        copy.wait()

        @pl.loop(0, (len_ref[seg] + WKB - 1) // WKB)
        def _(j):
            at = pl.ds(pl.multiple_of(j * WKB, WKB), WKB)
            dw_ref[...] += dot(dkv_ref[seg, :, at], m_ref[seg, at, :])

    dkv0_ref[...] = dkv_ref[0]
    dkv1_ref[...] = dkv_ref[1]


def attention_backward(lens, qt, dot_t, lse, delta, k, v, kt, mem, mem_near, pair0):
    nq = qt.shape[1]
    rows = k.shape[0]
    off = pair0
    across = pl.BlockSpec((PAIR, nq), lambda p, s: (off, 0))
    stat = pl.BlockSpec((2, 1, nq), lambda p, s: (off, 0, 0))
    keys = pl.BlockSpec((rows, PAIR), lambda p, s: (0, off))
    keys_t = pl.BlockSpec((PAIR, rows), lambda p, s: (off, 0))
    spec = pltpu.PrefetchScalarGridSpec(
        num_scalar_prefetch=1,
        grid=(1,),
        in_specs=[across, across, stat, stat, keys, keys, keys_t] + [pl.BlockSpec(memory_space=pltpu.HBM)] * 2,
        out_specs=[pl.BlockSpec((2 * PAIR, rows // 2), lambda p, s: (0, 0)),
                   pl.BlockSpec((2 * PAIR, rows // 2), lambda p, s: (0, 0)),
                   pl.BlockSpec((2, 64, nq), lambda p, s: (0, 0, 0)),
                   pl.BlockSpec((2 * PAIR, mem.shape[1]), lambda p, s: (0, 0))],
        scratch_shapes=[pltpu.VMEM((2, PAIR, nq), BF), pltpu.VMEM((2, PAIR, nq), BF),
                        pltpu.VMEM((2, 2 * PAIR, rows // 2), BF), pltpu.VMEM((2,) + mem.shape, BF),
                        pltpu.SemaphoreType.DMA((2,))])
    work = 2 * nq * rows
    return pl.pallas_call(
        bwd_kernel,
        out_shape=[jax.ShapeDtypeStruct((2 * PAIR, rows // 2), BF)] * 2
                  + [jax.ShapeDtypeStruct((2, 64, nq), F32), jax.ShapeDtypeStruct((2 * PAIR, mem.shape[1]), F32)],
        grid_spec=spec,
        compiler_params=pltpu.CompilerParams(vmem_limit_bytes=40 << 20),
        cost_estimate=cost(work * 2000, 8 << 20, work),
        name="attn_bwd",
    )(lens, qt, dot_t, lse, delta, k, v, kt, mem, mem_near)


def combine_kernel(a_ref, b_ref, o_ref, ob_ref, lse_ref):
    for h in range(2):
        ma, mb = a_ref[h, 64:65, :], b_ref[h, 64:65, :]
        top = jnp.maximum(ma, mb)
        ea, eb = jnp.exp(ma - top), jnp.exp(mb - top)
        den = a_ref[h, 65:66, :] * ea + b_ref[h, 65:66, :] * eb
        o = (a_ref[h, :64, :] * ea + b_ref[h, :64, :] * eb) / den
        o_ref[h] = o
        ob_ref[h * 64:(h + 1) * 64, :] = o.astype(BF)
        lse_ref[h] = top + jnp.log(den)


def combine(a, b):
    _, rows, nq = a.shape
    fix = lambda *shape: pl.BlockSpec(shape, lambda i: (0,) * len(shape))
    return pl.pallas_call(
        combine_kernel,
        grid=(1,),
        in_specs=[fix(2, rows, nq)] * 2,
        out_specs=[fix(2, 64, nq), fix(PAIR, nq), fix(2, 1, nq)],
        out_shape=[jax.ShapeDtypeStruct((2, 64, nq), F32), jax.ShapeDtypeStruct((PAIR, nq), BF),
                   jax.ShapeDtypeStruct((2, 1, nq), F32)],
        compiler_params=pltpu.CompilerParams(vmem_limit_bytes=16 << 20),
        cost_estimate=cost(500 * nq, 2 << 20),
        name="combine",
    )(a, b)


def sum_queries_kernel(a0_ref, a1_ref, a2_ref, b0_ref, b1_ref, b2_ref, o_ref):
    for i, (a, b) in enumerate(((a0_ref, b0_ref), (a1_ref, b1_ref), (a2_ref, b2_ref))):
        for h in range(2):
            at = i * PAIR + h * 64
            o_ref[at:at + 64, :] = ((a[h] + b[h]) * 0.125).astype(BF)


def sum_queries(mine, far):
    nq = mine[0].shape[2]
    part = pl.BlockSpec((2, 64, nq // 2), lambda i: (0, 0, i))
    return pl.pallas_call(
        sum_queries_kernel,
        grid=(2,),
        in_specs=[part] * 6,
        out_specs=pl.BlockSpec((3 * PAIR, nq // 2), lambda i: (0, i)),
        out_shape=jax.ShapeDtypeStruct((3 * PAIR, nq), BF),
        compiler_params=pltpu.CompilerParams(vmem_limit_bytes=16 << 20),
        cost_estimate=cost(1000 * nq, 4 << 20),
        name="sum_queries",
    )(*mine, *far)


def mlp_kernel(h_ref, g_ref, gain_ref, w1_ref, w3_ref, w2_ref,
               n2t_ref, gt_ref, dgate_ref, dup_ref, ut_ref, dh_ref, dhb_ref, gn_ref, n2_ref, acc_ref):
    step = pl.program_id(0)
    rows = h_ref.shape[0]
    chunk = 256

    @pl.when(step == 0)
    def _():
        for c in range(rows // chunk):
            rs = slice(c * chunk, (c + 1) * chunk)
            hid = h_ref[rs, :].astype(F32)
            n2 = (hid * inv_rms(hid) * gain_ref[...]).astype(BF)
            n2_ref[rs, :] = n2
            n2t_ref[:, rs] = n2.T
            gt_ref[rs, :] = g_ref[rs, :].astype(BF)
        acc_ref[...] = jnp.zeros(acc_ref.shape, F32)

    w1, w3, w2 = w1_ref[...], w3_ref[...], w2_ref[...]
    for c in range(rows // chunk):
        rs = slice(c * chunk, (c + 1) * chunk)
        n2 = n2_ref[rs, :]
        gate = dot(n2, w1)
        up = dot(n2, w3)
        ga = dot_nt(gt_ref[rs, :], w2)
        sig = 0.5 * jnp.tanh(0.5 * gate) + 0.5
        act = gate * sig
        ut_ref[:, rs] = (act * up).astype(BF).T
        dup = (ga * act).astype(BF)
        dgate = (ga * up * (sig + act * (1.0 - sig))).astype(BF)
        dup_ref[rs, :] = dup
        dgate_ref[rs, :] = dgate
        acc_ref[rs, :] += dot_nt(dgate, w1) + dot_nt(dup, w3)

    @pl.when(step == pl.num_programs(0) - 1)
    def _():
        total = jnp.zeros(gn_ref.shape, F32)
        for c in range(rows // chunk):
            rs = slice(c * chunk, (c + 1) * chunk)
            hid = h_ref[rs, :].astype(F32)
            inv = inv_rms(hid)
            unit = hid * inv
            grad = acc_ref[rs, :]
            total += jnp.sum(grad * unit, axis=0, keepdims=True)
            dh = g_ref[rs, :] + norm_back(unit, inv, gain_ref[...], grad)
            dh_ref[rs, :] = dh
            dhb_ref[rs, :] = dh.astype(BF)
        gn_ref[...] = total


def mlp(hidden, g_all, gain, w_gate, w_up, w_down):
    rows, dim = hidden.shape
    ff = w_gate.shape[1]
    fix = lambda *shape: pl.BlockSpec(shape, lambda i: (0,) * len(shape))
    wide = pl.BlockSpec((dim, FFB), lambda i: (0, i))
    tall = pl.BlockSpec((FFB, dim), lambda i: (i, 0))
    act = pl.BlockSpec((rows, FFB), lambda i: (0, i))
    act_t = pl.BlockSpec((FFB, rows), lambda i: (i, 0))
    return pl.pallas_call(
        mlp_kernel,
        grid=(ff // FFB,),
        in_specs=[fix(rows, dim), fix(rows, dim), fix(1, dim), wide, wide, tall],
        out_specs=[fix(dim, rows), fix(rows, dim), act, act, act_t, fix(rows, dim), fix(rows, dim), fix(1, dim)],
        out_shape=[jax.ShapeDtypeStruct((dim, rows), BF), jax.ShapeDtypeStruct((rows, dim), BF),
                   jax.ShapeDtypeStruct((rows, ff), BF), jax.ShapeDtypeStruct((rows, ff), BF),
                   jax.ShapeDtypeStruct((ff, rows), BF), jax.ShapeDtypeStruct((rows, dim), F32),
                   jax.ShapeDtypeStruct((rows, dim), BF), jax.ShapeDtypeStruct((1, dim), F32)],
        scratch_shapes=[pltpu.VMEM((rows, dim), BF), pltpu.VMEM((rows, dim), F32)],
        compiler_params=pltpu.CompilerParams(vmem_limit_bytes=56 << 20),
        cost_estimate=cost(10 * rows * dim * ff, 40 << 20, rows * ff),
        name="mlp",
    )(hidden, g_all, gain, w_gate, w_up, w_down)


def mlp_weights_kernel(n2t_ref, gt_ref, dgate_ref, dup_ref, ut_ref, n2t2_ref, gt2_ref, dgate2_ref, dup2_ref, ut2_ref,
                       g1_ref, g3_ref, g2_ref):
    g1_ref[...] = dot(n2t_ref[...], dgate_ref[...]) + dot(n2t2_ref[...], dgate2_ref[...])
    g3_ref[...] = dot(n2t_ref[...], dup_ref[...]) + dot(n2t2_ref[...], dup2_ref[...])
    g2_ref[...] = dot(ut_ref[...], gt_ref[...]) + dot(ut2_ref[...], gt2_ref[...])


def mlp_weights(factors, factors_near):
    dim, rows = factors[0].shape
    ff = factors[2].shape[1]
    fix = lambda *shape: pl.BlockSpec(shape, lambda i: (0,) * len(shape))
    act = pl.BlockSpec((rows, WFB), lambda i: (0, i))
    wide = pl.BlockSpec((dim, WFB), lambda i: (0, i))
    ins = [fix(dim, rows), fix(rows, dim), act, act, pl.BlockSpec((WFB, rows), lambda i: (i, 0))]
    return pl.pallas_call(
        mlp_weights_kernel,
        grid=(ff // WFB,),
        in_specs=ins + ins,
        out_specs=[wide, wide, pl.BlockSpec((WFB, dim), lambda i: (i, 0))],
        out_shape=[jax.ShapeDtypeStruct((dim, ff), F32)] * 2 + [jax.ShapeDtypeStruct((ff, dim), F32)],
        compiler_params=pltpu.CompilerParams(vmem_limit_bytes=60 << 20),
        cost_estimate=cost(12 * rows * dim * ff, 50 << 20),
        name="mlp_weights",
    )(*factors, *factors_near)


def memory_kernel(core_ref, a0_ref, a1_ref, a2_ref, b0_ref, b1_ref, b2_ref, wk_ref, wv_ref, o_ref):
    core = core_ref[0]
    total = None
    for who, refs in ((core, (a0_ref, a1_ref, a2_ref)), (1 - core, (b0_ref, b1_ref, b2_ref))):
        for i, ref in enumerate(refs):
            rows = pl.ds(pl.multiple_of((who * 3 + i) * PAIR, PAIR), PAIR)
            part = dot(ref[...].T, jnp.concatenate([wk_ref[rows, :], wv_ref[rows, :]], axis=0))
            total = part if total is None else total + part
    o_ref[...] = total


def memory_grad(core, mine, near, wkt, wvt):
    rows = mine[0].shape[-1]
    dim = wkt.shape[1]
    block = pl.BlockSpec((2 * PAIR, MB), lambda i, s: (0, i))
    whole = pl.BlockSpec(wkt.shape, lambda i, s: (0, 0))
    return pl.pallas_call(
        memory_kernel,
        out_shape=jax.ShapeDtypeStruct((rows, dim), F32),
        grid_spec=pltpu.PrefetchScalarGridSpec(
            num_scalar_prefetch=1, grid=(rows // MB,),
            in_specs=[block] * 6 + [whole, whole],
            out_specs=pl.BlockSpec((MB, dim), lambda i, s: (i, 0))),
        compiler_params=pltpu.CompilerParams(vmem_limit_bytes=32 << 20),
        cost_estimate=cost(4 * rows * dim * dim, 16 << 20),
        name="memory_grad",
    )(core, *mine, *near, wkt, wvt)


def half_index(i, core):
    return i + core - 2 * i * core


def out_proj_kernel(core_ref, mine_ref, near0_ref, near1_ref, dh_ref, o_ref):
    half = near0_ref.shape[1]

    @pl.when(pl.program_id(0) == 0)
    def _():
        o_ref[...] = dot(mine_ref[...], dh_ref[...])

    @pl.when(pl.program_id(0) == 1)
    def _():
        o_ref[...] = dot(near0_ref[...], dh_ref[:half, :]) + dot(near1_ref[...], dh_ref[half:, :])


def out_proj_grad(core, mine, near, dh):
    width, rows = mine.shape
    dim = dh.shape[1]
    whole = pl.BlockSpec((width, rows), lambda i, s: (0, 0))
    part = pl.BlockSpec((width, rows // 2), lambda i, s: (0, 0))
    return pl.pallas_call(
        out_proj_kernel,
        out_shape=jax.ShapeDtypeStruct((2 * width, dim), F32),
        grid_spec=pltpu.PrefetchScalarGridSpec(
            num_scalar_prefetch=1, grid=(2,),
            in_specs=[whole, part, part, pl.BlockSpec((rows, dim), lambda i, s: (0, 0))],
            out_specs=pl.BlockSpec((width, dim), lambda i, s: (half_index(i, s[0]), 0))),
        compiler_params=pltpu.CompilerParams(vmem_limit_bytes=24 << 20),
        cost_estimate=cost(4 * rows * dim * width, 6 << 20),
        name="out_proj_grad",
    )(core, mine, *near, dh)


def query_grad_kernel(place_ref, mine_ref, near_ref, n1_ref, wq_ref, x_ref, dh_ref, gain_ref,
                      gw_ref, gx_ref, gn_ref, acc_ref):
    half = acc_ref.shape[0] // 2

    @pl.when(pl.program_id(0) == 0)
    def _():
        gw_ref[...] = dot(mine_ref[...], n1_ref[...])
        acc_ref[...] = dot(mine_ref[...].T, wq_ref[...])

    @pl.when(pl.program_id(0) == 1)
    def _():
        first, second = near_ref[:, half:], near_ref[:, :half]
        gw_ref[...] = dot(first, n1_ref[:half, :]) + dot(second, n1_ref[half:, :])
        acc_ref[:half, :] += dot(first.T, wq_ref[...])
        acc_ref[half:, :] += dot(second.T, wq_ref[...])

    @pl.when(pl.program_id(0) == 1)
    def _():
        rows = gx_ref.shape[0]
        total = jnp.zeros(gn_ref.shape, F32)
        for c in range(acc_ref.shape[0] // rows):
            rs = slice(c * rows, (c + 1) * rows)
            x = x_ref[rs, :].astype(F32)
            total += jnp.sum(acc_ref[rs, :] * (x * inv_rms(x)), axis=0, keepdims=True)
        gn_ref[...] = total
        own = pl.ds(pl.multiple_of(place_ref[0] * rows, rows), rows)
        x = x_ref[own, :].astype(F32)
        inv = inv_rms(x)
        gx_ref[...] = dh_ref[...] + norm_back(x * inv, inv, gain_ref[...], acc_ref[own, :])


def query_grad(place, mine, near, n1, wqt, x_all, d_hid, gain, rows):
    width, total = mine.shape
    dim = n1.shape[1]
    fix = lambda *shape: pl.BlockSpec(shape, lambda i, s: (0,) * len(shape))
    half = pl.BlockSpec((width, dim), lambda i, s: (half_index(i, s[4]), 0))
    return pl.pallas_call(
        query_grad_kernel,
        out_shape=[jax.ShapeDtypeStruct((2 * width, dim), F32), jax.ShapeDtypeStruct((rows, dim), F32),
                   jax.ShapeDtypeStruct((1, dim), F32)],
        grid_spec=pltpu.PrefetchScalarGridSpec(
            num_scalar_prefetch=1, grid=(2,),
            in_specs=[fix(width, total), fix(width, total), fix(total, dim), half, fix(total, dim),
                      pl.BlockSpec((rows, dim), lambda i, s: (s[0], 0)), fix(1, dim)],
            out_specs=[half, fix(rows, dim), fix(1, dim)],
            scratch_shapes=[pltpu.VMEM((total, dim), F32)]),
        compiler_params=pltpu.CompilerParams(vmem_limit_bytes=32 << 20),
        cost_estimate=cost(8 * total * dim * width, 10 << 20),
        name="query_grad",
    )(place, mine, near, n1, wqt, x_all, d_hid, gain)


def key_weights_kernel(core_ref, *refs):
    gk_ref, gv_ref = refs[-2:]
    count = (len(refs) - 2) // 2
    for at in range(count):
        @pl.when(pl.program_id(0) == at)
        def _():
            a, b = refs[at], refs[count + at]
            gk_ref[...] = a[:PAIR, :] + b[:PAIR, :]
            gv_ref[...] = a[PAIR:, :] + b[PAIR:, :]


def key_weights(core, parts, others):
    pairs = len(parts) // 2
    dim = parts[0].shape[1]
    out = pl.BlockSpec((PAIR, dim), lambda i, s: (half_index(i // pairs, s[0]) * pairs + i % pairs, 0))
    return pl.pallas_call(
        key_weights_kernel,
        out_shape=[jax.ShapeDtypeStruct((2 * pairs * PAIR, dim), F32)] * 2,
        grid_spec=pltpu.PrefetchScalarGridSpec(
            num_scalar_prefetch=1, grid=(2 * pairs,),
            in_specs=[pl.BlockSpec((2 * PAIR, dim), lambda i, s: (0, 0))] * (4 * pairs),
            out_specs=[out, out]),
        compiler_params=pltpu.CompilerParams(vmem_limit_bytes=24 << 20),
        cost_estimate=cost(4 * pairs * PAIR * dim, 10 << 20),
        name="key_weights",
    )(core, *parts, *others)


def inv_rms(tensor):
    return lax.rsqrt(jnp.mean(tensor * tensor, axis=-1, keepdims=True) + 1e-6)


def norm_back(unit, inv, gain, grad):
    scaled = grad * gain
    return inv * (scaled - unit * jnp.mean(scaled * unit, axis=-1, keepdims=True))


def mm(a, b, ca, cb, dtype=F32):
    out = lax.dot_general(a, b, (((ca,), (cb,)), ((), ())), preferred_element_type=F32)
    return out if dtype == F32 else out.astype(dtype)


def solution(mesh):
    n = mesh.shape['seq']
    near = [(i, i ^ 1) for i in range(n)]
    far = [(i, i ^ 2) for i in range(n)]
    row_spec = P(('data', 'seq'), None)
    weight_spec = P()
    part_vec = P('data')
    part_mat = P('data', None)
    part_cube = P('data', None, None)

    def to_near(a):
        return lax.ppermute(a, 'seq', near)

    def to_far(a):
        return lax.ppermute(a, 'seq', far)

    def device_work(dec_in, memory, mem_len, grad_out, norm_attn, wq, wk, wv, wo, norm_mlp, w_gate, w_up, w_down):
        rows, dim = dec_in.shape
        m_rows = memory.shape[0]
        heads, head = wq.shape[1], wq.shape[2]
        mine = heads // 2
        width = mine * head
        dev = lax.axis_index('seq')
        core = lax.rem(dev, 2)
        core1 = core.reshape(1).astype(jnp.int32)
        wqt, wkt, wvt = (w.transpose(1, 2, 0).reshape(heads * head, dim) for w in (wq, wk, wv))
        wo2 = wo.reshape(heads * head, dim)
        lens = jnp.stack([jnp.clip(mem_len[0] - i * m_rows, 0, m_rows) for i in (dev, dev ^ 1)]).astype(jnp.int32)
        chip = dev // 2
        place = jnp.stack([chip, 2 + chip, 1 - chip, 3 - chip, core]).astype(jnp.int32)
        gain1 = norm_attn.astype(F32).reshape(1, dim)
        gain2 = norm_mlp.astype(F32).reshape(1, dim)

        def gather_parts(a):
            across = to_far(a)
            beside = to_near(a)
            return a, beside, across, to_near(across)

        x_parts = gather_parts(dec_in)
        mem_near = to_near(memory)
        g_parts = (grad_out, to_far(grad_out))

        k, v, kt, vt = project(core1, memory, mem_near, wkt, wvt)
        x_all_b, n1, _, qt_s = queries(place, x_parts, gain1, wqt)

        pairs = mine // 2
        pieces = [(pair, 0, n * rows) for pair in range(pairs - 1)]
        pieces += [(pairs - 1, 0, n * rows // 2), (pairs - 1, n * rows // 2, n * rows // 2)]
        outs, lses = [], []
        parts = []
        for pair, at, count in pieces:
            part = attention_forward(lens, qt_s, k, vt, pair, 1, at, count)
            parts.append((part, to_far(part)))
        outs_b = []
        for a, b in parts:
            o_piece, ob_piece, lse_piece = combine(a, b)
            outs.append(o_piece)
            outs_b.append(ob_piece)
            lses.append(lse_piece)
        for pieces_of, axis in ((outs, 2), (outs_b, 1), (lses, 2)):
            pieces_of[-2:] = [jnp.concatenate(pieces_of[-2:], axis=axis)]
        g_half = place_rows(place, g_parts)
        o_t = jnp.concatenate(outs, axis=0)
        lse = jnp.concatenate(lses, axis=0)
        o_t_b = jnp.concatenate(outs_b, axis=0)
        half = n * rows // 2
        o_t_first, o_t_second = o_t_b[:, :half], o_t_b[:, half:]
        o_near_first = to_near(o_t_second)

        def half_rows(w, who):
            return lax.dynamic_slice(w, (who * width, 0), (width, dim))

        wo_m, wo_n = half_rows(wo2, core), half_rows(wo2, 1 - core)
        hidden = (x_all_b[:half].astype(F32) + mm(o_t_first, wo_m, 0, 0) + mm(o_near_first, wo_n, 0, 0)).astype(BF)

        n2t, g_top, d_gate, d_up, act_t, d_hid, d_hid_half, g_norm_half = mlp(
            hidden, g_half, gain2, w_gate, w_up, w_down)
        d_hid_b = jnp.concatenate([d_hid_half, to_near(d_hid_half)], axis=0)
        factors = (n2t, g_top, d_gate, d_up, act_t)
        factors_near = tuple(to_near(a) for a in factors)
        o_near_second = to_near(o_t_first)
        g_norm_mlp = g_norm_half + to_near(g_norm_half)

        do_t_f = mm(wo_m, d_hid_b, 1, 1)
        delta = jnp.sum(do_t_f.reshape(mine, head, n * rows) * o_t, axis=1, keepdims=True)
        do_t = do_t_f.astype(BF)
        dkvs, dkvs_near, dqs, dws = [], [], [], []
        lens_now = lens
        for pair in range(pairs):
            dkv, dkv_near, dqt, dw = attention_backward(
                lens_now, qt_s, do_t, lse, delta, k, v, kt, memory, mem_near, pair)
            dqs.append((dqt, to_far(dqt)))
            dws.append((dw, to_far(dw)))
            dkvs.append(dkv)
            dkvs_near.append(to_near(dkv_near))
            lens_now, dw_last = lax.optimization_barrier((lens, dw))

        act_t, _ = lax.optimization_barrier((act_t, dw_last))
        factors = (n2t, g_top, d_gate, d_up, act_t)
        g_gate, g_up, g_down = mlp_weights(factors, factors_near)
        g_mem = memory_grad(core1, dkvs, dkvs_near, wkt, wvt)

        def as_weight(rows_by_dim):
            return rows_by_dim.reshape(heads, head, dim).transpose(2, 0, 1)

        g_wo = out_proj_grad(core1, o_t_b, (o_near_first, o_near_second), d_hid_b).reshape(heads, head, dim)

        dqt_b = sum_queries([a for a, _ in dqs], [b for _, b in dqs])
        dqt_near = to_near(dqt_b)
        g_wqt, g_dec, g_norm_attn = query_grad(place, dqt_b, dqt_near, n1, wqt, x_all_b, d_hid, gain1, rows)

        mine_near = []
        for a, b in dws:
            mine_near.append((to_near(a), to_near(b)))
        g_wkt, g_wvt = key_weights(core1, [a for a, _ in dws] + [a for a, _ in mine_near],
                                   [b for _, b in dws] + [b for _, b in mine_near])
        g_wq, g_wk, g_wv = as_weight(g_wqt), as_weight(g_wkt), as_weight(g_wvt)
        return (g_dec, g_mem, g_norm_attn.reshape(dim), g_wq, g_wk, g_wv, g_wo, g_norm_mlp.reshape(dim), g_gate, g_up, g_down)


    return jax.shard_map(device_work, mesh=mesh,
                         in_specs=(row_spec, row_spec, part_vec, row_spec) + (weight_spec,) * 9,
                         out_specs=(row_spec, row_spec, part_vec, part_cube, part_cube, part_cube, part_cube,
                                    part_vec, part_mat, part_mat, part_mat),
                         check_vma=False)
```

```python
import jax
import jax.numpy as jnp
from jax import lax
from jax.experimental import pallas as pl
from jax.experimental.pallas import tpu as pltpu
from jax.sharding import PartitionSpec as P


LOG2E = 1.4426950408889634
NEG = -1e30
BF = jnp.bfloat16
F32 = jnp.float32
FKB = 512
FQB = 512
BKB = 512
BQB = 256
WKB = 1024
PAIR = 128
OROWS = 72
FFB = 512
WFB = 512
MB = 512


def dot(a, b):
    return jnp.dot(a, b, preferred_element_type=F32)


def dot_nt(a, b):
    return lax.dot_general(a, b, (((1,), (1,)), ((), ())), preferred_element_type=F32)


def cost(flops, bytes_accessed, exps=0):
    return pl.CostEstimate(flops=int(flops), bytes_accessed=int(bytes_accessed), transcendentals=int(exps))


def proj_kernel(core_ref, m_ref, wk_ref, wv_ref, *refs):
    k_ref, v_ref, kt_ref, vt_ref = refs[-4:]
    m = m_ref[...]
    k = dot_nt(m, wk_ref[...]).astype(BF)
    v = dot_nt(m, wv_ref[...]).astype(BF)
    k_ref[...] = k
    v_ref[...] = v
    kt_ref[...] = k.T
    vt_ref[...] = v.T


def project(core, mem, wkt, wvt, seg, before):
    rows, dim = mem.shape
    width = wkt.shape[0] // 2
    steps = rows // MB
    base = seg * steps
    weights = pl.BlockSpec((width, dim), lambda i, s: (s[0], 0))
    down = pl.BlockSpec((MB, width), lambda i, s: (base + i, 0))
    across = pl.BlockSpec((width, MB), lambda i, s: (0, base + i))
    outs = [jax.ShapeDtypeStruct((2 * rows, width), BF)] * 2 + [jax.ShapeDtypeStruct((width, 2 * rows), BF)] * 2
    return pl.pallas_call(
        proj_kernel,
        out_shape=outs,
        grid_spec=pltpu.PrefetchScalarGridSpec(
            num_scalar_prefetch=1, grid=(steps,),
            in_specs=[pl.BlockSpec((MB, dim), lambda i, s: (i, 0)), weights, weights]
                     + [pl.BlockSpec(memory_space=pl.ANY)] * len(before),
            out_specs=[down, down, across, across]),
        input_output_aliases={4 + i: i for i in range(len(before))},
        compiler_params=pltpu.CompilerParams(vmem_limit_bytes=60 << 20),
        cost_estimate=cost(4 * rows * dim * width, 12 << 20),
        name="kv_proj",
    )(core, mem, wkt, wvt, *before)


def query_kernel(place_ref, x0_ref, x1_ref, x2_ref, x3_ref, gain_ref, wq_ref, x_ref, n_ref, q_ref, qt_ref):
    for part, src in enumerate((x0_ref, x1_ref, x2_ref, x3_ref)):
        @pl.when(pl.program_id(0) == part)
        def _():
            xb = src[...]
            x = xb.astype(F32)
            n1 = (x * inv_rms(x) * gain_ref[...]).astype(BF)
            q = dot_nt(n1, wq_ref[...]).astype(BF) * jnp.asarray(0.125, BF)
            x_ref[...] = xb
            n_ref[...] = n1
            q_ref[...] = q
            qt_ref[...] = q.T


def queries(place, parts, gain, wqt):
    rows, dim = parts[0].shape
    width = wqt.shape[0] // 2
    n = len(parts)
    whole = pl.BlockSpec((rows, dim), lambda i, s: (0, 0))
    put = pl.BlockSpec((rows, dim), lambda i, s: (s[i], 0))
    return pl.pallas_call(
        query_kernel,
        out_shape=[jax.ShapeDtypeStruct((n * rows, dim), BF)] * 2
                  + [jax.ShapeDtypeStruct((n * rows, width), BF), jax.ShapeDtypeStruct((width, n * rows), BF)],
        grid_spec=pltpu.PrefetchScalarGridSpec(
            num_scalar_prefetch=1, grid=(n,),
            in_specs=[whole] * n + [pl.BlockSpec((1, dim), lambda i, s: (0, 0)),
                                    pl.BlockSpec((width, dim), lambda i, s: (s[n], 0))],
            out_specs=[put, put, pl.BlockSpec((rows, width), lambda i, s: (s[i], 0)),
                       pl.BlockSpec((width, rows), lambda i, s: (0, s[i]))]),
        compiler_params=pltpu.CompilerParams(vmem_limit_bytes=60 << 20),
        cost_estimate=cost(2 * n * rows * dim * width, 6 << 20),
        name="queries",
    )(place, *parts, gain, wqt)


def place_kernel(place_ref, x0_ref, x1_ref, o_ref):
    for part, src in enumerate((x0_ref, x1_ref)):
        @pl.when(pl.program_id(0) == part)
        def _():
            o_ref[...] = src[...]


def place_rows(place, parts):
    rows, dim = parts[0].shape
    n = len(parts)
    return pl.pallas_call(
        place_kernel,
        out_shape=jax.ShapeDtypeStruct((n * rows, dim), parts[0].dtype),
        grid_spec=pltpu.PrefetchScalarGridSpec(
            num_scalar_prefetch=1, grid=(n,),
            in_specs=[pl.BlockSpec((rows, dim), lambda i, s: (0, 0))] * n,
            out_specs=pl.BlockSpec((rows, dim), lambda i, s: (s[2 * i], 0))),
        compiler_params=pltpu.CompilerParams(vmem_limit_bytes=62 << 20),
        cost_estimate=cost(n * rows * dim, 6 << 20),
        name="place_rows",
    )(place, *parts)


def fwd_kernel(len_ref, qt_ref, k_ref, vt_ref, o_ref, m_ref, l_ref, acc_ref, qz_ref, sa_ref, sb_ref):
    qb = qt_ref.shape[1]
    seg_rows = k_ref.shape[0] // 2
    half = lax.broadcasted_iota(jnp.int32, (PAIR, qb), 0) // 64
    for h in range(2):
        qz_ref[h] = jnp.where(half == h, qt_ref[...], jnp.zeros((), BF))
    m_ref[...] = jnp.full(m_ref.shape, NEG, F32)
    l_ref[...] = jnp.zeros(l_ref.shape, F32)
    acc_ref[...] = jnp.zeros(acc_ref.shape, F32)
    first = len_ref[0] // FKB
    total = first + len_ref[1] // FKB

    def base(t):
        t = jnp.clip(t, 0, jnp.maximum(total - 1, 0))
        return pl.multiple_of(jnp.where(t < first, t * FKB, seg_rows + (t - first) * FKB), FKB)

    def scores(row, s_ref):
        kb = k_ref[pl.ds(row, FKB), :]
        for h in range(2):
            s_ref[h] = dot(kb, qz_ref[h])

    def absorb(row, s_ref, count=None):
        rows = pl.ds(row, FKB)
        for h in range(2):
            st = s_ref[h]
            if count is not None:
                st = jnp.where(lax.broadcasted_iota(jnp.int32, st.shape, 0) < count, st, NEG)
            m_old = m_ref[h]
            m_new = jnp.maximum(m_old, jnp.max(st, axis=0, keepdims=True))
            p = jnp.exp2((st - m_new) * LOG2E)
            alpha = jnp.exp2((m_old - m_new) * LOG2E)
            l_ref[h] = l_ref[h] * alpha + jnp.sum(p, axis=0, keepdims=True)
            pv = dot(vt_ref[h * 64:(h + 1) * 64, rows], p.astype(BF))
            acc_ref[h] = acc_ref[h] * alpha + pv
            m_ref[h] = m_new

    scores(base(0), sa_ref)

    @pl.loop(0, total // 2)
    def _(i):
        scores(base(2 * i + 1), sb_ref)
        absorb(base(2 * i), sa_ref)
        scores(base(2 * i + 2), sa_ref)
        absorb(base(2 * i + 1), sb_ref)

    @pl.when(total % 2 == 1)
    def _():
        absorb(base(total - 1), sa_ref)

    @pl.loop(0, 2)
    def _(s):
        full = len_ref[s] // FKB
        rest = len_ref[s] - full * FKB

        @pl.when(rest > 0)
        def _():
            row = pl.multiple_of(s * seg_rows + full * FKB, FKB)
            scores(row, sa_ref)
            absorb(row, sa_ref, rest)

    for h in range(2):
        o_ref[h, 0:64, :] = acc_ref[h]
        o_ref[h, 64:72, :] = jnp.concatenate([m_ref[h], l_ref[h], jnp.zeros((6, qb), F32)], axis=0)


def attention_forward(lens, qt, k, vt, pair0, pairs, at, nq):
    q_off = at // FQB
    rows = k.shape[0]
    off = pair0
    spec = pltpu.PrefetchScalarGridSpec(
        num_scalar_prefetch=1,
        grid=(pairs, nq // FQB),
        in_specs=[
            pl.BlockSpec((PAIR, FQB), lambda p, i, s: (p + off, i + q_off)),
            pl.BlockSpec((rows, PAIR), lambda p, i, s: (0, p + off)),
            pl.BlockSpec((PAIR, rows), lambda p, i, s: (p + off, 0)),
        ],
        out_specs=pl.BlockSpec((2, OROWS, FQB), lambda p, i, s: (p, 0, i)),
        scratch_shapes=[
            pltpu.VMEM((2, 1, FQB), F32), pltpu.VMEM((2, 1, FQB), F32), pltpu.VMEM((2, 64, FQB), F32),
            pltpu.VMEM((2, PAIR, FQB), BF), pltpu.VMEM((2, FKB, FQB), F32), pltpu.VMEM((2, FKB, FQB), F32),
        ])
    work = 2 * pairs * nq * rows
    return pl.pallas_call(
        fwd_kernel,
        out_shape=jax.ShapeDtypeStruct((2 * pairs, OROWS, nq), F32),
        grid_spec=spec,
        compiler_params=pltpu.CompilerParams(vmem_limit_bytes=24 << 20),
        cost_estimate=cost(work * 1024, 4 << 20, work),
        name="attn_fwd",
    )(lens, qt, k, vt)


def bwd_kernel(len_ref, qt_ref, dot_ref, lse_ref, dl_ref, k_ref, v_ref, kt_ref, m0_ref, m1_ref,
               dkv0_ref, dkv1_ref, dqt_ref, dw_ref, qzt_ref, dozt_ref, dkv_ref, m_ref, sems):
    copies = [pltpu.make_async_copy(src, m_ref.at[i], sems.at[i]) for i, src in enumerate((m0_ref, m1_ref))]
    for copy in copies:
        copy.start()
    nq = qt_ref.shape[1]
    seg_rows = k_ref.shape[0] // 2
    blocks = seg_rows // BKB
    half = lax.broadcasted_iota(jnp.int32, (PAIR, nq), 0) // 64
    zero = jnp.zeros((), BF)
    for h in range(2):
        qzt_ref[h] = jnp.where(half == h, qt_ref[...], zero)
        dozt_ref[h] = jnp.where(half == h, dot_ref[...], zero)
    dqt_ref[...] = jnp.zeros(dqt_ref.shape, F32)

    def step(seg, j, count):
        cols = pl.ds(pl.multiple_of(j * BKB, BKB), BKB)
        allc = pl.ds(pl.multiple_of(seg * seg_rows + j * BKB, BKB), BKB)
        kb, vb = k_ref[allc, :], v_ref[allc, :]
        chunks = [(h, slice(c * BQB, (c + 1) * BQB)) for h in range(2) for c in range(nq // BQB)]

        def products(h, qs):
            return dot(kb, qzt_ref[h, :, qs]), dot(vb, dozt_ref[h, :, qs])

        ahead = products(*chunks[0])
        for i, (h, qs) in enumerate(chunks):
            st, dp = ahead
            if i + 1 < len(chunks):
                ahead = products(*chunks[i + 1])
            hs = slice(h * 64, (h + 1) * 64)
            if qs.start == 0:
                dk = jnp.zeros((64, BKB), F32)
                dv = jnp.zeros((64, BKB), F32)
            p = jnp.exp2((st - lse_ref[h, :, qs]) * LOG2E)
            if count is not None:
                p = jnp.where(lax.broadcasted_iota(jnp.int32, st.shape, 0) < count, p, 0.0)
            ds = (p * (dp - dl_ref[h, :, qs])).astype(BF)
            dv = dv + dot_nt(dot_ref[hs, qs], p.astype(BF))
            dk = dk + dot_nt(qt_ref[hs, qs], ds)
            dqt_ref[h, :, qs] += dot(kt_ref[hs, allc], ds)
            if qs.stop == nq:
                dkv_ref[seg, hs, cols] = dk.astype(BF)
                dkv_ref[seg, PAIR + h * 64:PAIR + (h + 1) * 64, cols] = dv.astype(BF)

    first = len_ref[0] // BKB

    @pl.loop(0, first + len_ref[1] // BKB)
    def _(t):
        seg = jnp.where(t < first, 0, 1)
        step(seg, t - seg * first, None)

    @pl.loop(0, 2)
    def _(seg):
        full = len_ref[seg] // BKB
        rest = len_ref[seg] - full * BKB

        @pl.when(rest > 0)
        def _():
            step(seg, full, rest)

        @pl.loop(full + jnp.where(rest > 0, 1, 0), blocks)
        def _(j):
            cols = pl.ds(pl.multiple_of(j * BKB, BKB), BKB)
            dkv_ref[seg, :, cols] = jnp.zeros((2 * PAIR, BKB), BF)

    dw_ref[...] = jnp.zeros(dw_ref.shape, F32)
    for seg, copy in enumerate(copies):
        copy.wait()

        @pl.loop(0, (len_ref[seg] + WKB - 1) // WKB)
        def _(j):
            at = pl.ds(pl.multiple_of(j * WKB, WKB), WKB)
            dw_ref[...] += dot(dkv_ref[seg, :, at], m_ref[seg, at, :])

    dkv0_ref[...] = dkv_ref[0]
    dkv1_ref[...] = dkv_ref[1]


def attention_backward(lens, qt, dot_t, lse, delta, k, v, kt, mem, mem_near, pair0):
    nq = qt.shape[1]
    rows = k.shape[0]
    off = pair0
    across = pl.BlockSpec((PAIR, nq), lambda p, s: (off, 0))
    stat = pl.BlockSpec((2, 1, nq), lambda p, s: (off, 0, 0))
    keys = pl.BlockSpec((rows, PAIR), lambda p, s: (0, off))
    keys_t = pl.BlockSpec((PAIR, rows), lambda p, s: (off, 0))
    spec = pltpu.PrefetchScalarGridSpec(
        num_scalar_prefetch=1,
        grid=(1,),
        in_specs=[across, across, stat, stat, keys, keys, keys_t] + [pl.BlockSpec(memory_space=pltpu.HBM)] * 2,
        out_specs=[pl.BlockSpec((2 * PAIR, rows // 2), lambda p, s: (0, 0)),
                   pl.BlockSpec((2 * PAIR, rows // 2), lambda p, s: (0, 0)),
                   pl.BlockSpec((2, 64, nq), lambda p, s: (0, 0, 0)),
                   pl.BlockSpec((2 * PAIR, mem.shape[1]), lambda p, s: (0, 0))],
        scratch_shapes=[pltpu.VMEM((2, PAIR, nq), BF), pltpu.VMEM((2, PAIR, nq), BF),
                        pltpu.VMEM((2, 2 * PAIR, rows // 2), BF), pltpu.VMEM((2,) + mem.shape, BF),
                        pltpu.SemaphoreType.DMA((2,))])
    work = 2 * nq * rows
    return pl.pallas_call(
        bwd_kernel,
        out_shape=[jax.ShapeDtypeStruct((2 * PAIR, rows // 2), BF)] * 2
                  + [jax.ShapeDtypeStruct((2, 64, nq), F32), jax.ShapeDtypeStruct((2 * PAIR, mem.shape[1]), F32)],
        grid_spec=spec,
        compiler_params=pltpu.CompilerParams(vmem_limit_bytes=32 << 20),
        cost_estimate=cost(work * 2000, 8 << 20, work),
        name="attn_bwd",
    )(lens, qt, dot_t, lse, delta, k, v, kt, mem, mem_near)


def combine_kernel(a_ref, b_ref, o_ref, ob_ref, lse_ref):
    for h in range(2):
        ma, mb = a_ref[h, 64:65, :], b_ref[h, 64:65, :]
        top = jnp.maximum(ma, mb)
        ea, eb = jnp.exp(ma - top), jnp.exp(mb - top)
        den = a_ref[h, 65:66, :] * ea + b_ref[h, 65:66, :] * eb
        o = (a_ref[h, :64, :] * ea + b_ref[h, :64, :] * eb) / den
        o_ref[h] = o
        ob_ref[h * 64:(h + 1) * 64, :] = o.astype(BF)
        lse_ref[h] = top + jnp.log(den)


def combine(a, b):
    _, rows, nq = a.shape
    fix = lambda *shape: pl.BlockSpec(shape, lambda i: (0,) * len(shape))
    return pl.pallas_call(
        combine_kernel,
        grid=(1,),
        in_specs=[fix(2, rows, nq)] * 2,
        out_specs=[fix(2, 64, nq), fix(PAIR, nq), fix(2, 1, nq)],
        out_shape=[jax.ShapeDtypeStruct((2, 64, nq), F32), jax.ShapeDtypeStruct((PAIR, nq), BF),
                   jax.ShapeDtypeStruct((2, 1, nq), F32)],
        compiler_params=pltpu.CompilerParams(vmem_limit_bytes=62 << 20),
        cost_estimate=cost(500 * nq, 2 << 20),
        name="combine",
    )(a, b)


def sum_queries_kernel(a0_ref, a1_ref, a2_ref, b0_ref, b1_ref, b2_ref, o_ref):
    for i, (a, b) in enumerate(((a0_ref, b0_ref), (a1_ref, b1_ref), (a2_ref, b2_ref))):
        for h in range(2):
            at = i * PAIR + h * 64
            o_ref[at:at + 64, :] = ((a[h] + b[h]) * 0.125).astype(BF)


def sum_queries(mine, far):
    nq = mine[0].shape[2]
    part = pl.BlockSpec((2, 64, nq // 2), lambda i: (0, 0, i))
    return pl.pallas_call(
        sum_queries_kernel,
        grid=(2,),
        in_specs=[part] * 6,
        out_specs=pl.BlockSpec((3 * PAIR, nq // 2), lambda i: (0, i)),
        out_shape=jax.ShapeDtypeStruct((3 * PAIR, nq), BF),
        compiler_params=pltpu.CompilerParams(vmem_limit_bytes=16 << 20),
        cost_estimate=cost(1000 * nq, 4 << 20),
        name="sum_queries",
    )(*mine, *far)


def mlp_kernel(h_ref, g_ref, gain_ref, w1_ref, w3_ref, w2_ref,
               n2t_ref, gt_ref, dgate_ref, dup_ref, ut_ref, dh_ref, dhb_ref, gn_ref, n2_ref, acc_ref):
    step = pl.program_id(0)
    rows = h_ref.shape[0]
    chunk = 256

    @pl.when(step == 0)
    def _():
        for c in range(rows // chunk):
            rs = slice(c * chunk, (c + 1) * chunk)
            hid = h_ref[rs, :].astype(F32)
            n2 = (hid * inv_rms(hid) * gain_ref[...]).astype(BF)
            n2_ref[rs, :] = n2
            n2t_ref[:, rs] = n2.T
            gt_ref[rs, :] = g_ref[rs, :].astype(BF)
        acc_ref[...] = jnp.zeros(acc_ref.shape, F32)

    w1, w3, w2 = w1_ref[...], w3_ref[...], w2_ref[...]
    for c in range(rows // chunk):
        rs = slice(c * chunk, (c + 1) * chunk)
        n2 = n2_ref[rs, :]
        gate = dot(n2, w1)
        up = dot(n2, w3)
        ga = dot_nt(gt_ref[rs, :], w2)
        sig = 0.5 * jnp.tanh(0.5 * gate) + 0.5
        act = gate * sig
        ut_ref[:, rs] = (act * up).astype(BF).T
        dup = (ga * act).astype(BF)
        dgate = (ga * up * (sig + act * (1.0 - sig))).astype(BF)
        dup_ref[rs, :] = dup
        dgate_ref[rs, :] = dgate
        acc_ref[rs, :] += dot_nt(dgate, w1) + dot_nt(dup, w3)

    @pl.when(step == pl.num_programs(0) - 1)
    def _():
        total = jnp.zeros(gn_ref.shape, F32)
        for c in range(rows // chunk):
            rs = slice(c * chunk, (c + 1) * chunk)
            hid = h_ref[rs, :].astype(F32)
            inv = inv_rms(hid)
            unit = hid * inv
            grad = acc_ref[rs, :]
            total += jnp.sum(grad * unit, axis=0, keepdims=True)
            dh = g_ref[rs, :] + norm_back(unit, inv, gain_ref[...], grad)
            dh_ref[rs, :] = dh
            dhb_ref[rs, :] = dh.astype(BF)
        gn_ref[...] = total


def mlp(hidden, g_all, gain, w_gate, w_up, w_down):
    rows, dim = hidden.shape
    ff = w_gate.shape[1]
    fix = lambda *shape: pl.BlockSpec(shape, lambda i: (0,) * len(shape))
    wide = pl.BlockSpec((dim, FFB), lambda i: (0, i))
    tall = pl.BlockSpec((FFB, dim), lambda i: (i, 0))
    act = pl.BlockSpec((rows, FFB), lambda i: (0, i))
    act_t = pl.BlockSpec((FFB, rows), lambda i: (i, 0))
    return pl.pallas_call(
        mlp_kernel,
        grid=(ff // FFB,),
        in_specs=[fix(rows, dim), fix(rows, dim), fix(1, dim), wide, wide, tall],
        out_specs=[fix(dim, rows), fix(rows, dim), act, act, act_t, fix(rows, dim), fix(rows, dim), fix(1, dim)],
        out_shape=[jax.ShapeDtypeStruct((dim, rows), BF), jax.ShapeDtypeStruct((rows, dim), BF),
                   jax.ShapeDtypeStruct((rows, ff), BF), jax.ShapeDtypeStruct((rows, ff), BF),
                   jax.ShapeDtypeStruct((ff, rows), BF), jax.ShapeDtypeStruct((rows, dim), F32),
                   jax.ShapeDtypeStruct((rows, dim), BF), jax.ShapeDtypeStruct((1, dim), F32)],
        scratch_shapes=[pltpu.VMEM((rows, dim), BF), pltpu.VMEM((rows, dim), F32)],
        compiler_params=pltpu.CompilerParams(vmem_limit_bytes=56 << 20),
        cost_estimate=cost(10 * rows * dim * ff, 40 << 20, rows * ff),
        name="mlp",
    )(hidden, g_all, gain, w_gate, w_up, w_down)


def mlp_weights_kernel(n2t_ref, gt_ref, dgate_ref, dup_ref, ut_ref, n2t2_ref, gt2_ref, dgate2_ref, dup2_ref, ut2_ref,
                       g1_ref, g3_ref, g2_ref):
    g1_ref[...] = dot(n2t_ref[...], dgate_ref[...]) + dot(n2t2_ref[...], dgate2_ref[...])
    g3_ref[...] = dot(n2t_ref[...], dup_ref[...]) + dot(n2t2_ref[...], dup2_ref[...])
    g2_ref[...] = dot(ut_ref[...], gt_ref[...]) + dot(ut2_ref[...], gt2_ref[...])


def mlp_weights(factors, factors_near):
    dim, rows = factors[0].shape
    ff = factors[2].shape[1]
    fix = lambda *shape: pl.BlockSpec(shape, lambda i: (0,) * len(shape))
    act = pl.BlockSpec((rows, WFB), lambda i: (0, i))
    wide = pl.BlockSpec((dim, WFB), lambda i: (0, i))
    ins = [fix(dim, rows), fix(rows, dim), act, act, pl.BlockSpec((WFB, rows), lambda i: (i, 0))]
    return pl.pallas_call(
        mlp_weights_kernel,
        grid=(ff // WFB,),
        in_specs=ins + ins,
        out_specs=[wide, wide, pl.BlockSpec((WFB, dim), lambda i: (i, 0))],
        out_shape=[jax.ShapeDtypeStruct((dim, ff), F32)] * 2 + [jax.ShapeDtypeStruct((ff, dim), F32)],
        compiler_params=pltpu.CompilerParams(vmem_limit_bytes=60 << 20),
        cost_estimate=cost(12 * rows * dim * ff, 50 << 20),
        name="mlp_weights",
    )(*factors, *factors_near)


def memory_kernel(core_ref, a0_ref, a1_ref, a2_ref, b0_ref, b1_ref, b2_ref, wk_ref, wv_ref, o_ref):
    core = core_ref[0]
    total = None
    for who, refs in ((core, (a0_ref, a1_ref, a2_ref)), (1 - core, (b0_ref, b1_ref, b2_ref))):
        for i, ref in enumerate(refs):
            rows = pl.ds(pl.multiple_of((who * 3 + i) * PAIR, PAIR), PAIR)
            part = dot(ref[...].T, jnp.concatenate([wk_ref[rows, :], wv_ref[rows, :]], axis=0))
            total = part if total is None else total + part
    o_ref[...] = total


def memory_grad(core, mine, near, wkt, wvt):
    rows = mine[0].shape[-1]
    dim = wkt.shape[1]
    block = pl.BlockSpec((2 * PAIR, MB), lambda i, s: (0, i))
    whole = pl.BlockSpec(wkt.shape, lambda i, s: (0, 0))
    return pl.pallas_call(
        memory_kernel,
        out_shape=jax.ShapeDtypeStruct((rows, dim), F32),
        grid_spec=pltpu.PrefetchScalarGridSpec(
            num_scalar_prefetch=1, grid=(rows // MB,),
            in_specs=[block] * 6 + [whole, whole],
            out_specs=pl.BlockSpec((MB, dim), lambda i, s: (i, 0))),
        compiler_params=pltpu.CompilerParams(vmem_limit_bytes=60 << 20),
        cost_estimate=cost(4 * rows * dim * dim, 16 << 20),
        name="memory_grad",
    )(core, *mine, *near, wkt, wvt)


def half_index(i, core):
    return i + core - 2 * i * core


def out_proj_kernel(core_ref, mine_ref, near0_ref, near1_ref, dh_ref, o_ref):
    half = near0_ref.shape[1]

    @pl.when(pl.program_id(0) == 0)
    def _():
        o_ref[...] = dot(mine_ref[...], dh_ref[...])

    @pl.when(pl.program_id(0) == 1)
    def _():
        o_ref[...] = dot(near0_ref[...], dh_ref[:half, :]) + dot(near1_ref[...], dh_ref[half:, :])


def out_proj_grad(core, mine, near, dh):
    width, rows = mine.shape
    dim = dh.shape[1]
    whole = pl.BlockSpec((width, rows), lambda i, s: (0, 0))
    part = pl.BlockSpec((width, rows // 2), lambda i, s: (0, 0))
    return pl.pallas_call(
        out_proj_kernel,
        out_shape=jax.ShapeDtypeStruct((2 * width, dim), F32),
        grid_spec=pltpu.PrefetchScalarGridSpec(
            num_scalar_prefetch=1, grid=(2,),
            in_specs=[whole, part, part, pl.BlockSpec((rows, dim), lambda i, s: (0, 0))],
            out_specs=pl.BlockSpec((width, dim), lambda i, s: (half_index(i, s[0]), 0))),
        compiler_params=pltpu.CompilerParams(vmem_limit_bytes=24 << 20),
        cost_estimate=cost(4 * rows * dim * width, 6 << 20),
        name="out_proj_grad",
    )(core, mine, *near, dh)


def query_grad_kernel(place_ref, mine_ref, near_ref, n1_ref, wq_ref, x_ref, dh_ref, gain_ref,
                      gw_ref, gx_ref, gn_ref, acc_ref):
    half = acc_ref.shape[0] // 2

    @pl.when(pl.program_id(0) == 0)
    def _():
        gw_ref[...] = dot(mine_ref[...], n1_ref[...])
        acc_ref[...] = dot(mine_ref[...].T, wq_ref[...])

    @pl.when(pl.program_id(0) == 1)
    def _():
        first, second = near_ref[:, half:], near_ref[:, :half]
        gw_ref[...] = dot(first, n1_ref[:half, :]) + dot(second, n1_ref[half:, :])
        acc_ref[:half, :] += dot(first.T, wq_ref[...])
        acc_ref[half:, :] += dot(second.T, wq_ref[...])

    @pl.when(pl.program_id(0) == 1)
    def _():
        rows = gx_ref.shape[0]
        total = jnp.zeros(gn_ref.shape, F32)
        for c in range(acc_ref.shape[0] // rows):
            rs = slice(c * rows, (c + 1) * rows)
            x = x_ref[rs, :].astype(F32)
            total += jnp.sum(acc_ref[rs, :] * (x * inv_rms(x)), axis=0, keepdims=True)
        gn_ref[...] = total
        own = pl.ds(pl.multiple_of(place_ref[0] * rows, rows), rows)
        x = x_ref[own, :].astype(F32)
        inv = inv_rms(x)
        gx_ref[...] = dh_ref[...] + norm_back(x * inv, inv, gain_ref[...], acc_ref[own, :])


def query_grad(place, mine, near, n1, wqt, x_all, d_hid, gain, rows):
    width, total = mine.shape
    dim = n1.shape[1]
    fix = lambda *shape: pl.BlockSpec(shape, lambda i, s: (0,) * len(shape))
    half = pl.BlockSpec((width, dim), lambda i, s: (half_index(i, s[4]), 0))
    return pl.pallas_call(
        query_grad_kernel,
        out_shape=[jax.ShapeDtypeStruct((2 * width, dim), F32), jax.ShapeDtypeStruct((rows, dim), F32),
                   jax.ShapeDtypeStruct((1, dim), F32)],
        grid_spec=pltpu.PrefetchScalarGridSpec(
            num_scalar_prefetch=1, grid=(2,),
            in_specs=[fix(width, total), fix(width, total), fix(total, dim), half, fix(total, dim),
                      pl.BlockSpec((rows, dim), lambda i, s: (s[0], 0)), fix(1, dim)],
            out_specs=[half, fix(rows, dim), fix(1, dim)],
            scratch_shapes=[pltpu.VMEM((total, dim), F32)]),
        compiler_params=pltpu.CompilerParams(vmem_limit_bytes=32 << 20),
        cost_estimate=cost(8 * total * dim * width, 10 << 20),
        name="query_grad",
    )(place, mine, near, n1, wqt, x_all, d_hid, gain)


def key_weights_kernel(core_ref, *refs):
    gk_ref, gv_ref = refs[-2:]
    count = (len(refs) - 2) // 2
    for at in range(count):
        @pl.when(pl.program_id(0) == at)
        def _():
            a, b = refs[at], refs[count + at]
            gk_ref[...] = a[:PAIR, :] + b[:PAIR, :]
            gv_ref[...] = a[PAIR:, :] + b[PAIR:, :]


def key_weights(core, parts, others):
    pairs = len(parts) // 2
    dim = parts[0].shape[1]
    out = pl.BlockSpec((PAIR, dim), lambda i, s: (half_index(i // pairs, s[0]) * pairs + i % pairs, 0))
    return pl.pallas_call(
        key_weights_kernel,
        out_shape=[jax.ShapeDtypeStruct((2 * pairs * PAIR, dim), F32)] * 2,
        grid_spec=pltpu.PrefetchScalarGridSpec(
            num_scalar_prefetch=1, grid=(2 * pairs,),
            in_specs=[pl.BlockSpec((2 * PAIR, dim), lambda i, s: (0, 0))] * (4 * pairs),
            out_specs=[out, out]),
        compiler_params=pltpu.CompilerParams(vmem_limit_bytes=60 << 20),
        cost_estimate=cost(4 * pairs * PAIR * dim, 10 << 20),
        name="key_weights",
    )(core, *parts, *others)


def inv_rms(tensor):
    return lax.rsqrt(jnp.mean(tensor * tensor, axis=-1, keepdims=True) + 1e-6)


def norm_back(unit, inv, gain, grad):
    scaled = grad * gain
    return inv * (scaled - unit * jnp.mean(scaled * unit, axis=-1, keepdims=True))


def mm(a, b, ca, cb, dtype=F32):
    out = lax.dot_general(a, b, (((ca,), (cb,)), ((), ())), preferred_element_type=F32)
    return out if dtype == F32 else out.astype(dtype)


def solution(mesh):
    n = mesh.shape['seq']
    near = [(i, i ^ 1) for i in range(n)]
    far = [(i, i ^ 2) for i in range(n)]
    row_spec = P(('data', 'seq'), None)
    weight_spec = P()
    part_vec = P('data')
    part_mat = P('data', None)
    part_cube = P('data', None, None)

    def to_near(a):
        return lax.ppermute(a, 'seq', near)

    def to_far(a):
        return lax.ppermute(a, 'seq', far)

    def device_work(dec_in, memory, mem_len, grad_out, norm_attn, wq, wk, wv, wo, norm_mlp, w_gate, w_up, w_down):
        rows, dim = dec_in.shape
        m_rows = memory.shape[0]
        heads, head = wq.shape[1], wq.shape[2]
        mine = heads // 2
        width = mine * head
        dev = lax.axis_index('seq')
        core = lax.rem(dev, 2)
        core1 = core.reshape(1).astype(jnp.int32)
        wqt, wkt, wvt = (w.transpose(1, 2, 0).reshape(heads * head, dim) for w in (wq, wk, wv))
        wo2 = wo.reshape(heads * head, dim)
        lens = jnp.stack([jnp.clip(mem_len[0] - i * m_rows, 0, m_rows) for i in (dev, dev ^ 1)]).astype(jnp.int32)
        chip = dev // 2
        place = jnp.stack([chip, 2 + chip, 1 - chip, 3 - chip, core]).astype(jnp.int32)
        gain1 = norm_attn.astype(F32).reshape(1, dim)
        gain2 = norm_mlp.astype(F32).reshape(1, dim)

        def gather_parts(a):
            across = to_far(a)
            beside = to_near(a)
            return a, beside, across, to_near(across)

        x_parts = gather_parts(dec_in)
        mem_near = to_near(memory)
        g_parts = (grad_out, to_far(grad_out))

        first = project(core1, memory, wkt, wvt, 0, ())
        x_all_b, n1, _, qt_s = queries(place, x_parts, gain1, wqt)
        k, v, kt, vt = project(core1, mem_near, wkt, wvt, 1, first)

        pairs = mine // 2
        pieces = [(pair, 0, n * rows) for pair in range(pairs - 1)]
        pieces += [(pairs - 1, 0, n * rows // 2), (pairs - 1, n * rows // 2, n * rows // 2)]
        outs, lses = [], []
        parts = []
        for pair, at, count in pieces:
            part = attention_forward(lens, qt_s, k, vt, pair, 1, at, count)
            parts.append((part, to_far(part)))
        outs_b = []
        for a, b in parts:
            o_piece, ob_piece, lse_piece = combine(a, b)
            outs.append(o_piece)
            outs_b.append(ob_piece)
            lses.append(lse_piece)
        for pieces_of, axis in ((outs, 2), (outs_b, 1), (lses, 2)):
            pieces_of[-2:] = [jnp.concatenate(pieces_of[-2:], axis=axis)]
        g_half = place_rows(place, g_parts)
        o_t = jnp.concatenate(outs, axis=0)
        lse = jnp.concatenate(lses, axis=0)
        o_t_b = jnp.concatenate(outs_b, axis=0)
        half = n * rows // 2
        o_t_first, o_t_second = o_t_b[:, :half], o_t_b[:, half:]
        o_near_first = to_near(o_t_second)

        def half_rows(w, who):
            return lax.dynamic_slice(w, (who * width, 0), (width, dim))

        wo_m, wo_n = half_rows(wo2, core), half_rows(wo2, 1 - core)
        hidden = (x_all_b[:half].astype(F32) + mm(o_t_first, wo_m, 0, 0) + mm(o_near_first, wo_n, 0, 0)).astype(BF)

        n2t, g_top, d_gate, d_up, act_t, d_hid, d_hid_half, g_norm_half = mlp(
            hidden, g_half, gain2, w_gate, w_up, w_down)
        d_hid_b = jnp.concatenate([d_hid_half, to_near(d_hid_half)], axis=0)
        factors = (n2t, g_top, d_gate, d_up, act_t)
        factors_near = tuple(to_near(a) for a in factors)
        o_near_second = to_near(o_t_first)
        g_norm_mlp = g_norm_half + to_near(g_norm_half)

        do_t_f = mm(wo_m, d_hid_b, 1, 1)
        delta = jnp.sum(do_t_f.reshape(mine, head, n * rows) * o_t, axis=1, keepdims=True)
        do_t = do_t_f.astype(BF)
        dkvs, dkvs_near, dqs, dws = [], [], [], []
        lens_now = lens
        for pair in range(pairs):
            dkv, dkv_near, dqt, dw = attention_backward(
                lens_now, qt_s, do_t, lse, delta, k, v, kt, memory, mem_near, pair)
            dqs.append((dqt, to_far(dqt)))
            dws.append((dw, to_far(dw)))
            dkvs.append(dkv)
            dkvs_near.append(to_near(dkv_near))
            lens_now, dw_last = lax.optimization_barrier((lens, dw))

        act_t, _ = lax.optimization_barrier((act_t, dw_last))
        factors = (n2t, g_top, d_gate, d_up, act_t)
        g_gate, g_up, g_down = mlp_weights(factors, factors_near)
        g_mem = memory_grad(core1, dkvs, dkvs_near, wkt, wvt)

        def as_weight(rows_by_dim):
            return rows_by_dim.reshape(heads, head, dim).transpose(2, 0, 1)

        g_wo = out_proj_grad(core1, o_t_b, (o_near_first, o_near_second), d_hid_b).reshape(heads, head, dim)

        dqt_b = sum_queries([a for a, _ in dqs], [b for _, b in dqs])
        dqt_near = to_near(dqt_b)
        g_wqt, g_dec, g_norm_attn = query_grad(place, dqt_b, dqt_near, n1, wqt, x_all_b, d_hid, gain1, rows)

        mine_near = []
        for a, b in dws:
            a_near = to_near(a)
            mine_near.append((a_near, to_near(b)))
        g_wkt, g_wvt = key_weights(core1, [a for a, _ in dws] + [a for a, _ in mine_near],
                                   [b for _, b in dws] + [b for _, b in mine_near])
        g_wq, g_wk, g_wv = as_weight(g_wqt), as_weight(g_wkt), as_weight(g_wvt)
        return (g_dec, g_mem, g_norm_attn.reshape(dim), g_wq, g_wk, g_wv, g_wo, g_norm_mlp.reshape(dim), g_gate, g_up, g_down)


    return jax.shard_map(device_work, mesh=mesh,
                         in_specs=(row_spec, row_spec, part_vec, row_spec) + (weight_spec,) * 9,
                         out_specs=(row_spec, row_spec, part_vec, part_cube, part_cube, part_cube, part_cube,
                                    part_vec, part_mat, part_mat, part_mat),
                         check_vma=False)
```

```python
import jax
import jax.numpy as jnp
from jax import lax
from jax.experimental import pallas as pl
from jax.experimental.pallas import tpu as pltpu
from jax.sharding import PartitionSpec as P


LOG2E = 1.4426950408889634
NEG = -1e30
BF = jnp.bfloat16
F32 = jnp.float32
FKB = 512
FQB = 512
BKB = 512
BQB = 256
WKB = 1024
PAIR = 128
OROWS = 72
FFB = 512
WFB = 512
MB = 512


def dot(a, b):
    return jnp.dot(a, b, preferred_element_type=F32)


def dot_nt(a, b):
    return lax.dot_general(a, b, (((1,), (1,)), ((), ())), preferred_element_type=F32)


def cost(flops, bytes_accessed, exps=0):
    return pl.CostEstimate(flops=int(flops), bytes_accessed=int(bytes_accessed), transcendentals=int(exps))


def proj_kernel(core_ref, m_ref, wk_ref, wv_ref, *refs):
    k_ref, v_ref, kt_ref, vt_ref = refs[-4:]
    m = m_ref[...]
    k = dot_nt(m, wk_ref[...]).astype(BF)
    v = dot_nt(m, wv_ref[...]).astype(BF)
    k_ref[...] = k
    v_ref[...] = v
    kt_ref[...] = k.T
    vt_ref[...] = v.T


def project(core, mem, wkt, wvt, seg, before):
    rows, dim = mem.shape
    width = wkt.shape[0] // 2
    steps = rows // MB
    base = seg * steps
    weights = pl.BlockSpec((width, dim), lambda i, s: (s[0], 0))
    down = pl.BlockSpec((MB, width), lambda i, s: (base + i, 0))
    across = pl.BlockSpec((width, MB), lambda i, s: (0, base + i))
    outs = [jax.ShapeDtypeStruct((2 * rows, width), BF)] * 2 + [jax.ShapeDtypeStruct((width, 2 * rows), BF)] * 2
    return pl.pallas_call(
        proj_kernel,
        out_shape=outs,
        grid_spec=pltpu.PrefetchScalarGridSpec(
            num_scalar_prefetch=1, grid=(steps,),
            in_specs=[pl.BlockSpec((MB, dim), lambda i, s: (i, 0)), weights, weights]
                     + [pl.BlockSpec(memory_space=pl.ANY)] * len(before),
            out_specs=[down, down, across, across]),
        input_output_aliases={4 + i: i for i in range(len(before))},
        compiler_params=pltpu.CompilerParams(vmem_limit_bytes=60 << 20),
        cost_estimate=cost(4 * rows * dim * width, 12 << 20),
        name="kv_proj",
    )(core, mem, wkt, wvt, *before)


def query_kernel(place_ref, x0_ref, x1_ref, x2_ref, x3_ref, gain_ref, wq_ref, x_ref, n_ref, q_ref, qt_ref):
    for part, src in enumerate((x0_ref, x1_ref, x2_ref, x3_ref)):
        @pl.when(pl.program_id(0) == part)
        def _():
            xb = src[...]
            x = xb.astype(F32)
            n1 = (x * inv_rms(x) * gain_ref[...]).astype(BF)
            q = dot_nt(n1, wq_ref[...]).astype(BF) * jnp.asarray(0.125, BF)
            x_ref[...] = xb
            n_ref[...] = n1
            q_ref[...] = q
            qt_ref[...] = q.T


def queries(place, parts, gain, wqt):
    rows, dim = parts[0].shape
    width = wqt.shape[0] // 2
    n = len(parts)
    whole = pl.BlockSpec((rows, dim), lambda i, s: (0, 0))
    put = pl.BlockSpec((rows, dim), lambda i, s: (s[i], 0))
    return pl.pallas_call(
        query_kernel,
        out_shape=[jax.ShapeDtypeStruct((n * rows, dim), BF)] * 2
                  + [jax.ShapeDtypeStruct((n * rows, width), BF), jax.ShapeDtypeStruct((width, n * rows), BF)],
        grid_spec=pltpu.PrefetchScalarGridSpec(
            num_scalar_prefetch=1, grid=(n,),
            in_specs=[whole] * n + [pl.BlockSpec((1, dim), lambda i, s: (0, 0)),
                                    pl.BlockSpec((width, dim), lambda i, s: (s[n], 0))],
            out_specs=[put, put, pl.BlockSpec((rows, width), lambda i, s: (s[i], 0)),
                       pl.BlockSpec((width, rows), lambda i, s: (0, s[i]))]),
        compiler_params=pltpu.CompilerParams(vmem_limit_bytes=24 << 20),
        cost_estimate=cost(2 * n * rows * dim * width, 6 << 20),
        name="queries",
    )(place, *parts, gain, wqt)


def fwd_kernel(len_ref, qt_ref, k_ref, vt_ref, o_ref, m_ref, l_ref, acc_ref, qz_ref, sa_ref, sb_ref):
    qb = qt_ref.shape[1]
    seg_rows = k_ref.shape[0] // 2
    half = lax.broadcasted_iota(jnp.int32, (PAIR, qb), 0) // 64
    for h in range(2):
        qz_ref[h] = jnp.where(half == h, qt_ref[...], jnp.zeros((), BF))
    m_ref[...] = jnp.full(m_ref.shape, NEG, F32)
    l_ref[...] = jnp.zeros(l_ref.shape, F32)
    acc_ref[...] = jnp.zeros(acc_ref.shape, F32)
    first = len_ref[0] // FKB
    total = first + len_ref[1] // FKB

    def base(t):
        t = jnp.clip(t, 0, jnp.maximum(total - 1, 0))
        return pl.multiple_of(jnp.where(t < first, t * FKB, seg_rows + (t - first) * FKB), FKB)

    def scores(row, s_ref):
        kb = k_ref[pl.ds(row, FKB), :]
        for h in range(2):
            s_ref[h] = dot(kb, qz_ref[h])

    def absorb(row, s_ref, count=None):
        rows = pl.ds(row, FKB)
        for h in range(2):
            st = s_ref[h]
            if count is not None:
                st = jnp.where(lax.broadcasted_iota(jnp.int32, st.shape, 0) < count, st, NEG)
            m_old = m_ref[h]
            m_new = jnp.maximum(m_old, jnp.max(st, axis=0, keepdims=True))
            p = jnp.exp2((st - m_new) * LOG2E)
            alpha = jnp.exp2((m_old - m_new) * LOG2E)
            l_ref[h] = l_ref[h] * alpha + jnp.sum(p, axis=0, keepdims=True)
            pv = dot(vt_ref[h * 64:(h + 1) * 64, rows], p.astype(BF))
            acc_ref[h] = acc_ref[h] * alpha + pv
            m_ref[h] = m_new

    scores(base(0), sa_ref)

    @pl.loop(0, total // 2)
    def _(i):
        scores(base(2 * i + 1), sb_ref)
        absorb(base(2 * i), sa_ref)
        scores(base(2 * i + 2), sa_ref)
        absorb(base(2 * i + 1), sb_ref)

    @pl.when(total % 2 == 1)
    def _():
        absorb(base(total - 1), sa_ref)

    @pl.loop(0, 2)
    def _(s):
        full = len_ref[s] // FKB
        rest = len_ref[s] - full * FKB

        @pl.when(rest > 0)
        def _():
            row = pl.multiple_of(s * seg_rows + full * FKB, FKB)
            scores(row, sa_ref)
            absorb(row, sa_ref, rest)

    for h in range(2):
        o_ref[h, 0:64, :] = acc_ref[h]
        o_ref[h, 64:72, :] = jnp.concatenate([m_ref[h], l_ref[h], jnp.zeros((6, qb), F32)], axis=0)


def attention_forward(lens, qt, k, vt, pair0, pairs, at, nq):
    q_off = at // FQB
    rows = k.shape[0]
    off = pair0
    spec = pltpu.PrefetchScalarGridSpec(
        num_scalar_prefetch=1,
        grid=(pairs, nq // FQB),
        in_specs=[
            pl.BlockSpec((PAIR, FQB), lambda p, i, s: (p + off, i + q_off)),
            pl.BlockSpec((rows, PAIR), lambda p, i, s: (0, p + off)),
            pl.BlockSpec((PAIR, rows), lambda p, i, s: (p + off, 0)),
        ],
        out_specs=pl.BlockSpec((2, OROWS, FQB), lambda p, i, s: (p, 0, i)),
        scratch_shapes=[
            pltpu.VMEM((2, 1, FQB), F32), pltpu.VMEM((2, 1, FQB), F32), pltpu.VMEM((2, 64, FQB), F32),
            pltpu.VMEM((2, PAIR, FQB), BF), pltpu.VMEM((2, FKB, FQB), F32), pltpu.VMEM((2, FKB, FQB), F32),
        ])
    work = 2 * pairs * nq * rows
    return pl.pallas_call(
        fwd_kernel,
        out_shape=jax.ShapeDtypeStruct((2 * pairs, OROWS, nq), F32),
        grid_spec=spec,
        compiler_params=pltpu.CompilerParams(vmem_limit_bytes=67_000_000),
        cost_estimate=cost(work * 1024, 4 << 20, work),
        name="attn_fwd",
    )(lens, qt, k, vt)


def bwd_kernel(len_ref, qt_ref, dot_ref, lse_ref, dl_ref, k_ref, v_ref, kt_ref, m0_ref, m1_ref,
               dkv0_ref, dkv1_ref, dqt_ref, dw_ref, qzt_ref, dozt_ref, dkv_ref, m_ref, sems):
    copies = [pltpu.make_async_copy(src, m_ref.at[i], sems.at[i]) for i, src in enumerate((m0_ref, m1_ref))]
    for copy in copies:
        copy.start()
    nq = qt_ref.shape[1]
    seg_rows = k_ref.shape[0] // 2
    blocks = seg_rows // BKB
    half = lax.broadcasted_iota(jnp.int32, (PAIR, nq), 0) // 64
    zero = jnp.zeros((), BF)
    for h in range(2):
        qzt_ref[h] = jnp.where(half == h, qt_ref[...], zero)
        dozt_ref[h] = jnp.where(half == h, dot_ref[...], zero)
    dqt_ref[...] = jnp.zeros(dqt_ref.shape, F32)

    def step(seg, j, count):
        cols = pl.ds(pl.multiple_of(j * BKB, BKB), BKB)
        allc = pl.ds(pl.multiple_of(seg * seg_rows + j * BKB, BKB), BKB)
        kb, vb = k_ref[allc, :], v_ref[allc, :]
        chunks = [(h, slice(c * BQB, (c + 1) * BQB)) for h in range(2) for c in range(nq // BQB)]

        def products(h, qs):
            return dot(kb, qzt_ref[h, :, qs]), dot(vb, dozt_ref[h, :, qs])

        ahead = products(*chunks[0])
        for i, (h, qs) in enumerate(chunks):
            st, dp = ahead
            if i + 1 < len(chunks):
                ahead = products(*chunks[i + 1])
            hs = slice(h * 64, (h + 1) * 64)
            if qs.start == 0:
                dk = jnp.zeros((64, BKB), F32)
                dv = jnp.zeros((64, BKB), F32)
            p = jnp.exp2((st - lse_ref[h, :, qs]) * LOG2E)
            if count is not None:
                p = jnp.where(lax.broadcasted_iota(jnp.int32, st.shape, 0) < count, p, 0.0)
            ds = (p * (dp - dl_ref[h, :, qs])).astype(BF)
            dv = dv + dot_nt(dot_ref[hs, qs], p.astype(BF))
            dk = dk + dot_nt(qt_ref[hs, qs], ds)
            dqt_ref[h, :, qs] += dot(kt_ref[hs, allc], ds)
            if qs.stop == nq:
                dkv_ref[seg, hs, cols] = dk.astype(BF)
                dkv_ref[seg, PAIR + h * 64:PAIR + (h + 1) * 64, cols] = dv.astype(BF)

    first = len_ref[0] // BKB

    @pl.loop(0, first + len_ref[1] // BKB)
    def _(t):
        seg = jnp.where(t < first, 0, 1)
        step(seg, t - seg * first, None)

    @pl.loop(0, 2)
    def _(seg):
        full = len_ref[seg] // BKB
        rest = len_ref[seg] - full * BKB

        @pl.when(rest > 0)
        def _():
            step(seg, full, rest)

        @pl.loop(full + jnp.where(rest > 0, 1, 0), blocks)
        def _(j):
            cols = pl.ds(pl.multiple_of(j * BKB, BKB), BKB)
            dkv_ref[seg, :, cols] = jnp.zeros((2 * PAIR, BKB), BF)

    dw_ref[...] = jnp.zeros(dw_ref.shape, F32)
    for seg, copy in enumerate(copies):
        copy.wait()

        @pl.loop(0, (len_ref[seg] + WKB - 1) // WKB)
        def _(j):
            at = pl.ds(pl.multiple_of(j * WKB, WKB), WKB)
            dw_ref[...] += dot(dkv_ref[seg, :, at], m_ref[seg, at, :])

    dkv0_ref[...] = dkv_ref[0]
    dkv1_ref[...] = dkv_ref[1]


def attention_backward(lens, qt, dot_t, lse, delta, k, v, kt, mem, mem_near, pair0):
    nq = qt.shape[1]
    rows = k.shape[0]
    off = pair0
    across = pl.BlockSpec((PAIR, nq), lambda p, s: (off, 0))
    stat = pl.BlockSpec((2, 1, nq), lambda p, s: (off, 0, 0))
    keys = pl.BlockSpec((rows, PAIR), lambda p, s: (0, off))
    keys_t = pl.BlockSpec((PAIR, rows), lambda p, s: (off, 0))
    spec = pltpu.PrefetchScalarGridSpec(
        num_scalar_prefetch=1,
        grid=(1,),
        in_specs=[across, across, stat, stat, keys, keys, keys_t] + [pl.BlockSpec(memory_space=pltpu.HBM)] * 2,
        out_specs=[pl.BlockSpec((2 * PAIR, rows // 2), lambda p, s: (0, 0)),
                   pl.BlockSpec((2 * PAIR, rows // 2), lambda p, s: (0, 0)),
                   pl.BlockSpec((2, 64, nq), lambda p, s: (0, 0, 0)),
                   pl.BlockSpec((2 * PAIR, mem.shape[1]), lambda p, s: (0, 0))],
        scratch_shapes=[pltpu.VMEM((2, PAIR, nq), BF), pltpu.VMEM((2, PAIR, nq), BF),
                        pltpu.VMEM((2, 2 * PAIR, rows // 2), BF), pltpu.VMEM((2,) + mem.shape, BF),
                        pltpu.SemaphoreType.DMA((2,))])
    work = 2 * nq * rows
    return pl.pallas_call(
        bwd_kernel,
        out_shape=[jax.ShapeDtypeStruct((2 * PAIR, rows // 2), BF)] * 2
                  + [jax.ShapeDtypeStruct((2, 64, nq), F32), jax.ShapeDtypeStruct((2 * PAIR, mem.shape[1]), F32)],
        grid_spec=spec,
        compiler_params=pltpu.CompilerParams(vmem_limit_bytes=40 << 20),
        cost_estimate=cost(work * 2000, 8 << 20, work),
        name="attn_bwd",
    )(lens, qt, dot_t, lse, delta, k, v, kt, mem, mem_near)


def combine_kernel(a_ref, b_ref, o_ref, ob_ref, lse_ref):
    for h in range(2):
        ma, mb = a_ref[h, 64:65, :], b_ref[h, 64:65, :]
        top = jnp.maximum(ma, mb)
        ea, eb = jnp.exp(ma - top), jnp.exp(mb - top)
        den = a_ref[h, 65:66, :] * ea + b_ref[h, 65:66, :] * eb
        o = (a_ref[h, :64, :] * ea + b_ref[h, :64, :] * eb) / den
        o_ref[h] = o
        ob_ref[h * 64:(h + 1) * 64, :] = o.astype(BF)
        lse_ref[h] = top + jnp.log(den)


def combine(a, b):
    _, rows, nq = a.shape
    fix = lambda *shape: pl.BlockSpec(shape, lambda i: (0,) * len(shape))
    return pl.pallas_call(
        combine_kernel,
        grid=(1,),
        in_specs=[fix(2, rows, nq)] * 2,
        out_specs=[fix(2, 64, nq), fix(PAIR, nq), fix(2, 1, nq)],
        out_shape=[jax.ShapeDtypeStruct((2, 64, nq), F32), jax.ShapeDtypeStruct((PAIR, nq), BF),
                   jax.ShapeDtypeStruct((2, 1, nq), F32)],
        compiler_params=pltpu.CompilerParams(vmem_limit_bytes=67_000_000),
        cost_estimate=cost(500 * nq, 2 << 20),
        name="combine",
    )(a, b)


def sum_queries_kernel(a0_ref, a1_ref, a2_ref, b0_ref, b1_ref, b2_ref, o_ref):
    for i, (a, b) in enumerate(((a0_ref, b0_ref), (a1_ref, b1_ref), (a2_ref, b2_ref))):
        for h in range(2):
            at = i * PAIR + h * 64
            o_ref[at:at + 64, :] = ((a[h] + b[h]) * 0.125).astype(BF)


def sum_queries(mine, far):
    nq = mine[0].shape[2]
    part = pl.BlockSpec((2, 64, nq // 2), lambda i: (0, 0, i))
    return pl.pallas_call(
        sum_queries_kernel,
        grid=(2,),
        in_specs=[part] * 6,
        out_specs=pl.BlockSpec((3 * PAIR, nq // 2), lambda i: (0, i)),
        out_shape=jax.ShapeDtypeStruct((3 * PAIR, nq), BF),
        compiler_params=pltpu.CompilerParams(vmem_limit_bytes=16 << 20),
        cost_estimate=cost(1000 * nq, 4 << 20),
        name="sum_queries",
    )(*mine, *far)


def mlp_kernel(place_ref, h_ref, g0_ref, g1_ref, gain_ref, w1_ref, w3_ref, w2_ref,
               n2t_ref, gt_ref, dgate_ref, dup_ref, ut_ref, dh_ref, dhb_ref, gn_ref, n2_ref, acc_ref):
    step = pl.program_id(0)
    rows = h_ref.shape[0]
    chunk = g0_ref.shape[0]

    def grad_rows(c):
        return jnp.where(place_ref[0] == c, g0_ref[...], g1_ref[...])

    @pl.when(step == 0)
    def _():
        for c in range(rows // chunk):
            rs = slice(c * chunk, (c + 1) * chunk)
            hid = h_ref[rs, :].astype(F32)
            n2 = (hid * inv_rms(hid) * gain_ref[...]).astype(BF)
            n2_ref[rs, :] = n2
            n2t_ref[:, rs] = n2.T
            gt_ref[rs, :] = grad_rows(c).astype(BF)
        acc_ref[...] = jnp.zeros(acc_ref.shape, F32)

    w1, w3, w2 = w1_ref[...], w3_ref[...], w2_ref[...]
    for c in range(rows // chunk):
        rs = slice(c * chunk, (c + 1) * chunk)
        n2 = n2_ref[rs, :]
        gate = dot(n2, w1)
        up = dot(n2, w3)
        ga = dot_nt(gt_ref[rs, :], w2)
        sig = 0.5 * jnp.tanh(0.5 * gate) + 0.5
        act = gate * sig
        ut_ref[:, rs] = (act * up).astype(BF).T
        dup = (ga * act).astype(BF)
        dgate = (ga * up * (sig + act * (1.0 - sig))).astype(BF)
        dup_ref[rs, :] = dup
        dgate_ref[rs, :] = dgate
        acc_ref[rs, :] += dot_nt(dgate, w1) + dot_nt(dup, w3)

    @pl.when(step == pl.num_programs(0) - 1)
    def _():
        total = jnp.zeros(gn_ref.shape, F32)
        for c in range(rows // chunk):
            rs = slice(c * chunk, (c + 1) * chunk)
            hid = h_ref[rs, :].astype(F32)
            inv = inv_rms(hid)
            unit = hid * inv
            grad = acc_ref[rs, :]
            total += jnp.sum(grad * unit, axis=0, keepdims=True)
            dh = grad_rows(c) + norm_back(unit, inv, gain_ref[...], grad)
            dh_ref[rs, :] = dh
            dhb_ref[rs, :] = dh.astype(BF)
        gn_ref[...] = total


def mlp(place, hidden, g_parts, gain, w_gate, w_up, w_down):
    rows, dim = hidden.shape
    ff = w_gate.shape[1]
    fix = lambda *shape: pl.BlockSpec(shape, lambda i, s: (0,) * len(shape))
    wide = pl.BlockSpec((dim, FFB), lambda i, s: (0, i))
    tall = pl.BlockSpec((FFB, dim), lambda i, s: (i, 0))
    act = pl.BlockSpec((rows, FFB), lambda i, s: (0, i))
    act_t = pl.BlockSpec((FFB, rows), lambda i, s: (i, 0))
    return pl.pallas_call(
        mlp_kernel,
        grid_spec=pltpu.PrefetchScalarGridSpec(
            num_scalar_prefetch=1, grid=(ff // FFB,),
            in_specs=[fix(rows, dim), fix(rows // 2, dim), fix(rows // 2, dim), fix(1, dim), wide, wide, tall],
            out_specs=[fix(dim, rows), fix(rows, dim), act, act, act_t, fix(rows, dim), fix(rows, dim), fix(1, dim)],
            scratch_shapes=[pltpu.VMEM((rows, dim), BF), pltpu.VMEM((rows, dim), F32)]),
        out_shape=[jax.ShapeDtypeStruct((dim, rows), BF), jax.ShapeDtypeStruct((rows, dim), BF),
                   jax.ShapeDtypeStruct((rows, ff), BF), jax.ShapeDtypeStruct((rows, ff), BF),
                   jax.ShapeDtypeStruct((ff, rows), BF), jax.ShapeDtypeStruct((rows, dim), F32),
                   jax.ShapeDtypeStruct((rows, dim), BF), jax.ShapeDtypeStruct((1, dim), F32)],
        compiler_params=pltpu.CompilerParams(vmem_limit_bytes=56 << 20),
        cost_estimate=cost(10 * rows * dim * ff, 40 << 20, rows * ff),
        name="mlp",
    )(place, hidden, *g_parts, gain, w_gate, w_up, w_down)


def mlp_weights_kernel(n2t_ref, gt_ref, dgate_ref, dup_ref, ut_ref, n2t2_ref, gt2_ref, dgate2_ref, dup2_ref, ut2_ref,
                       g1_ref, g3_ref, g2_ref):
    g1_ref[...] = dot(n2t_ref[...], dgate_ref[...]) + dot(n2t2_ref[...], dgate2_ref[...])
    g3_ref[...] = dot(n2t_ref[...], dup_ref[...]) + dot(n2t2_ref[...], dup2_ref[...])
    g2_ref[...] = dot(ut_ref[...], gt_ref[...]) + dot(ut2_ref[...], gt2_ref[...])


def mlp_weights(factors, factors_near):
    dim, rows = factors[0].shape
    ff = factors[2].shape[1]
    fix = lambda *shape: pl.BlockSpec(shape, lambda i: (0,) * len(shape))
    act = pl.BlockSpec((rows, WFB), lambda i: (0, i))
    wide = pl.BlockSpec((dim, WFB), lambda i: (0, i))
    ins = [fix(dim, rows), fix(rows, dim), act, act, pl.BlockSpec((WFB, rows), lambda i: (i, 0))]
    return pl.pallas_call(
        mlp_weights_kernel,
        grid=(ff // WFB,),
        in_specs=ins + ins,
        out_specs=[wide, wide, pl.BlockSpec((WFB, dim), lambda i: (i, 0))],
        out_shape=[jax.ShapeDtypeStruct((dim, ff), F32)] * 2 + [jax.ShapeDtypeStruct((ff, dim), F32)],
        compiler_params=pltpu.CompilerParams(vmem_limit_bytes=60 << 20),
        cost_estimate=cost(12 * rows * dim * ff, 50 << 20),
        name="mlp_weights",
    )(*factors, *factors_near)


def memory_kernel(core_ref, a0_ref, a1_ref, a2_ref, b0_ref, b1_ref, b2_ref, wk_ref, wv_ref, o_ref):
    core = core_ref[0]
    total = None
    for who, refs in ((core, (a0_ref, a1_ref, a2_ref)), (1 - core, (b0_ref, b1_ref, b2_ref))):
        for i, ref in enumerate(refs):
            rows = pl.ds(pl.multiple_of((who * 3 + i) * PAIR, PAIR), PAIR)
            part = dot(ref[...].T, jnp.concatenate([wk_ref[rows, :], wv_ref[rows, :]], axis=0))
            total = part if total is None else total + part
    o_ref[...] = total


def memory_grad(core, mine, near, wkt, wvt):
    rows = mine[0].shape[-1]
    dim = wkt.shape[1]
    block = pl.BlockSpec((2 * PAIR, MB), lambda i, s: (0, i))
    whole = pl.BlockSpec(wkt.shape, lambda i, s: (0, 0))
    return pl.pallas_call(
        memory_kernel,
        out_shape=jax.ShapeDtypeStruct((rows, dim), F32),
        grid_spec=pltpu.PrefetchScalarGridSpec(
            num_scalar_prefetch=1, grid=(rows // MB,),
            in_specs=[block] * 6 + [whole, whole],
            out_specs=pl.BlockSpec((MB, dim), lambda i, s: (i, 0))),
        compiler_params=pltpu.CompilerParams(vmem_limit_bytes=32 << 20),
        cost_estimate=cost(4 * rows * dim * dim, 16 << 20),
        name="memory_grad",
    )(core, *mine, *near, wkt, wvt)


def half_index(i, core):
    return i + core - 2 * i * core


def out_proj_kernel(core_ref, mine_ref, near0_ref, near1_ref, dh_ref, o_ref):
    half = near0_ref.shape[1]

    @pl.when(pl.program_id(0) == 0)
    def _():
        o_ref[...] = dot(mine_ref[...], dh_ref[...])

    @pl.when(pl.program_id(0) == 1)
    def _():
        o_ref[...] = dot(near0_ref[...], dh_ref[:half, :]) + dot(near1_ref[...], dh_ref[half:, :])


def out_proj_grad(core, mine, near, dh):
    width, rows = mine.shape
    dim = dh.shape[1]
    whole = pl.BlockSpec((width, rows), lambda i, s: (0, 0))
    part = pl.BlockSpec((width, rows // 2), lambda i, s: (0, 0))
    return pl.pallas_call(
        out_proj_kernel,
        out_shape=jax.ShapeDtypeStruct((2 * width, dim), F32),
        grid_spec=pltpu.PrefetchScalarGridSpec(
            num_scalar_prefetch=1, grid=(2,),
            in_specs=[whole, part, part, pl.BlockSpec((rows, dim), lambda i, s: (0, 0))],
            out_specs=pl.BlockSpec((width, dim), lambda i, s: (half_index(i, s[0]), 0))),
        compiler_params=pltpu.CompilerParams(vmem_limit_bytes=24 << 20),
        cost_estimate=cost(4 * rows * dim * width, 6 << 20),
        name="out_proj_grad",
    )(core, mine, *near, dh)


def query_grad_kernel(place_ref, mine_ref, near_ref, n1_ref, wq_ref, x_ref, dh_ref, gain_ref,
                      gw_ref, gx_ref, gn_ref, acc_ref):
    half = acc_ref.shape[0] // 2

    @pl.when(pl.program_id(0) == 0)
    def _():
        gw_ref[...] = dot(mine_ref[...], n1_ref[...])
        acc_ref[...] = dot(mine_ref[...].T, wq_ref[...])

    @pl.when(pl.program_id(0) == 1)
    def _():
        first, second = near_ref[:, half:], near_ref[:, :half]
        gw_ref[...] = dot(first, n1_ref[:half, :]) + dot(second, n1_ref[half:, :])
        acc_ref[:half, :] += dot(first.T, wq_ref[...])
        acc_ref[half:, :] += dot(second.T, wq_ref[...])

    @pl.when(pl.program_id(0) == 1)
    def _():
        rows = gx_ref.shape[0]
        total = jnp.zeros(gn_ref.shape, F32)
        for c in range(acc_ref.shape[0] // rows):
            rs = slice(c * rows, (c + 1) * rows)
            x = x_ref[rs, :].astype(F32)
            total += jnp.sum(acc_ref[rs, :] * (x * inv_rms(x)), axis=0, keepdims=True)
        gn_ref[...] = total
        own = pl.ds(pl.multiple_of(place_ref[0] * rows, rows), rows)
        x = x_ref[own, :].astype(F32)
        inv = inv_rms(x)
        gx_ref[...] = dh_ref[...] + norm_back(x * inv, inv, gain_ref[...], acc_ref[own, :])


def query_grad(place, mine, near, n1, wqt, x_all, d_hid, gain, rows):
    width, total = mine.shape
    dim = n1.shape[1]
    fix = lambda *shape: pl.BlockSpec(shape, lambda i, s: (0,) * len(shape))
    half = pl.BlockSpec((width, dim), lambda i, s: (half_index(i, s[4]), 0))
    return pl.pallas_call(
        query_grad_kernel,
        out_shape=[jax.ShapeDtypeStruct((2 * width, dim), F32), jax.ShapeDtypeStruct((rows, dim), F32),
                   jax.ShapeDtypeStruct((1, dim), F32)],
        grid_spec=pltpu.PrefetchScalarGridSpec(
            num_scalar_prefetch=1, grid=(2,),
            in_specs=[fix(width, total), fix(width, total), fix(total, dim), half, fix(total, dim),
                      pl.BlockSpec((rows, dim), lambda i, s: (s[0], 0)), fix(1, dim)],
            out_specs=[half, fix(rows, dim), fix(1, dim)],
            scratch_shapes=[pltpu.VMEM((total, dim), F32)]),
        compiler_params=pltpu.CompilerParams(vmem_limit_bytes=32 << 20),
        cost_estimate=cost(8 * total * dim * width, 10 << 20),
        name="query_grad",
    )(place, mine, near, n1, wqt, x_all, d_hid, gain)


def key_weights_kernel(core_ref, *refs):
    gk_ref, gv_ref = refs[-2:]
    count = (len(refs) - 2) // 2
    for at in range(count):
        @pl.when(pl.program_id(0) == at)
        def _():
            a, b = refs[at], refs[count + at]
            gk_ref[...] = a[:PAIR, :] + b[:PAIR, :]
            gv_ref[...] = a[PAIR:, :] + b[PAIR:, :]


def key_weights(core, parts, others):
    pairs = len(parts) // 2
    dim = parts[0].shape[1]
    out = pl.BlockSpec((PAIR, dim), lambda i, s: (half_index(i // pairs, s[0]) * pairs + i % pairs, 0))
    return pl.pallas_call(
        key_weights_kernel,
        out_shape=[jax.ShapeDtypeStruct((2 * pairs * PAIR, dim), F32)] * 2,
        grid_spec=pltpu.PrefetchScalarGridSpec(
            num_scalar_prefetch=1, grid=(2 * pairs,),
            in_specs=[pl.BlockSpec((2 * PAIR, dim), lambda i, s: (0, 0))] * (4 * pairs),
            out_specs=[out, out]),
        compiler_params=pltpu.CompilerParams(vmem_limit_bytes=60 << 20),
        cost_estimate=cost(4 * pairs * PAIR * dim, 10 << 20),
        name="key_weights",
    )(core, *parts, *others)


def inv_rms(tensor):
    return lax.rsqrt(jnp.mean(tensor * tensor, axis=-1, keepdims=True) + 1e-6)


def norm_back(unit, inv, gain, grad):
    scaled = grad * gain
    return inv * (scaled - unit * jnp.mean(scaled * unit, axis=-1, keepdims=True))


def mm(a, b, ca, cb, dtype=F32):
    out = lax.dot_general(a, b, (((ca,), (cb,)), ((), ())), preferred_element_type=F32)
    return out if dtype == F32 else out.astype(dtype)


def solution(mesh):
    n = mesh.shape['seq']
    near = [(i, i ^ 1) for i in range(n)]
    far = [(i, i ^ 2) for i in range(n)]
    row_spec = P(('data', 'seq'), None)
    weight_spec = P()
    part_vec = P('data')
    part_mat = P('data', None)
    part_cube = P('data', None, None)

    def to_near(a):
        return lax.ppermute(a, 'seq', near)

    def to_far(a):
        return lax.ppermute(a, 'seq', far)

    def device_work(dec_in, memory, mem_len, grad_out, norm_attn, wq, wk, wv, wo, norm_mlp, w_gate, w_up, w_down):
        rows, dim = dec_in.shape
        m_rows = memory.shape[0]
        heads, head = wq.shape[1], wq.shape[2]
        mine = heads // 2
        width = mine * head
        dev = lax.axis_index('seq')
        core = lax.rem(dev, 2)
        core1 = core.reshape(1).astype(jnp.int32)
        wqt, wkt, wvt = (w.transpose(1, 2, 0).reshape(heads * head, dim) for w in (wq, wk, wv))
        wo2 = wo.reshape(heads * head, dim)
        lens = jnp.stack([jnp.clip(mem_len[0] - i * m_rows, 0, m_rows) for i in (dev, dev ^ 1)]).astype(jnp.int32)
        chip = dev // 2
        place = jnp.stack([chip, 2 + chip, 1 - chip, 3 - chip, core]).astype(jnp.int32)
        gain1 = norm_attn.astype(F32).reshape(1, dim)
        gain2 = norm_mlp.astype(F32).reshape(1, dim)

        def gather_parts(a):
            across = to_far(a)
            beside = to_near(a)
            return a, beside, across, to_near(across)

        x_parts = gather_parts(dec_in)
        mem_near = to_near(memory)
        g_parts = (grad_out, to_far(grad_out))

        first = project(core1, memory, wkt, wvt, 0, ())
        x_all_b, n1, _, qt_s = queries(place, x_parts, gain1, wqt)
        k, v, kt, vt = project(core1, mem_near, wkt, wvt, 1, first)

        pairs = mine // 2
        pieces = [(pair, 0, n * rows) for pair in range(pairs - 1)]
        pieces += [(pairs - 1, 0, n * rows // 2), (pairs - 1, n * rows // 2, n * rows // 2)]
        outs, lses = [], []
        parts = []
        for pair, at, count in pieces:
            part = attention_forward(lens, qt_s, k, vt, pair, 1, at, count)
            parts.append((part, to_far(part)))
        outs_b = []
        for a, b in parts:
            o_piece, ob_piece, lse_piece = combine(a, b)
            outs.append(o_piece)
            outs_b.append(ob_piece)
            lses.append(lse_piece)
        for pieces_of, axis in ((outs, 2), (outs_b, 1), (lses, 2)):
            pieces_of[-2:] = [jnp.concatenate(pieces_of[-2:], axis=axis)]
        o_t = jnp.concatenate(outs, axis=0)
        lse = jnp.concatenate(lses, axis=0)
        o_t_b = jnp.concatenate(outs_b, axis=0)
        half = n * rows // 2
        o_t_first, o_t_second = o_t_b[:, :half], o_t_b[:, half:]
        o_near_first = to_near(o_t_second)

        def half_rows(w, who):
            return lax.dynamic_slice(w, (who * width, 0), (width, dim))

        wo_m, wo_n = half_rows(wo2, core), half_rows(wo2, 1 - core)
        hidden = (x_all_b[:half].astype(F32) + mm(o_t_first, wo_m, 0, 0) + mm(o_near_first, wo_n, 0, 0)).astype(BF)

        n2t, g_top, d_gate, d_up, act_t, d_hid, d_hid_half, g_norm_half = mlp(
            place, hidden, g_parts, gain2, w_gate, w_up, w_down)
        d_hid_b = jnp.concatenate([d_hid_half, to_near(d_hid_half)], axis=0)
        factors = (n2t, g_top, d_gate, d_up, act_t)
        factors_near = tuple(to_near(a) for a in factors)
        o_near_second = to_near(o_t_first)
        g_norm_mlp = g_norm_half + to_near(g_norm_half)

        do_t_f = mm(wo_m, d_hid_b, 1, 1)
        delta = jnp.sum(do_t_f.reshape(mine, head, n * rows) * o_t, axis=1, keepdims=True)
        do_t = do_t_f.astype(BF)
        dkvs, dkvs_near, dqs, dws = [], [], [], []
        lens_now = lens
        for pair in range(pairs):
            dkv, dkv_near, dqt, dw = attention_backward(
                lens_now, qt_s, do_t, lse, delta, k, v, kt, memory, mem_near, pair)
            dqs.append((dqt, to_far(dqt)))
            dws.append((dw, to_far(dw)))
            dkvs.append(dkv)
            dkvs_near.append(to_near(dkv_near))
            lens_now, dw_last = lax.optimization_barrier((lens, dw))

        act_t, _ = lax.optimization_barrier((act_t, dw_last))
        factors = (n2t, g_top, d_gate, d_up, act_t)
        g_gate, g_up, g_down = mlp_weights(factors, factors_near)
        g_mem = memory_grad(core1, dkvs, dkvs_near, wkt, wvt)

        def as_weight(rows_by_dim):
            return rows_by_dim.reshape(heads, head, dim).transpose(2, 0, 1)

        g_wo = out_proj_grad(core1, o_t_b, (o_near_first, o_near_second), d_hid_b).reshape(heads, head, dim)

        dqt_b = sum_queries([a for a, _ in dqs], [b for _, b in dqs])
        dqt_near = to_near(dqt_b)
        g_wqt, g_dec, g_norm_attn = query_grad(place, dqt_b, dqt_near, n1, wqt, x_all_b, d_hid, gain1, rows)

        mine_near = []
        for a, b in dws:
            a_near = to_near(a)
            mine_near.append((a_near, to_near(b)))
        g_wkt, g_wvt = key_weights(core1, [a for a, _ in dws] + [a for a, _ in mine_near],
                                   [b for _, b in dws] + [b for _, b in mine_near])
        g_wq, g_wk, g_wv = as_weight(g_wqt), as_weight(g_wkt), as_weight(g_wvt)
        return (g_dec, g_mem, g_norm_attn.reshape(dim), g_wq, g_wk, g_wv, g_wo, g_norm_mlp.reshape(dim), g_gate, g_up, g_down)


    return jax.shard_map(device_work, mesh=mesh,
                         in_specs=(row_spec, row_spec, part_vec, row_spec) + (weight_spec,) * 9,
                         out_specs=(row_spec, row_spec, part_vec, part_cube, part_cube, part_cube, part_cube,
                                    part_vec, part_mat, part_mat, part_mat),
                         check_vma=False)
```
